32 devices in a mesh: dp: 2 (over x), row: 4 (over z), col: 4 (over y, core).
Axes of the slice: x: 2, y: 2, z: 4, core: 2. Of those that a mesh axis runs over, the one named last changes fastest.
Arguments:
- pair_rep: bfloat16 [1024, 512, 128], P(('dp', 'row'), 'col'), parts along dimension 0
- res_mask: int32 [1024], P('dp'), parts along dimension 0
- ln_gamma: float32 [128], replicated
- ln_beta: float32 [128], replicated
- w_q: bfloat16 [128, 128], replicated
- w_k: bfloat16 [128, 128], replicated
- w_v: bfloat16 [128, 128], replicated
- w_b: bfloat16 [128, 4], replicated
- w_g: bfloat16 [128, 128], replicated
- w_o: bfloat16 [128, 128], replicated
Outputs:
- output: bfloat16 [1024, 512, 128], P(('dp', 'row'), 'col'), parts along dimension 0
There are 2 independent parts. The reference program is written for one: setup_inputs(seed, part) draws one part's arguments, and reference() takes and returns one part's arrays. A program takes and returns all parts, laid end to end along the dimension named above; an argument that names none is the same for every part.
All inputs are finite; a program needn't handle non-finite values.
Results may differ from the reference program's by a relative error of at most 0.00749931.
Values are sent between devices in bfloat16 or wider.
A program may use at most 1 GiB of HBM per device.

```python
import jax
import jax.numpy as jnp
from jax import lax

N = 512
C_Z = 128
HEADS = 4
HEAD = 32
LN_EPS = 1e-5


def layer_norm(pair_rep, ln_gamma, ln_beta):
    pair_f32 = pair_rep.astype(jnp.float32)
    mean_c = jnp.mean(pair_f32, axis=-1, keepdims=True)
    centered = pair_f32 - mean_c
    var_c = jnp.mean(jnp.square(centered), axis=-1, keepdims=True)
    return (centered * lax.rsqrt(var_c + LN_EPS) * ln_gamma + ln_beta).astype(jnp.bfloat16)


def setup_inputs(seed: int = 0, part: int = 0) -> dict:
    part_key = jax.random.fold_in(jax.random.key(seed), part)
    pair_key, len_key = jax.random.split(part_key)
    weight_keys = jax.random.split(jax.random.key(seed + 1), 8)
    proj_dim = HEADS * HEAD
    in_scale = C_Z ** -0.5
    pair_rep = jax.random.normal(pair_key, (N, N, C_Z), jnp.float32).astype(jnp.bfloat16)
    seq_len = jax.random.randint(len_key, (), N // 4, N - N // 8 + 1)
    res_mask = (jnp.arange(N) < seq_len).astype(jnp.int32)
    ln_gamma = 1.0 + 0.5 * jax.random.normal(weight_keys[0], (C_Z,), jnp.float32)
    ln_beta = 0.5 * jax.random.normal(weight_keys[1], (C_Z,), jnp.float32)
    w_q = (jax.random.normal(weight_keys[2], (C_Z, proj_dim), jnp.float32) * in_scale).astype(jnp.bfloat16)
    w_k = (jax.random.normal(weight_keys[3], (C_Z, proj_dim), jnp.float32) * in_scale).astype(jnp.bfloat16)
    w_v = (jax.random.normal(weight_keys[4], (C_Z, proj_dim), jnp.float32) * in_scale).astype(jnp.bfloat16)
    w_b = (jax.random.normal(weight_keys[5], (C_Z, HEADS), jnp.float32) * in_scale).astype(jnp.bfloat16)
    w_g = (jax.random.normal(weight_keys[6], (C_Z, proj_dim), jnp.float32) * in_scale).astype(jnp.bfloat16)
    w_o = (jax.random.normal(weight_keys[7], (proj_dim, C_Z), jnp.float32) * (4.0 * proj_dim ** -0.5)).astype(jnp.bfloat16)
    return {'pair_rep': pair_rep, 'res_mask': res_mask, 'ln_gamma': ln_gamma, 'ln_beta': ln_beta, 'w_q': w_q, 'w_k': w_k, 'w_v': w_v, 'w_b': w_b, 'w_g': w_g, 'w_o': w_o}


def reference(pair_rep, res_mask, ln_gamma, ln_beta, w_q, w_k, w_v, w_b, w_g, w_o):
    proj_dim = HEADS * HEAD
    normed = layer_norm(pair_rep, ln_gamma, ln_beta)
    pair_bias = jnp.dot(normed.reshape(N * N, C_Z), w_b, preferred_element_type=jnp.float32).astype(jnp.bfloat16)
    key_bias = jnp.where(res_mask > 0, 0.0, -1e9).astype(jnp.float32)
    full_bias = pair_bias.reshape(N, N, HEADS).astype(jnp.float32) + key_bias[None, :, None]

    def one_row(row_args):
        pair_row, normed_row = row_args
        queries = (jnp.dot(normed_row, w_q, preferred_element_type=jnp.float32) * HEAD ** -0.5).astype(jnp.bfloat16)
        key_row = jnp.dot(normed_row, w_k, preferred_element_type=jnp.float32).astype(jnp.bfloat16)
        val_row = jnp.dot(normed_row, w_v, preferred_element_type=jnp.float32).astype(jnp.bfloat16)
        gate_vals = jax.nn.sigmoid(jnp.dot(normed_row, w_g, preferred_element_type=jnp.float32))
        logits = jnp.einsum('jhd,khd->jkh', queries.reshape(N, HEADS, HEAD).astype(jnp.float32), key_row.reshape(N, HEADS, HEAD).astype(jnp.float32)) + full_bias
        weights = jax.nn.softmax(logits, axis=1)
        attended = jnp.einsum('jkh,khd->jhd', weights, val_row.reshape(N, HEADS, HEAD).astype(jnp.float32))
        gated_out = (gate_vals * attended.reshape(N, proj_dim)).astype(jnp.bfloat16)
        update = jnp.dot(gated_out, w_o, preferred_element_type=jnp.float32)
        return (pair_row.astype(jnp.float32) + update).astype(jnp.bfloat16)

    return lax.map(one_row, (pair_rep, normed))
```

```python
import functools

import jax
import jax.numpy as jnp
from jax import lax
from jax.experimental import pallas as pl
from jax.experimental.pallas import tpu as pltpu
from jax.sharding import PartitionSpec as P

LN_EPS = 1e-5
F32 = jnp.float32
BF16 = jnp.bfloat16


def layer_norm(pair_rep, ln_gamma, ln_beta):
    pair_f32 = pair_rep.astype(F32)
    mean_c = jnp.mean(pair_f32, axis=-1, keepdims=True)
    centered = pair_f32 - mean_c
    var_c = jnp.mean(jnp.square(centered), axis=-1, keepdims=True)
    return (centered * lax.rsqrt(var_c + LN_EPS) * ln_gamma + ln_beta).astype(BF16)


def row_kernel(heads, n_q, z_ref, bias_ref, gamma_ref, beta_ref, wkt_ref, wv_ref, wqg_ref, wo_ref, out_ref):
    chan = z_ref.shape[-1]
    proj = wv_ref.shape[1]
    head_dim = proj // heads
    z = z_ref[0]
    a = layer_norm(z, gamma_ref[...], beta_ref[...])
    kt = lax.dot_general(wkt_ref[...], a, (((1,), (1,)), ((), ())), preferred_element_type=F32).astype(BF16)
    v = jnp.dot(a, wv_ref[...], preferred_element_type=F32).astype(BF16)
    qg = jnp.dot(a[:n_q], wqg_ref[...], preferred_element_type=F32)
    q = (qg[:, :proj] * head_dim ** -0.5).astype(BF16)
    gate = jax.nn.sigmoid(qg[:, proj:])
    lane_head = lax.broadcasted_iota(jnp.int32, (1, proj), 1) // head_dim
    att = jnp.zeros((n_q, proj), F32)
    for h in range(heads):
        mine = lane_head == h
        qh = jnp.where(mine, q, jnp.zeros_like(q))
        s = jnp.dot(qh, kt, preferred_element_type=F32) + bias_ref[h]
        m = jnp.max(s, axis=-1, keepdims=True)
        p = jnp.exp(s - m)
        l = jnp.sum(p, axis=-1, keepdims=True)
        o = jnp.dot(p.astype(BF16), v, preferred_element_type=F32)
        att = jnp.where(mine, o / l, att)
    go = (gate * att).astype(BF16)
    upd = jnp.dot(go, wo_ref[...], preferred_element_type=F32)
    out_ref[0] = (z[:n_q].astype(F32) + upd).astype(BF16)


def solution(mesh):
    col_size = mesh.shape['col']
    tile_spec = P(('dp', 'row'), 'col', None)
    partner_pairs = [(d, d ^ 1) for d in range(col_size)]

    def per_device(pair_tile, res_mask, ln_gamma, ln_beta, w_q, w_k, w_v, w_b, w_g, w_o):
        row_len, col_len, chan = pair_tile.shape
        heads = w_b.shape[1]
        proj = w_q.shape[1]
        col_idx = lax.axis_index('col')
        core = col_idx % 2
        half = row_len // 2
        n_q = 2 * col_len
        n_k = col_size * col_len
        shift = (col_idx // 2) * n_q

        normed = layer_norm(pair_tile, ln_gamma, ln_beta)
        bias_tile = jnp.dot(normed, w_b, preferred_element_type=F32).astype(BF16)
        bias_cols = lax.all_gather(bias_tile, 'row', axis=0, tiled=True)
        bias_rows = lax.all_to_all(bias_cols, 'col', 0, 1, tiled=True)
        bias_rows = jnp.transpose(bias_rows, (2, 0, 1))
        other = lax.ppermute(bias_rows, 'col', partner_pairs)
        both = jnp.where(core == 0, jnp.concatenate([bias_rows, other], 1), jnp.concatenate([other, bias_rows], 1))
        key_bias = jnp.where(res_mask > 0, 0.0, -1e9).astype(F32)
        full_bias = both.astype(F32) + key_bias
        full_bias = jnp.where(shift > 0, jnp.roll(full_bias, -n_q, 2), full_bias)

        z_all = lax.all_gather(pair_tile, 'col', axis=1, tiled=True)
        z_half = lax.dynamic_slice_in_dim(z_all, core * half, half, 0)
        z_half = jnp.where(shift > 0, jnp.roll(z_half, -n_q, 1), z_half)

        full = lambda *shape: pl.BlockSpec(shape, lambda i: (0,) * len(shape))
        out = pl.pallas_call(
            functools.partial(row_kernel, heads, n_q),
            grid=(half,),
            in_specs=[
                pl.BlockSpec((1, n_k, chan), lambda i: (i, 0, 0)),
                full(heads, n_q, n_k), full(1, chan), full(1, chan),
                full(proj, chan), full(chan, proj), full(chan, 2 * proj), full(proj, chan),
            ],
            out_specs=pl.BlockSpec((1, n_q, chan), lambda i: (i, 0, 0)),
            out_shape=jax.ShapeDtypeStruct((half, n_q, chan), BF16),
            compiler_params=pltpu.CompilerParams(vmem_limit_bytes=60 * 1024 * 1024),
        )(z_half, full_bias, ln_gamma.reshape(1, -1), ln_beta.reshape(1, -1), w_k.T, w_v, jnp.concatenate([w_q, w_g], 1), w_o)
        mine = lax.dynamic_slice_in_dim(out, core * col_len, col_len, 1)
        theirs = lax.dynamic_slice_in_dim(out, (1 - core) * col_len, col_len, 1)
        got = lax.ppermute(theirs, 'col', partner_pairs)
        return jnp.where(core == 0, jnp.concatenate([mine, got], 0), jnp.concatenate([got, mine], 0))

    return jax.shard_map(per_device, mesh=mesh, in_specs=(tile_spec, P('dp'), P(), P(), P(), P(), P(), P(), P(), P()), out_specs=tile_spec, check_vma=False)
```

```python
import functools

import jax
import jax.numpy as jnp
from jax import lax
from jax.experimental import pallas as pl
from jax.experimental.pallas import tpu as pltpu
from jax.sharding import PartitionSpec as P

LN_EPS = 1e-5
F32 = jnp.float32
BF16 = jnp.bfloat16
NT = (((1,), (1,)), ((), ()))
TN = (((0,), (0,)), ((), ()))
LOG2E = 1.4426950408889634
CORES = 2
SEND_ROWS = 2
OUT_ROWS = 4
EARLY = 4


def layer_norm(z, gamma, beta):
    x = z.astype(F32)
    centered = x - jnp.mean(x, axis=-1, keepdims=True)
    var = jnp.mean(jnp.square(centered), axis=-1, keepdims=True)
    return (centered * lax.rsqrt(var + LN_EPS) * gamma + beta).astype(BF16)


def over_keys(x, op):
    n, width = x.shape
    groups = 8
    t = op(x.reshape(groups, n // 8 // groups, 8, width), axis=1)
    return op(op(t, axis=0), axis=0, keepdims=True)


def kernel(heads, z_hbm, mask_ref, gamma_ref, beta_ref, wk_ref, wt_ref, wb_ref, wo_ref, out_hbm,
           zbuf, own, outv, bias, btile, bsend, brow, a0, a1, k0, k1, v0, v1, q0, q1, g0, g1,
           s0, s1, s2, s3, go,
           local_sem, zp_send, zp_recv, zs_send, zs_recv, b1_send, b1_recv, b2_send, b2_recv,
           b3_send, b3_recv, o_local, o_send, o_recv):
    rows_all, width, chan = z_hbm.shape
    rows = rows_all // CORES
    n_q = CORES * width
    proj = wk_ref.shape[1]
    hd = proj // heads
    steps = rows // SEND_ROWS
    dp, row, col = lax.axis_index('dp'), lax.axis_index('row'), lax.axis_index('col')
    n_row = lax.axis_size('row')
    core, chip = lax.rem(col, CORES), col // CORES
    partner = chip * CORES + 1 - core
    far = (1 - chip) * CORES
    home_chip = row // CORES
    jslot = lax.rem(row, CORES)
    home = chip == home_chip

    def remote(src, dst, send, recv, r, c):
        return pltpu.make_async_remote_copy(src, dst, send, recv, device_id=(dp, r, c),
                                            device_id_type=pl.DeviceIdType.MESH)

    barrier = pltpu.get_barrier_semaphore()
    peers = [(row, partner), (row, far), (row, far + 1)]
    peers += [(lax.rem(row + d, n_row), col) for d in range(1, 4)]
    for r, c in peers:
        pl.semaphore_signal(barrier, inc=1, device_id=(dp, r, c), device_id_type=pl.DeviceIdType.MESH)

    own_copy = pltpu.make_async_copy(z_hbm, own, local_sem.at[0])
    own_copy.start()
    mine_at = pl.ds(pl.multiple_of(core * width, width), width)
    theirs_at = pl.ds(pl.multiple_of((1 - core) * width, width), width)
    far_at = pl.ds(pl.multiple_of((CORES + core) * width, width), width)
    z_copy = pltpu.make_async_copy(z_hbm.at[pl.ds(core * rows, rows)], zbuf.at[:, mine_at, :], local_sem.at[1])
    z_copy.start()
    pl.semaphore_wait(barrier, len(peers))

    to_partner = remote(z_hbm.at[pl.ds((1 - core) * rows, rows)], zbuf.at[:, mine_at, :], zp_send, zp_recv, row, partner)

    def z_send(g, k):
        return remote(z_hbm.at[pl.ds(k * rows + g * SEND_ROWS, SEND_ROWS)],
                      zbuf.at[pl.ds(g * SEND_ROWS, SEND_ROWS), far_at, :],
                      zs_send.at[k, g], zs_recv.at[core, g], row, far + k)

    def z_wait(g):
        for k in range(CORES):
            at = pl.ds((CORES + k) * width, width)
            remote(z_hbm.at[pl.ds(0, SEND_ROWS)], zbuf.at[pl.ds(g * SEND_ROWS, SEND_ROWS), at, :],
                   zs_send.at[k, g], zs_recv.at[k, g], row, far + k).wait_recv()

    def send_step(g, carry):
        for k in range(CORES):
            z_send(g, k).start()
        return carry

    lax.fori_loop(0, EARLY, send_step, 0)
    to_partner.start()

    own_copy.wait()
    batch = 8

    def bias_step(i, carry):
        a = layer_norm(own[pl.ds(i * batch, batch)].reshape(batch * width, chan), gamma_ref[...], beta_ref[...])
        t = lax.dot_general(wb_ref[...], a, NT, preferred_element_type=F32)
        for j in range(batch):
            for h in range(heads):
                brow[h, pl.ds(i * batch + j, 1), :] = t[h:h + 1, j * width:(j + 1) * width]
        return carry

    lax.fori_loop(0, rows_all // batch, bias_step, 0)
    home_slot = core * CORES + jslot
    cross_slot = (CORES + core) * CORES + jslot
    for h in range(heads):
        tile = brow[h].T.astype(BF16)
        bsend[h] = tile

        @pl.when(home)
        def _():
            btile[home_slot, h] = tile

    masks = []
    for s in range(2 * CORES):
        block = chip * CORES + s if s < CORES else far + s - CORES
        m = mask_ref[:, pl.ds(pl.multiple_of(block * width, width), width)]
        masks.append(jnp.broadcast_to(jnp.where(m > 0, 0.0, -1e9).astype(F32), (width, width)).T)

    cross = remote(bsend, btile.at[cross_slot], b1_send, b1_recv, row, far + core)

    @pl.when(jnp.logical_not(home))
    def _():
        cross.start()

    lax.fori_loop(EARLY, steps, send_step, 0)

    def spread(t, d):
        src = bsend if t == 0 else btile.at[cross_slot]
        slot = home_slot if t == 0 else cross_slot
        return remote(src, btile.at[slot], b2_send.at[t, d - 1], b2_recv.at[t, jslot], lax.rem(row + d, n_row), col)

    @pl.when(home)
    def _():
        for d in range(1, 4):
            spread(0, d).start()
        cross.wait_recv()
        for d in range(1, 4):
            spread(1, d).start()

    def forward(t, j):
        slot = (core + CORES * t) * CORES + j
        return remote(btile.at[slot], btile.at[slot], b3_send.at[t, j], b3_recv.at[t, j], row, partner)

    for j in range(CORES):
        for t in range(2):
            slot = (core + CORES * t) * CORES + j

            @pl.when(row != chip * CORES + j)
            def _():
                remote(bsend, btile.at[slot], b1_send, b2_recv.at[t, j], row, partner).wait_recv()

            forward(t, j).start()
    for j in range(CORES):
        for t in range(2):
            slot = (1 - core + CORES * t) * CORES + j
            remote(bsend, btile.at[slot], b1_send, b3_recv.at[t, j], row, partner).wait_recv()

    for s in range(2 * CORES):
        for j in range(CORES):
            for h in range(heads):
                b = btile[s * CORES + j, h].astype(F32)
                bias[h, s * width:(s + 1) * width, j * width:(j + 1) * width] = (b + masks[s]) * LOG2E

    a_s, k_s, v_s, q_s, g_s, sc = (a0, a1), (k0, k1), (v0, v1), (q0, q1), (g0, g1), (s0, s1, s2, s3)
    scale = hd ** -0.5 * LOG2E

    def scores(slot, h):
        part = q_s[slot][h * hd:(h + 1) * hd, :]
        none = jnp.zeros_like(part)
        rhs = jnp.concatenate([part if i == h else none for i in range(heads)], axis=0)
        sc[h][...] = jnp.dot(k_s[slot][...], rhs, preferred_element_type=F32) + bias[h]

    def finish(r):
        upd = lax.dot_general(go[...], wo_ref[...], TN, preferred_element_type=F32)
        outv[r] = (zbuf[r, :n_q].astype(F32) + upd).astype(BF16)

    def out_copies(g):
        src = pl.ds(g * OUT_ROWS, OUT_ROWS)
        dst = out_hbm.at[pl.ds(core * rows + g * OUT_ROWS, OUT_ROWS)]
        return (pltpu.make_async_copy(outv.at[src, mine_at, :], dst, o_local.at[g]),
                remote(outv.at[src, theirs_at, :], dst, o_send.at[g], o_recv.at[g], row, partner))

    def step(i, carry):
        @pl.when(i < steps - 1)
        def _():
            z_wait(i + 1)

        lead = OUT_ROWS // 2 + 1

        @pl.when(jnp.logical_and(i >= lead, lax.rem(i - lead + OUT_ROWS, OUT_ROWS // 2) == 0))
        def _():
            for c in out_copies((i - lead) // (OUT_ROWS // 2)):
                c.start()

        for r in range(2):
            cur, nxt = r, 1 - r
            finish(jnp.maximum(2 * i + r - 1, 0))
            a_s[cur][...] = layer_norm(zbuf[jnp.minimum(2 * i + r + 2, rows - 1)], gamma_ref[...], beta_ref[...])
            a = a_s[nxt]
            for h in range(heads):
                if h < 2:
                    scores(cur, h + 2)
                else:
                    scores(nxt, h - 2)
                if h == 0:
                    k_s[nxt][...] = jnp.dot(a[...], wk_ref[...], preferred_element_type=F32).astype(BF16)
                    t = lax.dot_general(wt_ref[proj:2 * proj], a[:n_q], NT, preferred_element_type=F32)
                    q_s[nxt][...] = (t * scale).astype(BF16)
                if h == 1:
                    t = lax.dot_general(wt_ref[2 * proj:], a[:n_q], NT, preferred_element_type=F32)
                    g_s[nxt][...] = jax.nn.sigmoid(t)
                if h == 2:
                    t = lax.dot_general(wt_ref[:proj], a[...], NT, preferred_element_type=F32)
                    v_s[nxt][...] = t.astype(BF16)
                s = sc[h][...]
                p = jnp.exp2(s - over_keys(s, jnp.max))
                total = over_keys(p, jnp.sum)
                at = slice(h * hd, (h + 1) * hd)
                o = jnp.dot(v_s[cur][at, :], p.astype(BF16), preferred_element_type=F32)
                go[at, :] = (g_s[cur][at, :] * (o / total)).astype(BF16)
        return carry

    pltpu.make_async_copy(z_hbm.at[pl.ds(0, rows)], zbuf.at[:, mine_at, :], local_sem.at[1]).wait()
    to_partner_wait = remote(z_hbm.at[pl.ds(0, rows)], zbuf.at[:, theirs_at, :], zp_send, zp_recv, row, partner)
    to_partner_wait.wait_recv()
    lax.fori_loop(-1, steps, step, 0)
    finish(rows - 1)
    to_partner.wait_send()

    def sent(g, carry):
        for k in range(CORES):
            z_send(g, k).wait_send()
        return carry

    lax.fori_loop(0, steps, sent, 0)
    groups = rows // OUT_ROWS
    for c in out_copies(groups - 1):
        c.start()

    @pl.when(jnp.logical_not(home))
    def _():
        cross.wait_send()

    @pl.when(home)
    def _():
        for t in range(2):
            for d in range(1, 4):
                spread(t, d).wait_send()

    for j in range(CORES):
        for t in range(2):
            forward(t, j).wait_send()

    def drained(g, carry):
        mine, theirs = out_copies(g)
        mine.wait()
        theirs.wait_send()
        remote(outv.at[pl.ds(0, OUT_ROWS), theirs_at, :],
               out_hbm.at[pl.ds((1 - core) * rows + g * OUT_ROWS, OUT_ROWS)],
               o_send.at[g], o_recv.at[g], row, partner).wait_recv()
        return carry

    lax.fori_loop(0, groups, drained, 0)


def solution(mesh):
    tile_spec = P(('dp', 'row'), 'col', None)

    def per_device(pair_tile, res_mask, ln_gamma, ln_beta, w_q, w_k, w_v, w_b, w_g, w_o):
        row_len, width, chan = pair_tile.shape
        heads, proj = w_b.shape[1], w_q.shape[1]
        hd = proj // heads
        rows, n_q = row_len // CORES, CORES * width
        n_k = mesh.shape['col'] * width
        steps, groups = rows // SEND_ROWS, rows // OUT_ROWS
        vmem = pltpu.VMEM
        dma = pltpu.SemaphoreType.DMA
        pairs = lambda *s: [vmem(*s)] * 2
        whole = pl.BlockSpec(memory_space=pltpu.VMEM)
        hbm = pl.BlockSpec(memory_space=pl.ANY)
        return pl.pallas_call(
            functools.partial(kernel, heads),
            in_specs=[hbm] + [whole] * 7,
            out_specs=hbm,
            out_shape=jax.ShapeDtypeStruct(pair_tile.shape, BF16),
            scratch_shapes=[
                vmem((rows, n_k, chan), BF16), vmem((row_len, width, chan), BF16), vmem((rows, n_q, chan), BF16),
                vmem((heads, n_k, n_q), F32), vmem((8, heads, width, width), BF16), vmem((heads, width, width), BF16),
                vmem((heads, width, width), F32),
                *pairs((n_k, chan), BF16), *pairs((n_k, proj), BF16), *pairs((proj, n_k), BF16),
                *pairs((proj, n_q), BF16), *pairs((proj, n_q), F32),
                *[vmem((n_k, n_q), F32)] * 4, vmem((proj, n_q), BF16),
                dma((2,)), dma, dma, dma((CORES, steps)), dma((CORES, steps)), dma, dma, dma((2, 3)), dma((2, CORES)),
                dma((2, CORES)), dma((2, CORES)), dma((groups,)), dma((groups,)), dma((groups,)),
            ],
            compiler_params=pltpu.CompilerParams(collective_id=0, has_side_effects=True, vmem_limit_bytes=56 * 1024 * 1024),
        )(pair_tile, res_mask.reshape(1, -1), ln_gamma.reshape(1, -1), ln_beta.reshape(1, -1), w_k,
          jnp.concatenate([w_v.T, w_q.T, w_g.T], 0), jnp.pad(w_b.T, ((0, 8 - heads), (0, 0))), w_o)

    return jax.shard_map(per_device, mesh=mesh, in_specs=(tile_spec, P('dp'), P(), P(), P(), P(), P(), P(), P(), P()), out_specs=tile_spec, check_vma=False)
```

```python
import functools

import jax
import jax.numpy as jnp
from jax import lax
from jax.experimental import pallas as pl
from jax.experimental.pallas import tpu as pltpu
from jax.sharding import PartitionSpec as P

LN_EPS = 1e-5
F32 = jnp.float32
BF16 = jnp.bfloat16
NT = (((1,), (1,)), ((), ()))
TN = (((0,), (0,)), ((), ()))
LOG2E = 1.4426950408889634
CORES = 2
SEND_ROWS = 2
OUT_ROWS = 4
SMALLS = 9
EARLY = 4


def layer_norm(z, gamma, beta):
    x = z.astype(F32)
    centered = x - jnp.mean(x, axis=-1, keepdims=True)
    var = jnp.mean(jnp.square(centered), axis=-1, keepdims=True)
    return (centered * lax.rsqrt(var + LN_EPS) * gamma + beta).astype(BF16)


def over_keys(x, op):
    n, width = x.shape
    groups = 8
    t = op(x.reshape(groups, n // 8 // groups, 8, width), axis=1)
    return op(op(t, axis=0), axis=0, keepdims=True)


def kernel(heads, z_hbm, *refs):
    body(heads, z_hbm, refs[:SMALLS], refs[SMALLS + 1:2 * SMALLS + 1], refs[SMALLS], *refs[2 * SMALLS + 1:])


def body(heads, z_hbm, small_hbm, small_refs, out_ref,
           wt_ref, zbuf, own, outv, bias, btile, bsend, brow, a0, a1, k0, k1, v0, v1, q0, q1, g0, g1,
           s0, s1, s2, s3, go,
           small_sem, local_sem, zp_send, zp_recv, zs_send, zs_recv, b1_send, b1_recv, b2_send, b2_recv,
           b3_send, b3_recv, o_send, o_recv):
    mask_ref, gamma_ref, beta_ref, wq_ref, wk_ref, wv_ref, wbt_ref, wg_ref, wo_ref = small_refs
    rows_all, width, chan = z_hbm.shape
    rows = rows_all // CORES
    n_q = CORES * width
    proj = wk_ref.shape[1]
    hd = proj // heads
    steps = rows // SEND_ROWS
    dp, row, col = lax.axis_index('dp'), lax.axis_index('row'), lax.axis_index('col')
    n_row = lax.axis_size('row')
    core, chip = lax.rem(col, CORES), col // CORES
    partner = chip * CORES + 1 - core
    far = (1 - chip) * CORES
    home_chip = row // CORES
    jslot = lax.rem(row, CORES)
    home = chip == home_chip

    def remote(src, dst, send, recv, r, c):
        return pltpu.make_async_remote_copy(src, dst, send, recv, device_id=(dp, r, c),
                                            device_id_type=pl.DeviceIdType.MESH)

    barrier = pltpu.get_barrier_semaphore()
    peers = [(row, partner), (row, far), (row, far + 1)]
    peers += [(lax.rem(row + d, n_row), col) for d in range(1, 4)]
    for r, c in peers:
        pl.semaphore_signal(barrier, inc=1, device_id=(dp, r, c), device_id_type=pl.DeviceIdType.MESH)

    own_copy = pltpu.make_async_copy(z_hbm, own, local_sem.at[0])
    own_copy.start()
    mine_at = pl.ds(pl.multiple_of(core * width, width), width)
    theirs_at = pl.ds(pl.multiple_of((1 - core) * width, width), width)
    far_at = pl.ds(pl.multiple_of((CORES + core) * width, width), width)
    z_copy = pltpu.make_async_copy(z_hbm.at[pl.ds(core * rows, rows)], zbuf.at[:, mine_at, :], local_sem.at[1])
    z_copy.start()
    small_copies = [pltpu.make_async_copy(src, dst, small_sem.at[i]) for i, (src, dst) in enumerate(zip(small_hbm, small_refs))]
    for c in small_copies:
        c.start()
    for c in small_copies:
        c.wait()
    for i, w in enumerate((wv_ref, wq_ref, wg_ref)):
        wt_ref[i * proj:(i + 1) * proj] = w[...].T
    pl.semaphore_wait(barrier, len(peers))

    to_partner = remote(z_hbm.at[pl.ds((1 - core) * rows, rows)], zbuf.at[:, mine_at, :], zp_send, zp_recv, row, partner)

    def z_send(g, k):
        return remote(z_hbm.at[pl.ds(k * rows + g * SEND_ROWS, SEND_ROWS)],
                      zbuf.at[pl.ds(g * SEND_ROWS, SEND_ROWS), far_at, :],
                      zs_send.at[k, g], zs_recv.at[core, g], row, far + k)

    def z_wait(g):
        for k in range(CORES):
            at = pl.ds((CORES + k) * width, width)
            remote(z_hbm.at[pl.ds(0, SEND_ROWS)], zbuf.at[pl.ds(g * SEND_ROWS, SEND_ROWS), at, :],
                   zs_send.at[k, g], zs_recv.at[k, g], row, far + k).wait_recv()

    def send_step(g, carry):
        for k in range(CORES):
            z_send(g, k).start()
        return carry

    lax.fori_loop(0, EARLY, send_step, 0)
    to_partner.start()

    own_copy.wait()
    batch = 8

    def bias_step(i, carry):
        a = layer_norm(own[pl.ds(i * batch, batch)].reshape(batch * width, chan), gamma_ref[...], beta_ref[...])
        t = lax.dot_general(wbt_ref[...], a, NT, preferred_element_type=F32)
        for j in range(batch):
            for h in range(heads):
                brow[h, pl.ds(i * batch + j, 1), :] = t[h:h + 1, j * width:(j + 1) * width]
        return carry

    lax.fori_loop(0, rows_all // batch, bias_step, 0)
    home_slot = core * CORES + jslot
    cross_slot = (CORES + core) * CORES + jslot
    for h in range(heads):
        tile = brow[h].T.astype(BF16)
        bsend[h] = tile

        @pl.when(home)
        def _():
            btile[home_slot, h] = tile

    masks = []
    for s in range(2 * CORES):
        block = chip * CORES + s if s < CORES else far + s - CORES
        m = mask_ref[:, pl.ds(pl.multiple_of(block * width, width), width)]
        masks.append(jnp.broadcast_to(jnp.where(m > 0, 0.0, -1e9).astype(F32), (width, width)).T)

    cross = remote(bsend, btile.at[cross_slot], b1_send, b1_recv, row, far + core)

    @pl.when(jnp.logical_not(home))
    def _():
        cross.start()

    lax.fori_loop(EARLY, steps, send_step, 0)

    def spread(t, d):
        src = bsend if t == 0 else btile.at[cross_slot]
        slot = home_slot if t == 0 else cross_slot
        return remote(src, btile.at[slot], b2_send.at[t, d - 1], b2_recv.at[t, jslot], lax.rem(row + d, n_row), col)

    @pl.when(home)
    def _():
        for d in range(1, 4):
            spread(0, d).start()
        cross.wait_recv()
        for d in range(1, 4):
            spread(1, d).start()

    def forward(t, j):
        slot = (core + CORES * t) * CORES + j
        return remote(btile.at[slot], btile.at[slot], b3_send.at[t, j], b3_recv.at[t, j], row, partner)

    for j in range(CORES):
        for t in range(2):
            slot = (core + CORES * t) * CORES + j

            @pl.when(row != chip * CORES + j)
            def _():
                remote(bsend, btile.at[slot], b1_send, b2_recv.at[t, j], row, partner).wait_recv()

            forward(t, j).start()
    for j in range(CORES):
        for t in range(2):
            slot = (1 - core + CORES * t) * CORES + j
            remote(bsend, btile.at[slot], b1_send, b3_recv.at[t, j], row, partner).wait_recv()

    for s in range(2 * CORES):
        for j in range(CORES):
            for h in range(heads):
                b = btile[s * CORES + j, h].astype(F32)
                bias[h, s * width:(s + 1) * width, j * width:(j + 1) * width] = (b + masks[s]) * LOG2E

    a_s, k_s, v_s, q_s, g_s, sc = (a0, a1), (k0, k1), (v0, v1), (q0, q1), (g0, g1), (s0, s1, s2, s3)
    scale = hd ** -0.5 * LOG2E

    def scores(slot, h):
        part = q_s[slot][h * hd:(h + 1) * hd, :]
        none = jnp.zeros_like(part)
        rhs = jnp.concatenate([part if i == h else none for i in range(heads)], axis=0)
        sc[h][...] = jnp.dot(k_s[slot][...], rhs, preferred_element_type=F32) + bias[h]

    def finish(r):
        for at, dst, i in ((mine_at, out_ref, core * rows + r), (theirs_at, outv, r)):
            upd = lax.dot_general(go[:, at], wo_ref[...], TN, preferred_element_type=F32)
            dst[i] = (zbuf[r, at].astype(F32) + upd).astype(BF16)

    def out_copy(g):
        return remote(outv.at[pl.ds(g * OUT_ROWS, OUT_ROWS)], out_ref.at[pl.ds(core * rows + g * OUT_ROWS, OUT_ROWS)],
                      o_send.at[g], o_recv.at[g], row, partner)

    def step(i, carry):
        @pl.when(i < steps - 1)
        def _():
            z_wait(i + 1)

        lead = OUT_ROWS // 2 + 1

        @pl.when(jnp.logical_and(i >= lead, lax.rem(i - lead + OUT_ROWS, OUT_ROWS // 2) == 0))
        def _():
            out_copy((i - lead) // (OUT_ROWS // 2)).start()

        for r in range(2):
            cur, nxt = r, 1 - r
            finish(jnp.maximum(2 * i + r - 1, 0))
            a_s[cur][...] = layer_norm(zbuf[jnp.minimum(2 * i + r + 2, rows - 1)], gamma_ref[...], beta_ref[...])
            a = a_s[nxt]
            for h in range(heads):
                if h < 2:
                    scores(cur, h + 2)
                else:
                    scores(nxt, h - 2)
                if h == 0:
                    k_s[nxt][...] = jnp.dot(a[...], wk_ref[...], preferred_element_type=F32).astype(BF16)
                    t = lax.dot_general(wt_ref[proj:2 * proj], a[:n_q], NT, preferred_element_type=F32)
                    q_s[nxt][...] = (t * scale).astype(BF16)
                if h == 1:
                    t = lax.dot_general(wt_ref[2 * proj:], a[:n_q], NT, preferred_element_type=F32)
                    g_s[nxt][...] = jax.nn.sigmoid(t)
                if h == 2:
                    t = lax.dot_general(wt_ref[:proj], a[...], NT, preferred_element_type=F32)
                    v_s[nxt][...] = t.astype(BF16)
                s = sc[h][...]
                p = jnp.exp2(s - over_keys(s, jnp.max))
                total = over_keys(p, jnp.sum)
                at = slice(h * hd, (h + 1) * hd)
                o = jnp.dot(v_s[cur][at, :], p.astype(BF16), preferred_element_type=F32)
                go[at, :] = (g_s[cur][at, :] * (o / total)).astype(BF16)
        return carry

    pltpu.make_async_copy(z_hbm.at[pl.ds(0, rows)], zbuf.at[:, mine_at, :], local_sem.at[1]).wait()
    to_partner_wait = remote(z_hbm.at[pl.ds(0, rows)], zbuf.at[:, theirs_at, :], zp_send, zp_recv, row, partner)
    to_partner_wait.wait_recv()
    lax.fori_loop(-1, steps, step, 0)
    finish(rows - 1)
    to_partner.wait_send()

    def sent(g, carry):
        for k in range(CORES):
            z_send(g, k).wait_send()
        return carry

    lax.fori_loop(0, steps, sent, 0)
    groups = rows // OUT_ROWS
    out_copy(groups - 1).start()

    @pl.when(jnp.logical_not(home))
    def _():
        cross.wait_send()

    @pl.when(home)
    def _():
        for t in range(2):
            for d in range(1, 4):
                spread(t, d).wait_send()

    for j in range(CORES):
        for t in range(2):
            forward(t, j).wait_send()

    def drained(g, carry):
        out_copy(g).wait_send()
        remote(outv.at[pl.ds(0, OUT_ROWS)], out_ref.at[pl.ds((1 - core) * rows + g * OUT_ROWS, OUT_ROWS)],
               o_send.at[g], o_recv.at[g], row, partner).wait_recv()
        return carry

    lax.fori_loop(0, groups, drained, 0)


def solution(mesh):
    tile_spec = P(('dp', 'row'), 'col', None)

    def per_device(pair_tile, res_mask, ln_gamma, ln_beta, w_q, w_k, w_v, w_b, w_g, w_o):
        row_len, width, chan = pair_tile.shape
        heads, proj = w_b.shape[1], w_q.shape[1]
        hd = proj // heads
        rows, n_q = row_len // CORES, CORES * width
        n_k = mesh.shape['col'] * width
        steps, groups = rows // SEND_ROWS, rows // OUT_ROWS
        vmem = pltpu.VMEM
        dma = pltpu.SemaphoreType.DMA
        pairs = lambda *s: [vmem(*s)] * 2
        whole = pl.BlockSpec(memory_space=pltpu.VMEM)
        hbm = pl.BlockSpec(memory_space=pltpu.HBM)
        smalls = (res_mask.reshape(1, -1), ln_gamma.reshape(1, -1), ln_beta.reshape(1, -1), w_q, w_k, w_v, w_b.T, w_g, w_o)
        return pl.pallas_call(
            functools.partial(kernel, heads),
            in_specs=[hbm] * (1 + len(smalls)),
            out_specs=whole,
            out_shape=pltpu.VMEM(pair_tile.shape, BF16),
            scratch_shapes=[
                *[vmem(w.shape, w.dtype) for w in smalls], vmem((3 * proj, chan), BF16),
                vmem((rows, n_k, chan), BF16), vmem((row_len, width, chan), BF16), vmem((rows, width, chan), BF16),
                vmem((heads, n_k, n_q), F32), vmem((8, heads, width, width), BF16), vmem((heads, width, width), BF16),
                vmem((heads, width, width), F32),
                *pairs((n_k, chan), BF16), *pairs((n_k, proj), BF16), *pairs((proj, n_k), BF16),
                *pairs((proj, n_q), BF16), *pairs((proj, n_q), F32),
                *[vmem((n_k, n_q), F32)] * 4, vmem((proj, n_q), BF16),
                dma((len(smalls),)), dma((2,)), dma, dma, dma((CORES, steps)), dma((CORES, steps)), dma, dma, dma((2, 3)), dma((2, CORES)),
                dma((2, CORES)), dma((2, CORES)), dma((groups,)), dma((groups,)),
            ],
            compiler_params=pltpu.CompilerParams(collective_id=0, has_side_effects=True, vmem_limit_bytes=58_000_000),
        )(pair_tile, *smalls)

    return jax.shard_map(per_device, mesh=mesh, in_specs=(tile_spec, P('dp'), P(), P(), P(), P(), P(), P(), P(), P()), out_specs=tile_spec, check_vma=False)
```

```python
import functools

import jax
import jax.numpy as jnp
from jax import lax
from jax.experimental import pallas as pl
from jax.experimental.pallas import tpu as pltpu
from jax.sharding import PartitionSpec as P

LN_EPS = 1e-5
F32 = jnp.float32
BF16 = jnp.bfloat16
NT = (((1,), (1,)), ((), ()))
TN = (((0,), (0,)), ((), ()))
LOG2E = 1.4426950408889634
CORES = 2
STEP_ROWS = 2
LAST_ROWS = 10
SMALLS = 9
EARLY = 10


def layer_norm(z, gamma, beta):
    x = z.astype(F32)
    centered = x - jnp.mean(x, axis=-1, keepdims=True)
    var = jnp.mean(jnp.square(centered), axis=-1, keepdims=True)
    return (centered * lax.rsqrt(var + LN_EPS) * gamma + beta).astype(BF16)


def over_keys(x, op):
    n, width = x.shape
    groups = 8
    t = op(x.reshape(groups, n // 8 // groups, 8, width), axis=1)
    return op(op(t, axis=0), axis=0, keepdims=True)


def kernel(heads, z_hbm, *refs):
    body(heads, z_hbm, refs[:SMALLS], refs[SMALLS + 1:2 * SMALLS + 1], refs[SMALLS], *refs[2 * SMALLS + 1:])


def body(heads, z_hbm, small_hbm, small_refs, out_ref,
           wt_ref, zbuf, own, outv, bias, btile, bsend, relay, brow, a0, a1, k0, k1, v0, v1, q0, q1, g0, g1,
           s0, s1, s2, s3, go,
           small_sem, local_sem, zp_send, zp_recv, zs_send, zs_recv, b1_send, b1_recv, b2_send, b2_recv,
           b3_send, b3_recv, o_send, o_recv):
    mask_ref, gamma_ref, beta_ref, wq_ref, wk_ref, wv_ref, wbt_ref, wg_ref, wo_ref = small_refs
    rows_all, width, chan = z_hbm.shape
    rows = rows_all // CORES
    n_q = CORES * width
    proj = wk_ref.shape[1]
    hd = proj // heads
    steps = (rows - LAST_ROWS) // STEP_ROWS
    dp, row, col = lax.axis_index('dp'), lax.axis_index('row'), lax.axis_index('col')
    n_row = lax.axis_size('row')
    core, chip = lax.rem(col, CORES), col // CORES
    partner = chip * CORES + 1 - core
    far = (1 - chip) * CORES
    home_chip = row // CORES
    jslot = lax.rem(row, CORES)
    home = chip == home_chip

    def remote(src, dst, send, recv, r, c):
        return pltpu.make_async_remote_copy(src, dst, send, recv, device_id=(dp, r, c),
                                            device_id_type=pl.DeviceIdType.MESH)

    barrier = pltpu.get_barrier_semaphore()
    peers = [(row, partner), (row, far), (row, far + 1)]
    peers += [(lax.rem(row + d, n_row), col) for d in range(1, 4)]
    for r, c in peers:
        pl.semaphore_signal(barrier, inc=1, device_id=(dp, r, c), device_id_type=pl.DeviceIdType.MESH)

    own_copy = pltpu.make_async_copy(z_hbm, own, local_sem.at[0])
    own_copy.start()
    mine_at = pl.ds(pl.multiple_of(core * width, width), width)
    theirs_at = pl.ds(pl.multiple_of((1 - core) * width, width), width)
    far_at = pl.ds(pl.multiple_of((CORES + core) * width, width), width)
    z_copy = pltpu.make_async_copy(z_hbm.at[pl.ds(core * rows, rows)], zbuf.at[:, mine_at, :], local_sem.at[1])
    z_copy.start()
    pl.semaphore_wait(barrier, len(peers))

    to_partner = remote(z_hbm.at[pl.ds((1 - core) * rows, rows)], zbuf.at[:, mine_at, :], zp_send, zp_recv, row, partner)

    def z_send(r, k):
        return remote(z_hbm.at[k * rows + r], zbuf.at[r, far_at, :], zs_send.at[k, r], zs_recv.at[core, r], row, far + k)

    def z_wait(r):
        for k in range(CORES):
            at = pl.ds((CORES + k) * width, width)
            remote(z_hbm.at[0], zbuf.at[r, at, :], zs_send.at[k, r], zs_recv.at[k, r], row, far + k).wait_recv()

    def send_row(r, carry):
        for k in range(CORES):
            z_send(r, k).start()
        return carry

    lax.fori_loop(0, EARLY, send_row, 0)
    to_partner.start()
    small_copies = [pltpu.make_async_copy(src, dst, small_sem.at[i]) for i, (src, dst) in enumerate(zip(small_hbm, small_refs))]
    for c in small_copies:
        c.start()
    for c in small_copies:
        c.wait()
    for i, w in enumerate((wv_ref, wq_ref, wg_ref)):
        wt_ref[i * proj:(i + 1) * proj] = w[...].T

    own_copy.wait()
    batch = 8

    def bias_step(i, carry):
        a = layer_norm(own[pl.ds(i * batch, batch)].reshape(batch * width, chan), gamma_ref[...], beta_ref[...])
        t = lax.dot_general(wbt_ref[...], a, NT, preferred_element_type=F32)
        for j in range(batch):
            for h in range(heads):
                brow[h, pl.ds(i * batch + j, 1), :] = t[h:h + 1, j * width:(j + 1) * width]
        return carry

    lax.fori_loop(0, rows_all // batch, bias_step, 0)
    home_slot = core * CORES + jslot
    for h in range(heads):
        tile = brow[h].T.astype(BF16)
        bsend[h] = tile

        @pl.when(home)
        def _():
            btile[home_slot, h] = tile

    masks = []
    for s in range(2 * CORES):
        block = chip * CORES + s if s < CORES else far + s - CORES
        m = mask_ref[:, pl.ds(pl.multiple_of(block * width, width), width)]
        masks.append(jnp.broadcast_to(jnp.where(m > 0, 0.0, -1e9).astype(F32), (width, width)).T)

    paired = lax.rem(row + CORES, n_row)
    hand = remote(bsend, relay, b1_send.at[0], b1_recv.at[0], paired, col)
    cross_slot = (CORES + core) * CORES + jslot
    cross = remote(relay, btile.at[cross_slot], b1_send.at[1], b1_recv.at[1], row, far + core)

    def spread(src, slot, t, d):
        return remote(src, btile.at[slot], b2_send.at[d - 1], b2_recv.at[t, jslot], lax.rem(row + d, n_row), col)

    @pl.when(home)
    def _():
        for d in range(1, 4):
            spread(bsend, home_slot, 0, d).start()

    @pl.when(jnp.logical_not(home))
    def _():
        hand.start()

    @pl.when(home)
    def _():
        hand.wait_recv()
        cross.start()

    lax.fori_loop(EARLY, rows, send_row, 0)

    @pl.when(jnp.logical_not(home))
    def _():
        cross.wait_recv()
        for d in range(1, 4):
            spread(btile.at[cross_slot], cross_slot, 1, d).start()

    def forward(t, j):
        slot = (core + CORES * t) * CORES + j
        return remote(btile.at[slot], btile.at[slot], b3_send.at[t, j], b3_recv.at[t, j], row, partner)

    for t in range(2):
        for j in range(CORES):
            slot = (core + CORES * t) * CORES + j
            source = chip * CORES + j if t == 0 else far + j

            @pl.when(row != source)
            def _():
                remote(bsend, btile.at[slot], b1_send.at[0], b2_recv.at[t, j], row, partner).wait_recv()

            forward(t, j).start()
    for j in range(CORES):
        for t in range(2):
            slot = (1 - core + CORES * t) * CORES + j
            remote(bsend, btile.at[slot], b1_send.at[0], b3_recv.at[t, j], row, partner).wait_recv()

    for s in range(2 * CORES):
        for j in range(CORES):
            for h in range(heads):
                b = btile[s * CORES + j, h].astype(F32)
                bias[h, s * width:(s + 1) * width, j * width:(j + 1) * width] = (b + masks[s]) * LOG2E

    a_s, k_s, v_s, q_s, g_s, sc = (a0, a1), (k0, k1), (v0, v1), (q0, q1), (g0, g1), (s0, s1, s2, s3)
    scale = hd ** -0.5 * LOG2E

    def scores(slot, h):
        part = q_s[slot][h * hd:(h + 1) * hd, :]
        none = jnp.zeros_like(part)
        rhs = jnp.concatenate([part if i == h else none for i in range(heads)], axis=0)
        sc[h][...] = jnp.dot(k_s[slot][...], rhs, preferred_element_type=F32) + bias[h]

    def finish(r):
        for at, dst, i in ((mine_at, out_ref, core * rows + r), (theirs_at, outv, r)):
            upd = lax.dot_general(go[:, at], wo_ref[...], TN, preferred_element_type=F32)
            dst[i] = (zbuf[r, at].astype(F32) + upd).astype(BF16)

    def out_copy(g):
        return remote(outv.at[pl.ds(g * STEP_ROWS, STEP_ROWS)], out_ref.at[pl.ds(core * rows + g * STEP_ROWS, STEP_ROWS)],
                      o_send.at[g], o_recv.at[g], row, partner)

    def project(h, slot):
        a = a_s[slot]
        if h == 0:
            k_s[slot][...] = jnp.dot(a[...], wk_ref[...], preferred_element_type=F32).astype(BF16)
            t = lax.dot_general(wt_ref[proj:2 * proj], a[:n_q], NT, preferred_element_type=F32)
            q_s[slot][...] = (t * scale).astype(BF16)
        if h == 1:
            t = lax.dot_general(wt_ref[2 * proj:], a[:n_q], NT, preferred_element_type=F32)
            g_s[slot][...] = jax.nn.sigmoid(t)
        if h == 2:
            t = lax.dot_general(wt_ref[:proj], a[...], NT, preferred_element_type=F32)
            v_s[slot][...] = t.astype(BF16)

    def attend(h, slot):
        s = sc[h][...]
        p = jnp.exp2(s - over_keys(s, jnp.max))
        total = over_keys(p, jnp.sum)
        at = slice(h * hd, (h + 1) * hd)
        o = jnp.dot(v_s[slot][at, :], p.astype(BF16), preferred_element_type=F32)
        go[at, :] = (g_s[slot][at, :] * (o / total)).astype(BF16)

    def step(i, carry):
        @pl.when(i < steps)
        def _():
            for r in range(STEP_ROWS):
                z_wait(i * STEP_ROWS + r)

        @pl.when(i > 2)
        def _():
            out_copy(jnp.maximum(i, 3) - 3).start()

        for r in range(STEP_ROWS):
            cur, nxt = r, 1 - r
            finish(jnp.maximum(2 * i + r, 3) - 3)
            ahead = jnp.minimum(2 * i + r, steps * STEP_ROWS - 1)
            a_s[cur][...] = layer_norm(zbuf[ahead], gamma_ref[...], beta_ref[...])
            for h in range(heads):
                if h < 2:
                    scores(cur, h + 2)
                else:
                    scores(nxt, h - 2)
                project(h, nxt)
                attend(h, cur)
        return carry

    def last_row(r, carry):
        z_wait(r)

        @pl.when(lax.rem(r, STEP_ROWS) == 0)
        def _():
            out_copy(r // STEP_ROWS - 1).start()

        a_s[0][...] = layer_norm(zbuf[r], gamma_ref[...], beta_ref[...])
        project(0, 0)
        scores(0, 0)
        project(2, 0)
        scores(0, 1)
        project(1, 0)
        for h in range(heads):
            if h + 2 < heads:
                scores(0, h + 2)
            attend(h, 0)
        finish(r)
        return carry

    z_copy.wait()
    remote(z_hbm.at[pl.ds(0, rows)], zbuf.at[:, theirs_at, :], zp_send, zp_recv, row, partner).wait_recv()
    lax.fori_loop(0, steps + 1, step, 0)
    finish(steps * STEP_ROWS - 1)
    out_copy(steps - 2).start()
    lax.fori_loop(steps * STEP_ROWS, rows, last_row, 0)
    groups = rows // STEP_ROWS
    to_partner.wait_send()

    def sent(r, carry):
        for k in range(CORES):
            z_send(r, k).wait_send()
        return carry

    lax.fori_loop(0, rows, sent, 0)
    out_copy(groups - 1).start()

    @pl.when(jnp.logical_not(home))
    def _():
        hand.wait_send()
        for d in range(1, 4):
            spread(btile.at[cross_slot], cross_slot, 1, d).wait_send()

    @pl.when(home)
    def _():
        cross.wait_send()
        for d in range(1, 4):
            spread(bsend, home_slot, 0, d).wait_send()

    for j in range(CORES):
        for t in range(2):
            forward(t, j).wait_send()

    def drained(g, carry):
        out_copy(g).wait_send()
        remote(outv.at[pl.ds(0, STEP_ROWS)], out_ref.at[pl.ds((1 - core) * rows + g * STEP_ROWS, STEP_ROWS)],
               o_send.at[g], o_recv.at[g], row, partner).wait_recv()
        return carry

    lax.fori_loop(0, groups, drained, 0)


def solution(mesh):
    tile_spec = P(('dp', 'row'), 'col', None)

    def per_device(pair_tile, res_mask, ln_gamma, ln_beta, w_q, w_k, w_v, w_b, w_g, w_o):
        row_len, width, chan = pair_tile.shape
        heads, proj = w_b.shape[1], w_q.shape[1]
        hd = proj // heads
        rows, n_q = row_len // CORES, CORES * width
        n_k = mesh.shape['col'] * width
        groups = rows // STEP_ROWS
        vmem = pltpu.VMEM
        dma = pltpu.SemaphoreType.DMA
        pairs = lambda *s: [vmem(*s)] * 2
        whole = pl.BlockSpec(memory_space=pltpu.VMEM)
        hbm = pl.BlockSpec(memory_space=pltpu.HBM)
        smalls = (res_mask.reshape(1, -1), ln_gamma.reshape(1, -1), ln_beta.reshape(1, -1), w_q, w_k, w_v, w_b.T, w_g, w_o)
        return pl.pallas_call(
            functools.partial(kernel, heads),
            in_specs=[hbm] * (1 + len(smalls)),
            out_specs=whole,
            out_shape=pltpu.VMEM(pair_tile.shape, BF16),
            scratch_shapes=[
                *[vmem(w.shape, w.dtype) for w in smalls], vmem((3 * proj, chan), BF16),
                vmem((rows, n_k, chan), BF16), vmem((row_len, width, chan), BF16), vmem((rows, width, chan), BF16),
                vmem((heads, n_k, n_q), F32), vmem((8, heads, width, width), BF16), *pairs((heads, width, width), BF16),
                vmem((heads, width, width), F32),
                *pairs((n_k, chan), BF16), *pairs((n_k, proj), BF16), *pairs((proj, n_k), BF16),
                *pairs((proj, n_q), BF16), *pairs((proj, n_q), F32),
                *[vmem((n_k, n_q), F32)] * 4, vmem((proj, n_q), BF16),
                dma((len(smalls),)), dma((2,)), dma, dma, dma((CORES, rows)), dma((CORES, rows)), dma((2,)), dma((2,)), dma((3,)), dma((2, CORES)),
                dma((2, CORES)), dma((2, CORES)), dma((groups,)), dma((groups,)),
            ],
            compiler_params=pltpu.CompilerParams(collective_id=0, has_side_effects=True, vmem_limit_bytes=58_000_000),
        )(pair_tile, *smalls)

    return jax.shard_map(per_device, mesh=mesh, in_specs=(tile_spec, P('dp'), P(), P(), P(), P(), P(), P(), P(), P()), out_specs=tile_spec, check_vma=False)
```

```python
import functools

import jax
import jax.numpy as jnp
from jax import lax
from jax.experimental import pallas as pl
from jax.experimental.pallas import tpu as pltpu
from jax.sharding import PartitionSpec as P

LN_EPS = 1e-5
F32 = jnp.float32
BF16 = jnp.bfloat16
NT = (((1,), (1,)), ((), ()))
TN = (((0,), (0,)), ((), ()))
LOG2E = 1.4426950408889634
CORES = 2
STEP_ROWS = 2
LAST_ROWS = 4
SMALLS = 9
EARLY = 7


def layer_norm(z, gamma, beta):
    x = z.astype(F32)
    centered = x - jnp.mean(x, axis=-1, keepdims=True)
    var = jnp.mean(jnp.square(centered), axis=-1, keepdims=True)
    return (centered * lax.rsqrt(var + LN_EPS) * gamma + beta).astype(BF16)


def over_keys(x, op):
    n, width = x.shape
    groups = 8
    t = op(x.reshape(groups, n // 8 // groups, 8, width), axis=1)
    return op(op(t, axis=0), axis=0, keepdims=True)


def kernel(heads, z_hbm, *refs):
    body(heads, z_hbm, refs[:SMALLS], refs[SMALLS + 1:2 * SMALLS + 1], refs[SMALLS], *refs[2 * SMALLS + 1:])


def body(heads, z_hbm, small_hbm, small_refs, out_ref,
           wt_ref, zbuf, own, outv, bias, btile, bsend, relay, brow, a0, a1, k0, k1, v0, v1, q0, q1, g0, g1,
           s0, s1, s2, s3, s4, s5, s6, s7, go0, go1,
           small_sem, local_sem, zp_send, zp_recv, zs_send, zs_recv, b1_send, b1_recv, b2_send, b2_recv,
           b3_send, b3_recv, o_send, o_recv):
    mask_ref, gamma_ref, beta_ref, wq_ref, wk_ref, wv_ref, wbt_ref, wg_ref, wo_ref = small_refs
    rows_all, width, chan = z_hbm.shape
    rows = rows_all // CORES
    n_q = CORES * width
    proj = wk_ref.shape[1]
    hd = proj // heads
    groups = rows // STEP_ROWS
    steps = (rows - LAST_ROWS) // STEP_ROWS
    dp, row, col = lax.axis_index('dp'), lax.axis_index('row'), lax.axis_index('col')
    n_row = lax.axis_size('row')
    core, chip = lax.rem(col, CORES), col // CORES
    partner = chip * CORES + 1 - core
    far = (1 - chip) * CORES
    home_chip = row // CORES
    jslot = lax.rem(row, CORES)
    home = chip == home_chip

    def remote(src, dst, send, recv, r, c):
        return pltpu.make_async_remote_copy(src, dst, send, recv, device_id=(dp, r, c),
                                            device_id_type=pl.DeviceIdType.MESH)

    barrier = pltpu.get_barrier_semaphore()
    peers = [(row, partner), (row, far), (row, far + 1)]
    peers += [(lax.rem(row + d, n_row), col) for d in range(1, 4)]
    for r, c in peers:
        pl.semaphore_signal(barrier, inc=1, device_id=(dp, r, c), device_id_type=pl.DeviceIdType.MESH)

    own_copy = pltpu.make_async_copy(z_hbm, own, local_sem.at[0])
    own_copy.start()
    mine_at = pl.ds(pl.multiple_of(core * width, width), width)
    theirs_at = pl.ds(pl.multiple_of((1 - core) * width, width), width)
    far_at = pl.ds(pl.multiple_of((CORES + core) * width, width), width)
    z_copy = pltpu.make_async_copy(z_hbm.at[pl.ds(core * rows, rows)], zbuf.at[:, mine_at, :], local_sem.at[1])
    z_copy.start()
    pl.semaphore_wait(barrier, len(peers))

    to_partner = remote(z_hbm.at[pl.ds((1 - core) * rows, rows)], zbuf.at[:, mine_at, :], zp_send, zp_recv, row, partner)

    def z_send(g, k):
        return remote(z_hbm.at[pl.ds(k * rows + g * STEP_ROWS, STEP_ROWS)],
                      zbuf.at[pl.ds(g * STEP_ROWS, STEP_ROWS), far_at, :],
                      zs_send.at[k, g], zs_recv.at[core, g], row, far + k)

    def z_wait(g):
        for k in range(CORES):
            at = pl.ds((CORES + k) * width, width)
            remote(z_hbm.at[pl.ds(0, STEP_ROWS)], zbuf.at[pl.ds(g * STEP_ROWS, STEP_ROWS), at, :],
                   zs_send.at[k, g], zs_recv.at[k, g], row, far + k).wait_recv()

    def send_step(g, carry):
        for k in range(CORES):
            z_send(g, k).start()
        return carry

    lax.fori_loop(0, EARLY, send_step, 0)
    to_partner.start()
    small_copies = [pltpu.make_async_copy(src, dst, small_sem.at[i]) for i, (src, dst) in enumerate(zip(small_hbm, small_refs))]
    for c in small_copies:
        c.start()
    for c in small_copies:
        c.wait()
    for i, w in enumerate((wv_ref, wq_ref, wg_ref)):
        wt_ref[i * proj:(i + 1) * proj] = w[...].T

    own_copy.wait()
    batch = 8

    def bias_step(i, carry):
        a = layer_norm(own[pl.ds(i * batch, batch)].reshape(batch * width, chan), gamma_ref[...], beta_ref[...])
        t = lax.dot_general(wbt_ref[...], a, NT, preferred_element_type=F32)
        for j in range(batch):
            for h in range(heads):
                brow[h, pl.ds(i * batch + j, 1), :] = t[h:h + 1, j * width:(j + 1) * width]
        return carry

    lax.fori_loop(0, rows_all // batch, bias_step, 0)
    home_slot = core * CORES + jslot
    for h in range(heads):
        tile = brow[h].T.astype(BF16)
        bsend[h] = tile

        @pl.when(home)
        def _():
            btile[home_slot, h] = tile

    masks = []
    for s in range(2 * CORES):
        block = chip * CORES + s if s < CORES else far + s - CORES
        m = mask_ref[:, pl.ds(pl.multiple_of(block * width, width), width)]
        masks.append(jnp.broadcast_to(jnp.where(m > 0, 0.0, -1e9).astype(F32), (width, width)).T)

    paired = lax.rem(row + CORES, n_row)
    hand = remote(bsend, relay, b1_send.at[0], b1_recv.at[0], paired, col)
    cross_slot = (CORES + core) * CORES + jslot
    cross = remote(relay, btile.at[cross_slot], b1_send.at[1], b1_recv.at[1], row, far + core)

    def spread(src, slot, t, d):
        return remote(src, btile.at[slot], b2_send.at[d - 1], b2_recv.at[t, jslot], lax.rem(row + d, n_row), col)

    @pl.when(home)
    def _():
        for d in range(1, 4):
            spread(bsend, home_slot, 0, d).start()

    @pl.when(jnp.logical_not(home))
    def _():
        hand.start()

    @pl.when(home)
    def _():
        hand.wait_recv()
        cross.start()

    lax.fori_loop(EARLY, groups, send_step, 0)

    @pl.when(jnp.logical_not(home))
    def _():
        cross.wait_recv()
        for d in range(1, 4):
            spread(btile.at[cross_slot], cross_slot, 1, d).start()

    def forward(t, j):
        slot = (core + CORES * t) * CORES + j
        return remote(btile.at[slot], btile.at[slot], b3_send.at[t, j], b3_recv.at[t, j], row, partner)

    for t in range(2):
        for j in range(CORES):
            slot = (core + CORES * t) * CORES + j
            source = chip * CORES + j if t == 0 else far + j

            @pl.when(row != source)
            def _():
                remote(bsend, btile.at[slot], b1_send.at[0], b2_recv.at[t, j], row, partner).wait_recv()

            forward(t, j).start()
    for j in range(CORES):
        for t in range(2):
            slot = (1 - core + CORES * t) * CORES + j
            remote(bsend, btile.at[slot], b1_send.at[0], b3_recv.at[t, j], row, partner).wait_recv()

    for s in range(2 * CORES):
        for j in range(CORES):
            for h in range(heads):
                b = btile[s * CORES + j, h].astype(F32)
                bias[h, s * width:(s + 1) * width, j * width:(j + 1) * width] = (b + masks[s]) * LOG2E

    a_s, k_s, v_s, q_s, g_s = (a0, a1), (k0, k1), (v0, v1), (q0, q1), (g0, g1)
    sc, go = ((s0, s1, s2, s3), (s4, s5, s6, s7)), (go0, go1)
    scale = hd ** -0.5 * LOG2E

    every, near, distant = slice(0, 2 * n_q), slice(0, n_q), slice(n_q, 2 * n_q)

    def scores(slot, h, dst, keys=every):
        part = q_s[slot][h * hd:(h + 1) * hd, :]
        none = jnp.zeros_like(part)
        rhs = jnp.concatenate([part if i == h else none for i in range(heads)], axis=0)
        dst[h][keys, :] = jnp.dot(k_s[slot][keys, :], rhs, preferred_element_type=F32) + bias[h, keys, :]

    def finish(r, src):
        for at, dst, i in ((mine_at, out_ref, core * rows + r), (theirs_at, outv, r)):
            upd = lax.dot_general(src[:, at], wo_ref[...], TN, preferred_element_type=F32)
            dst[i] = (zbuf[r, at].astype(F32) + upd).astype(BF16)

    def out_copy(g):
        return remote(outv.at[pl.ds(g * STEP_ROWS, STEP_ROWS)], out_ref.at[pl.ds(core * rows + g * STEP_ROWS, STEP_ROWS)],
                      o_send.at[g], o_recv.at[g], row, partner)

    def norm(r, slot, keys=every):
        a_s[slot][keys, :] = layer_norm(zbuf[r, keys, :], gamma_ref[...], beta_ref[...])

    def keys_of(slot, keys=every):
        k_s[slot][keys, :] = jnp.dot(a_s[slot][keys, :], wk_ref[...], preferred_element_type=F32).astype(BF16)

    def values_of(slot, keys=every):
        t = lax.dot_general(wt_ref[:proj], a_s[slot][keys, :], NT, preferred_element_type=F32)
        v_s[slot][:, keys] = t.astype(BF16)

    def queries_of(slot):
        t = lax.dot_general(wt_ref[proj:2 * proj], a_s[slot][near, :], NT, preferred_element_type=F32)
        q_s[slot][...] = (t * scale).astype(BF16)

    def gates_of(slot):
        t = lax.dot_general(wt_ref[2 * proj:], a_s[slot][near, :], NT, preferred_element_type=F32)
        g_s[slot][...] = jax.nn.sigmoid(t)

    def attend(h, slot, src, dst):
        s = src[h][...]
        p = jnp.exp2(s - over_keys(s, jnp.max))
        total = over_keys(p, jnp.sum)
        at = slice(h * hd, (h + 1) * hd)
        o = jnp.dot(v_s[slot][at, :], p.astype(BF16), preferred_element_type=F32)
        dst[at, :] = (g_s[slot][at, :] * (o / total)).astype(BF16)

    def step(i, carry):
        @pl.when(i < steps)
        def _():
            z_wait(i)

        @pl.when(i > 2)
        def _():
            out_copy(jnp.maximum(i, 3) - 3).start()

        for r in range(STEP_ROWS):
            cur, nxt = r, 1 - r
            finish(jnp.maximum(2 * i + r, 3) - 3, go[0])
            norm(jnp.minimum(2 * i + r, steps * STEP_ROWS - 1), cur)
            for h in range(heads):
                if h < 2:
                    scores(cur, h + 2, sc[0])
                else:
                    scores(nxt, h - 2, sc[0])
                if h == 0:
                    keys_of(nxt)
                    queries_of(nxt)
                if h == 1:
                    gates_of(nxt)
                if h == 2:
                    values_of(nxt)
                attend(h, cur, sc[0], go[0])
        return carry

    def last_rows(i, carry):
        both = range(STEP_ROWS)
        units = [(r, h) for r in both for h in range(heads)]
        out_copy(i - 1).start()
        for r in both:
            norm(i * STEP_ROWS + r, r, near)
        for r in both:
            keys_of(r, near)
            queries_of(r)
            gates_of(r)
            values_of(r, near)
        for r, h in units:
            scores(r, h, sc[r], near)
        z_wait(i)
        for r in both:
            norm(i * STEP_ROWS + r, r, distant)
        for r in both:
            keys_of(r, distant)
        ahead = 2
        for r, h in units[:ahead]:
            scores(r, h, sc[r], distant)
        for r in both:
            values_of(r, distant)
        for n, (r, h) in enumerate(units):
            for r2, h2 in units[n + ahead:n + ahead + 1]:
                scores(r2, h2, sc[r2], distant)
            attend(h, r, sc[r], go[r])
        for r in both:
            finish(i * STEP_ROWS + r, go[r])
        return carry

    z_copy.wait()
    remote(z_hbm.at[pl.ds(0, rows)], zbuf.at[:, theirs_at, :], zp_send, zp_recv, row, partner).wait_recv()
    lax.fori_loop(0, steps + 1, step, 0)
    finish(steps * STEP_ROWS - 1, go[0])
    out_copy(steps - 2).start()
    lax.fori_loop(steps, groups, last_rows, 0)
    to_partner.wait_send()

    def sent(g, carry):
        for k in range(CORES):
            z_send(g, k).wait_send()
        return carry

    lax.fori_loop(0, groups, sent, 0)
    out_copy(groups - 1).start()

    @pl.when(jnp.logical_not(home))
    def _():
        hand.wait_send()
        for d in range(1, 4):
            spread(btile.at[cross_slot], cross_slot, 1, d).wait_send()

    @pl.when(home)
    def _():
        cross.wait_send()
        for d in range(1, 4):
            spread(bsend, home_slot, 0, d).wait_send()

    for j in range(CORES):
        for t in range(2):
            forward(t, j).wait_send()

    def drained(g, carry):
        out_copy(g).wait_send()
        remote(outv.at[pl.ds(0, STEP_ROWS)], out_ref.at[pl.ds((1 - core) * rows + g * STEP_ROWS, STEP_ROWS)],
               o_send.at[g], o_recv.at[g], row, partner).wait_recv()
        return carry

    lax.fori_loop(0, groups, drained, 0)


def solution(mesh):
    tile_spec = P(('dp', 'row'), 'col', None)

    def per_device(pair_tile, res_mask, ln_gamma, ln_beta, w_q, w_k, w_v, w_b, w_g, w_o):
        row_len, width, chan = pair_tile.shape
        heads, proj = w_b.shape[1], w_q.shape[1]
        hd = proj // heads
        rows, n_q = row_len // CORES, CORES * width
        n_k = mesh.shape['col'] * width
        groups = rows // STEP_ROWS
        vmem = pltpu.VMEM
        dma = pltpu.SemaphoreType.DMA
        pairs = lambda *s: [vmem(*s)] * 2
        whole = pl.BlockSpec(memory_space=pltpu.VMEM)
        hbm = pl.BlockSpec(memory_space=pltpu.HBM)
        smalls = (res_mask.reshape(1, -1), ln_gamma.reshape(1, -1), ln_beta.reshape(1, -1), w_q, w_k, w_v, w_b.T, w_g, w_o)
        return pl.pallas_call(
            functools.partial(kernel, heads),
            in_specs=[hbm] * (1 + len(smalls)),
            out_specs=whole,
            out_shape=pltpu.VMEM(pair_tile.shape, BF16),
            scratch_shapes=[
                *[vmem(w.shape, w.dtype) for w in smalls], vmem((3 * proj, chan), BF16),
                vmem((rows, n_k, chan), BF16), vmem((row_len, width, chan), BF16), vmem((rows, width, chan), BF16),
                vmem((heads, n_k, n_q), F32), vmem((8, heads, width, width), BF16), *pairs((heads, width, width), BF16),
                vmem((heads, width, width), F32),
                *pairs((n_k, chan), BF16), *pairs((n_k, proj), BF16), *pairs((proj, n_k), BF16),
                *pairs((proj, n_q), BF16), *pairs((proj, n_q), F32),
                *[vmem((n_k, n_q), F32)] * 8, *pairs((proj, n_q), BF16),
                dma((len(smalls),)), dma((2,)), dma, dma, dma((CORES, groups)), dma((CORES, groups)), dma((2,)), dma((2,)), dma((3,)), dma((2, CORES)),
                dma((2, CORES)), dma((2, CORES)), dma((groups,)), dma((groups,)),
            ],
            compiler_params=pltpu.CompilerParams(collective_id=0, has_side_effects=True, vmem_limit_bytes=58_000_000),
        )(pair_tile, *smalls)

    return jax.shard_map(per_device, mesh=mesh, in_specs=(tile_spec, P('dp'), P(), P(), P(), P(), P(), P(), P(), P()), out_specs=tile_spec, check_vma=False)
```

```python
import functools

import jax
import jax.numpy as jnp
from jax import lax
from jax.experimental import pallas as pl
from jax.experimental.pallas import tpu as pltpu
from jax.sharding import PartitionSpec as P

LN_EPS = 1e-5
F32 = jnp.float32
BF16 = jnp.bfloat16
NT = (((1,), (1,)), ((), ()))
TN = (((0,), (0,)), ((), ()))
LOG2E = 1.4426950408889634
CORES = 2
STEP_ROWS = 2
LAST_ROWS = 4
SMALLS = 9
LAG = 6
EARLY = 8


def layer_norm(z, gamma, beta):
    x = z.astype(F32)
    centered = x - jnp.mean(x, axis=-1, keepdims=True)
    var = jnp.mean(jnp.square(centered), axis=-1, keepdims=True)
    return (centered * lax.rsqrt(var + LN_EPS) * gamma + beta).astype(BF16)


def over_keys(x, op):
    n, width = x.shape
    groups = 8
    t = op(x.reshape(groups, n // 8 // groups, 8, width), axis=1)
    return op(op(t, axis=0), axis=0, keepdims=True)


def kernel(heads, z_hbm, *refs):
    body(heads, z_hbm, refs[:SMALLS], refs[SMALLS + 1:2 * SMALLS + 1], refs[SMALLS], *refs[2 * SMALLS + 1:])


def body(heads, z_hbm, small_hbm, small_refs, out_ref,
           wt_ref, zbuf, own, outv, bias, btile, bsend, relay, brow, a0, a1, k0, k1, v0, v1, q0, q1, g0, g1,
           s0, s1, s2, s3, s4, s5, s6, s7, go0, go1,
           small_sem, local_sem, zp_send, zp_recv, zs_send, zs_recv, b1_send, b1_recv, b2_send, b2_recv,
           b3_send, b3_recv, o_send, o_recv):
    mask_ref, gamma_ref, beta_ref, wq_ref, wk_ref, wv_ref, wbt_ref, wg_ref, wo_ref = small_refs
    rows_all, width, chan = z_hbm.shape
    rows = rows_all // CORES
    n_q = CORES * width
    proj = wk_ref.shape[1]
    hd = proj // heads
    groups = rows // STEP_ROWS
    steps = (rows - LAST_ROWS) // STEP_ROWS
    dp, row, col = lax.axis_index('dp'), lax.axis_index('row'), lax.axis_index('col')
    n_row = lax.axis_size('row')
    core, chip = lax.rem(col, CORES), col // CORES
    partner = chip * CORES + 1 - core
    far = (1 - chip) * CORES
    home_chip = row // CORES
    jslot = lax.rem(row, CORES)
    home = chip == home_chip

    def remote(src, dst, send, recv, r, c):
        return pltpu.make_async_remote_copy(src, dst, send, recv, device_id=(dp, r, c),
                                            device_id_type=pl.DeviceIdType.MESH)

    barrier = pltpu.get_barrier_semaphore()
    peers = [(row, partner), (row, far), (row, far + 1)]
    peers += [(lax.rem(row + d, n_row), col) for d in range(1, 4)]
    for r, c in peers:
        pl.semaphore_signal(barrier, inc=1, device_id=(dp, r, c), device_id_type=pl.DeviceIdType.MESH)

    own_copy = pltpu.make_async_copy(z_hbm, own, local_sem.at[0])
    own_copy.start()
    mine_at = pl.ds(pl.multiple_of(core * width, width), width)
    theirs_at = pl.ds(pl.multiple_of((1 - core) * width, width), width)
    z_copy = pltpu.make_async_copy(z_hbm.at[pl.ds(core * rows, rows)], zbuf.at[:, mine_at, :], local_sem.at[1])
    z_copy.start()
    pl.semaphore_wait(barrier, len(peers))

    to_partner = remote(z_hbm.at[pl.ds((1 - core) * rows, rows)], zbuf.at[:, mine_at, :], zp_send, zp_recv, row, partner)

    def z_copy_of(r, n, i, k, slot, c):
        at = pl.ds(pl.multiple_of((CORES + slot) * width, width), width)
        return remote(z_hbm.at[pl.ds(k * rows + r, n)], zbuf.at[pl.ds(r, n), at, :], zs_send.at[k, i], zs_recv.at[slot, i],
                      row, far + c)

    def z_send(g, k):
        return z_copy_of(g * STEP_ROWS, STEP_ROWS, g, k, core, k)

    def z_send_last(r, k):
        return z_copy_of(steps * STEP_ROWS + r, 1, steps + r, k, core, k)

    def z_wait(g):
        for k in range(CORES):
            z_copy_of(g * STEP_ROWS, STEP_ROWS, g, k, k, k).wait_recv()

    def z_wait_last(r):
        for k in range(CORES):
            z_copy_of(steps * STEP_ROWS + r, 1, steps + r, k, k, k).wait_recv()

    def send_step(g, carry):
        for k in range(CORES):
            z_send(g, k).start()
        return carry

    lax.fori_loop(0, EARLY, send_step, 0)
    to_partner.start()
    small_copies = [pltpu.make_async_copy(src, dst, small_sem.at[i]) for i, (src, dst) in enumerate(zip(small_hbm, small_refs))]
    for c in small_copies:
        c.start()
    for c in small_copies:
        c.wait()
    for i, w in enumerate((wv_ref, wq_ref, wg_ref)):
        wt_ref[i * proj:(i + 1) * proj] = w[...].T

    own_copy.wait()
    batch = 8

    def bias_step(i, carry):
        a = layer_norm(own[pl.ds(i * batch, batch)].reshape(batch * width, chan), gamma_ref[...], beta_ref[...])
        t = lax.dot_general(wbt_ref[...], a, NT, preferred_element_type=F32)
        for j in range(batch):
            for h in range(heads):
                brow[h, pl.ds(i * batch + j, 1), :] = t[h:h + 1, j * width:(j + 1) * width]
        return carry

    lax.fori_loop(0, rows_all // batch, bias_step, 0)
    home_slot = core * CORES + jslot
    for h in range(heads):
        tile = brow[h].T.astype(BF16)
        bsend[h] = tile

        @pl.when(home)
        def _():
            btile[home_slot, h] = tile

    masks = []
    for s in range(2 * CORES):
        block = chip * CORES + s if s < CORES else far + s - CORES
        m = mask_ref[:, pl.ds(pl.multiple_of(block * width, width), width)]
        masks.append(jnp.broadcast_to(jnp.where(m > 0, 0.0, -1e9).astype(F32), (width, width)).T)

    paired = lax.rem(row + CORES, n_row)
    hand = remote(bsend, relay, b1_send.at[0], b1_recv.at[0], paired, col)
    cross_slot = (CORES + core) * CORES + jslot
    cross = remote(relay, btile.at[cross_slot], b1_send.at[1], b1_recv.at[1], row, far + core)

    direct = remote(bsend, btile.at[cross_slot], b1_send.at[1], b1_recv.at[1], row, far + core)
    detour_out = jnp.logical_or(chip == 1, core == 1)
    detour_in = jnp.logical_or(chip == 0, core == 1)
    away = jnp.logical_not(home)
    lands = jnp.logical_or(jnp.logical_and(detour_in, away), jnp.logical_and(jnp.logical_not(detour_in), home))

    def spread(src, slot, t, d):
        return remote(src, btile.at[slot], b2_send.at[t, d - 1], b2_recv.at[t, jslot], lax.rem(row + d, n_row), col)

    @pl.when(jnp.logical_and(away, detour_out))
    def _():
        hand.start()

    @pl.when(jnp.logical_and(away, jnp.logical_not(detour_out)))
    def _():
        direct.start()

    @pl.when(home)
    def _():
        for d in range(1, 4):
            spread(bsend, home_slot, 0, d).start()

    @pl.when(jnp.logical_and(home, detour_out))
    def _():
        hand.wait_recv()
        cross.start()

    lax.fori_loop(EARLY, steps, send_step, 0)
    for r in range(LAST_ROWS):
        for k in range(CORES):
            z_send_last(r, k).start()

    @pl.when(lands)
    def _():
        cross.wait_recv()
        for d in range(1, 4):
            spread(btile.at[cross_slot], cross_slot, 1, d).start()

    def forward(t, j):
        slot = (core + CORES * t) * CORES + j
        return remote(btile.at[slot], btile.at[slot], b3_send.at[t, j], b3_recv.at[t, j], row, partner)

    for t in range(2):
        for j in range(CORES):
            slot = (core + CORES * t) * CORES + j
            source = chip * CORES + j
            if t == 1:
                source = jnp.where(detour_in, far + j, source)

            @pl.when(row != source)
            def _():
                remote(bsend, btile.at[slot], b1_send.at[0], b2_recv.at[t, j], row, partner).wait_recv()

            forward(t, j).start()
    for j in range(CORES):
        for t in range(2):
            slot = (1 - core + CORES * t) * CORES + j
            remote(bsend, btile.at[slot], b1_send.at[0], b3_recv.at[t, j], row, partner).wait_recv()

    for s in range(2 * CORES):
        for j in range(CORES):
            for h in range(heads):
                b = btile[s * CORES + j, h].astype(F32)
                bias[h, s * width:(s + 1) * width, j * width:(j + 1) * width] = (b + masks[s]) * LOG2E

    a_s, k_s, v_s, q_s, g_s = (a0, a1), (k0, k1), (v0, v1), (q0, q1), (g0, g1)
    sc, go = ((s0, s1, s2, s3), (s4, s5, s6, s7)), (go0, go1)
    scale = hd ** -0.5 * LOG2E

    every, near, distant = slice(0, 2 * n_q), slice(0, n_q), slice(n_q, 2 * n_q)

    def scores(slot, h, dst, keys=every):
        part = q_s[slot][h * hd:(h + 1) * hd, :]
        none = jnp.zeros_like(part)
        rhs = jnp.concatenate([part if i == h else none for i in range(heads)], axis=0)
        dst[h][keys, :] = jnp.dot(k_s[slot][keys, :], rhs, preferred_element_type=F32) + bias[h, keys, :]

    def finish(r, src):
        for at, dst, i in ((mine_at, out_ref, core * rows + r), (theirs_at, outv, r)):
            upd = lax.dot_general(src[:, at], wo_ref[...], TN, preferred_element_type=F32)
            dst[i] = (zbuf[r, at].astype(F32) + upd).astype(BF16)

    def out_copy(g):
        return remote(outv.at[pl.ds(g * STEP_ROWS, STEP_ROWS)], out_ref.at[pl.ds(core * rows + g * STEP_ROWS, STEP_ROWS)],
                      o_send.at[g], o_recv.at[g], row, partner)

    def norm(r, slot, keys=every):
        a_s[slot][keys, :] = layer_norm(zbuf[r, keys, :], gamma_ref[...], beta_ref[...])

    def keys_of(slot, keys=every):
        k_s[slot][keys, :] = jnp.dot(a_s[slot][keys, :], wk_ref[...], preferred_element_type=F32).astype(BF16)

    def values_of(slot, keys=every):
        t = lax.dot_general(wt_ref[:proj], a_s[slot][keys, :], NT, preferred_element_type=F32)
        v_s[slot][:, keys] = t.astype(BF16)

    def queries_of(slot):
        t = lax.dot_general(wt_ref[proj:2 * proj], a_s[slot][near, :], NT, preferred_element_type=F32)
        q_s[slot][...] = (t * scale).astype(BF16)

    def gates_of(slot):
        t = lax.dot_general(wt_ref[2 * proj:], a_s[slot][near, :], NT, preferred_element_type=F32)
        g_s[slot][...] = jax.nn.sigmoid(t)

    def attend(h, slot, src, dst):
        s = src[h][...]
        p = jnp.exp2(s - over_keys(s, jnp.max))
        total = over_keys(p, jnp.sum)
        at = slice(h * hd, (h + 1) * hd)
        o = jnp.dot(v_s[slot][at, :], p.astype(BF16), preferred_element_type=F32)
        dst[at, :] = (g_s[slot][at, :] * (o / total)).astype(BF16)

    def sent(g, carry):
        for k in range(CORES):
            z_send(g, k).wait_send()
        return carry

    def drained(g, carry):
        out_copy(g).wait_send()
        remote(outv.at[pl.ds(0, STEP_ROWS)], out_ref.at[pl.ds((1 - core) * rows + g * STEP_ROWS, STEP_ROWS)],
               o_send.at[g], o_recv.at[g], row, partner).wait_recv()
        return carry

    def step(i, carry):
        @pl.when(i < steps)
        def _():
            z_wait(i)

        @pl.when(i > 2)
        def _():
            out_copy(jnp.maximum(i, 3) - 3).start()

        @pl.when(i >= LAG)
        def _():
            g = jnp.maximum(i, LAG) - LAG
            sent(g, 0)
            drained(g, 0)

        for r in range(STEP_ROWS):
            cur, nxt = r, 1 - r
            finish(jnp.maximum(2 * i + r, 3) - 3, go[0])
            norm(jnp.minimum(2 * i + r, steps * STEP_ROWS - 1), cur)
            for h in range(heads):
                if h < 2:
                    scores(cur, h + 2, sc[0])
                else:
                    scores(nxt, h - 2, sc[0])
                if h == 0:
                    keys_of(nxt)
                    queries_of(nxt)
                if h == 1:
                    gates_of(nxt)
                if h == 2:
                    values_of(nxt)
                attend(h, cur, sc[0], go[0])
        return carry

    def last_rows(i, carry):
        both = range(STEP_ROWS)
        units = [(r, h) for r in both for h in range(heads)]
        out_copy(i - 1).start()
        for r in both:
            norm(i * STEP_ROWS + r, r, near)
        for r in both:
            keys_of(r, near)
            queries_of(r)
            gates_of(r)
            values_of(r, near)
        for r, h in units:
            scores(r, h, sc[r], near)
        for r in both:
            z_wait_last((i - steps) * STEP_ROWS + r)
            norm(i * STEP_ROWS + r, r, distant)
            keys_of(r, distant)
            scores(r, 0, sc[r], distant)
            scores(r, 1, sc[r], distant)
            values_of(r, distant)
            for h in range(heads):
                if h + 2 < heads:
                    scores(r, h + 2, sc[r], distant)
                attend(h, r, sc[r], go[r])
            finish(i * STEP_ROWS + r, go[r])
        return carry

    z_copy.wait()
    remote(z_hbm.at[pl.ds(0, rows)], zbuf.at[:, theirs_at, :], zp_send, zp_recv, row, partner).wait_recv()
    lax.fori_loop(0, steps + 1, step, 0)
    finish(steps * STEP_ROWS - 1, go[0])
    out_copy(steps - 2).start()
    lax.fori_loop(steps, groups, last_rows, 0)
    to_partner.wait_send()
    lax.fori_loop(steps + 1 - LAG, steps, sent, 0)
    for r in range(LAST_ROWS):
        for k in range(CORES):
            z_send_last(r, k).wait_send()
    out_copy(groups - 1).start()

    @pl.when(jnp.logical_and(away, detour_out))
    def _():
        hand.wait_send()

    @pl.when(jnp.logical_or(jnp.logical_and(home, detour_out), jnp.logical_and(away, jnp.logical_not(detour_out))))
    def _():
        cross.wait_send()

    @pl.when(home)
    def _():
        for d in range(1, 4):
            spread(bsend, home_slot, 0, d).wait_send()

    @pl.when(lands)
    def _():
        for d in range(1, 4):
            spread(btile.at[cross_slot], cross_slot, 1, d).wait_send()

    for j in range(CORES):
        for t in range(2):
            forward(t, j).wait_send()

    lax.fori_loop(steps + 1 - LAG, groups, drained, 0)


def solution(mesh):
    tile_spec = P(('dp', 'row'), 'col', None)

    def per_device(pair_tile, res_mask, ln_gamma, ln_beta, w_q, w_k, w_v, w_b, w_g, w_o):
        row_len, width, chan = pair_tile.shape
        heads, proj = w_b.shape[1], w_q.shape[1]
        hd = proj // heads
        rows, n_q = row_len // CORES, CORES * width
        n_k = mesh.shape['col'] * width
        groups = rows // STEP_ROWS
        copies = (rows - LAST_ROWS) // STEP_ROWS + LAST_ROWS
        vmem = pltpu.VMEM
        dma = pltpu.SemaphoreType.DMA
        pairs = lambda *s: [vmem(*s)] * 2
        whole = pl.BlockSpec(memory_space=pltpu.VMEM)
        hbm = pl.BlockSpec(memory_space=pltpu.HBM)
        smalls = (res_mask.reshape(1, -1), ln_gamma.reshape(1, -1), ln_beta.reshape(1, -1), w_q, w_k, w_v, w_b.T, w_g, w_o)
        return pl.pallas_call(
            functools.partial(kernel, heads),
            in_specs=[hbm] * (1 + len(smalls)),
            out_specs=whole,
            out_shape=pltpu.VMEM(pair_tile.shape, BF16),
            scratch_shapes=[
                *[vmem(w.shape, w.dtype) for w in smalls], vmem((3 * proj, chan), BF16),
                vmem((rows, n_k, chan), BF16), vmem((row_len, width, chan), BF16), vmem((rows, width, chan), BF16),
                vmem((heads, n_k, n_q), F32), vmem((8, heads, width, width), BF16), *pairs((heads, width, width), BF16),
                vmem((heads, width, width), F32),
                *pairs((n_k, chan), BF16), *pairs((n_k, proj), BF16), *pairs((proj, n_k), BF16),
                *pairs((proj, n_q), BF16), *pairs((proj, n_q), F32),
                *[vmem((n_k, n_q), F32)] * 8, *pairs((proj, n_q), BF16),
                dma((len(smalls),)), dma((2,)), dma, dma, dma((CORES, copies)), dma((CORES, copies)), dma((2,)), dma((2,)), dma((2, 3)), dma((2, CORES)),
                dma((2, CORES)), dma((2, CORES)), dma((groups,)), dma((groups,)),
            ],
            compiler_params=pltpu.CompilerParams(collective_id=0, has_side_effects=True, vmem_limit_bytes=58_000_000),
        )(pair_tile, *smalls)

    return jax.shard_map(per_device, mesh=mesh, in_specs=(tile_spec, P('dp'), P(), P(), P(), P(), P(), P(), P(), P()), out_specs=tile_spec, check_vma=False)
```

```python
import functools

import jax
import jax.numpy as jnp
from jax import lax
from jax.experimental import pallas as pl
from jax.experimental.pallas import tpu as pltpu
from jax.sharding import PartitionSpec as P

LN_EPS = 1e-5
F32 = jnp.float32
BF16 = jnp.bfloat16
NT = (((1,), (1,)), ((), ()))
TN = (((0,), (0,)), ((), ()))
LOG2E = 1.4426950408889634
CORES = 2
STEP_ROWS = 2
LAST_ROWS = 4
SMALLS = 9
LAG = 6
EARLY = 5


def layer_norm(z, gamma, beta):
    x = z.astype(F32)
    centered = x - jnp.mean(x, axis=-1, keepdims=True)
    var = jnp.mean(jnp.square(centered), axis=-1, keepdims=True)
    return (centered * lax.rsqrt(var + LN_EPS) * gamma + beta).astype(BF16)


def over_keys(x, op):
    n, width = x.shape
    groups = 8
    t = op(x.reshape(groups, n // 8 // groups, 8, width), axis=1)
    return op(op(t, axis=0), axis=0, keepdims=True)


def kernel(heads, z_hbm, *refs):
    body(heads, z_hbm, refs[:SMALLS], refs[SMALLS + 1:2 * SMALLS + 1], refs[SMALLS], *refs[2 * SMALLS + 1:])


def body(heads, z_hbm, small_hbm, small_refs, out_ref,
           wt_ref, zbuf, own, outv, bias, btile, bsend, relay, brow, a0, a1, k0, k1, v0, v1, q0, q1, g0, g1,
           s0, s1, s2, s3, s4, s5, s6, s7, go0, go1,
           small_sem, local_sem, zp_send, zp_recv, zs_send, zs_recv, b1_send, b1_recv, b2_send, b2_recv,
           b3_send, b3_recv, o_send, o_recv):
    mask_ref, gamma_ref, beta_ref, wq_ref, wk_ref, wv_ref, wbt_ref, wg_ref, wo_ref = small_refs
    rows_all, width, chan = z_hbm.shape
    rows = rows_all // CORES
    n_q = CORES * width
    proj = wk_ref.shape[1]
    hd = proj // heads
    groups = rows // STEP_ROWS
    steps = (rows - LAST_ROWS) // STEP_ROWS
    dp, row, col = lax.axis_index('dp'), lax.axis_index('row'), lax.axis_index('col')
    n_row = lax.axis_size('row')
    core, chip = lax.rem(col, CORES), col // CORES
    partner = chip * CORES + 1 - core
    far = (1 - chip) * CORES
    home_chip = row // CORES
    jslot = lax.rem(row, CORES)
    home = chip == home_chip

    def remote(src, dst, send, recv, r, c):
        return pltpu.make_async_remote_copy(src, dst, send, recv, device_id=(dp, r, c),
                                            device_id_type=pl.DeviceIdType.MESH)

    barrier = pltpu.get_barrier_semaphore()
    peers = [(row, partner), (row, far), (row, far + 1)]
    peers += [(lax.rem(row + d, n_row), col) for d in range(1, 4)]
    for r, c in peers:
        pl.semaphore_signal(barrier, inc=1, device_id=(dp, r, c), device_id_type=pl.DeviceIdType.MESH)

    own_copy = pltpu.make_async_copy(z_hbm, own, local_sem.at[0])
    own_copy.start()
    mine_at = pl.ds(pl.multiple_of(core * width, width), width)
    theirs_at = pl.ds(pl.multiple_of((1 - core) * width, width), width)
    z_copy = pltpu.make_async_copy(z_hbm.at[pl.ds(core * rows, rows)], zbuf.at[:, mine_at, :], local_sem.at[1])
    z_copy.start()
    pl.semaphore_wait(barrier, len(peers))

    to_partner = remote(z_hbm.at[pl.ds((1 - core) * rows, rows)], zbuf.at[:, mine_at, :], zp_send, zp_recv, row, partner)

    def z_copy_of(g, k, slot, c):
        at = pl.ds(pl.multiple_of((CORES + slot) * width, width), width)
        return remote(z_hbm.at[pl.ds(k * rows + g * STEP_ROWS, STEP_ROWS)],
                      zbuf.at[pl.ds(g * STEP_ROWS, STEP_ROWS), at, :], zs_send.at[k, g], zs_recv.at[slot, g], row, far + c)

    def z_send(g, k):
        return z_copy_of(g, k, core, k)

    def z_wait(g):
        for k in range(CORES):
            z_copy_of(g, k, k, k).wait_recv()

    def send_step(g, carry):
        for k in range(CORES):
            z_send(g, k).start()
        return carry

    lax.fori_loop(0, EARLY, send_step, 0)
    to_partner.start()
    small_copies = [pltpu.make_async_copy(src, dst, small_sem.at[i]) for i, (src, dst) in enumerate(zip(small_hbm, small_refs))]
    for c in small_copies:
        c.start()
    for c in small_copies:
        c.wait()
    for i, w in enumerate((wv_ref, wq_ref, wg_ref)):
        wt_ref[i * proj:(i + 1) * proj] = w[...].T

    own_copy.wait()
    batch = 16
    mean_of = jnp.full((chan, chan), 1 / chan, BF16)

    def bias_step(i, carry):
        z = own[pl.ds(i * batch, batch)].reshape(batch * width, chan)
        centered = z.astype(F32) - jnp.dot(z, mean_of, preferred_element_type=F32)
        var = jnp.mean(jnp.square(centered), axis=-1, keepdims=True)
        a = (centered * lax.rsqrt(var + LN_EPS) * gamma_ref[...] + beta_ref[...]).astype(BF16)
        t = lax.dot_general(wbt_ref[...], a, NT, preferred_element_type=F32)
        for j in range(batch):
            for h in range(heads):
                brow[h, pl.ds(i * batch + j, 1), :] = t[h:h + 1, j * width:(j + 1) * width]
        return carry

    lax.fori_loop(0, rows_all // batch, bias_step, 0)
    home_slot = core * CORES + jslot
    for h in range(heads):
        tile = brow[h].T.astype(BF16)
        bsend[h] = tile

        @pl.when(home)
        def _():
            btile[home_slot, h] = tile

    masks = []
    for s in range(2 * CORES):
        block = chip * CORES + s if s < CORES else far + s - CORES
        m = mask_ref[:, pl.ds(pl.multiple_of(block * width, width), width)]
        masks.append(jnp.broadcast_to(jnp.where(m > 0, 0.0, -1e9).astype(F32), (width, width)).T)

    paired = lax.rem(row + CORES, n_row)
    hand = remote(bsend, relay, b1_send.at[0], b1_recv.at[0], paired, col)
    cross_slot = (CORES + core) * CORES + jslot
    cross = remote(relay, btile.at[cross_slot], b1_send.at[1], b1_recv.at[1], row, far + core)

    direct = remote(bsend, btile.at[cross_slot], b1_send.at[1], b1_recv.at[1], row, far + core)
    detour_out = jnp.logical_or(chip == 1, core == 1)
    detour_in = jnp.logical_or(chip == 0, core == 1)
    away = jnp.logical_not(home)
    lands = jnp.logical_or(jnp.logical_and(detour_in, away), jnp.logical_and(jnp.logical_not(detour_in), home))

    def spread(src, slot, t, d):
        return remote(src, btile.at[slot], b2_send.at[t, d - 1], b2_recv.at[t, jslot], lax.rem(row + d, n_row), col)

    @pl.when(jnp.logical_and(away, detour_out))
    def _():
        hand.start()

    @pl.when(jnp.logical_and(away, jnp.logical_not(detour_out)))
    def _():
        direct.start()

    @pl.when(home)
    def _():
        for d in range(1, 4):
            spread(bsend, home_slot, 0, d).start()

    @pl.when(jnp.logical_and(home, detour_out))
    def _():
        hand.wait_recv()
        cross.start()

    lax.fori_loop(EARLY, groups, send_step, 0)

    @pl.when(lands)
    def _():
        cross.wait_recv()
        for d in range(1, 4):
            spread(btile.at[cross_slot], cross_slot, 1, d).start()

    def forward(t, j):
        slot = (core + CORES * t) * CORES + j
        return remote(btile.at[slot], btile.at[slot], b3_send.at[t, j], b3_recv.at[t, j], row, partner)

    for t in range(2):
        for j in range(CORES):
            slot = (core + CORES * t) * CORES + j
            source = chip * CORES + j
            if t == 1:
                source = jnp.where(detour_in, far + j, source)

            @pl.when(row != source)
            def _():
                remote(bsend, btile.at[slot], b1_send.at[0], b2_recv.at[t, j], row, partner).wait_recv()

            forward(t, j).start()
    for j in range(CORES):
        for t in range(2):
            slot = (1 - core + CORES * t) * CORES + j
            remote(bsend, btile.at[slot], b1_send.at[0], b3_recv.at[t, j], row, partner).wait_recv()

    for s in range(2 * CORES):
        for j in range(CORES):
            for h in range(heads):
                b = btile[s * CORES + j, h].astype(F32)
                bias[h, s * width:(s + 1) * width, j * width:(j + 1) * width] = (b + masks[s]) * LOG2E

    a_s, k_s, v_s, q_s, g_s = (a0, a1), (k0, k1), (v0, v1), (q0, q1), (g0, g1)
    sc, go = ((s0, s1, s2, s3), (s4, s5, s6, s7)), (go0, go1)
    scale = hd ** -0.5 * LOG2E

    every, near, distant = slice(0, 2 * n_q), slice(0, n_q), slice(n_q, 2 * n_q)

    def scores(slot, h, dst, keys=every):
        part = q_s[slot][h * hd:(h + 1) * hd, :]
        none = jnp.zeros_like(part)
        rhs = jnp.concatenate([part if i == h else none for i in range(heads)], axis=0)
        dst[h][keys, :] = jnp.dot(k_s[slot][keys, :], rhs, preferred_element_type=F32) + bias[h, keys, :]

    def finish(r, src):
        for at, dst, i in ((mine_at, out_ref, core * rows + r), (theirs_at, outv, r)):
            upd = lax.dot_general(src[:, at], wo_ref[...], TN, preferred_element_type=F32)
            dst[i] = (zbuf[r, at].astype(F32) + upd).astype(BF16)

    def out_copy(g):
        return remote(outv.at[pl.ds(g * STEP_ROWS, STEP_ROWS)], out_ref.at[pl.ds(core * rows + g * STEP_ROWS, STEP_ROWS)],
                      o_send.at[g], o_recv.at[g], row, partner)

    def norm(r, slot, keys=every):
        a_s[slot][keys, :] = layer_norm(zbuf[r, keys, :], gamma_ref[...], beta_ref[...])

    def keys_of(slot, keys=every):
        k_s[slot][keys, :] = jnp.dot(a_s[slot][keys, :], wk_ref[...], preferred_element_type=F32).astype(BF16)

    def values_of(slot, keys=every):
        t = lax.dot_general(wt_ref[:proj], a_s[slot][keys, :], NT, preferred_element_type=F32)
        v_s[slot][:, keys] = t.astype(BF16)

    def queries_of(slot):
        t = lax.dot_general(wt_ref[proj:2 * proj], a_s[slot][near, :], NT, preferred_element_type=F32)
        q_s[slot][...] = (t * scale).astype(BF16)

    def gates_of(slot):
        t = lax.dot_general(wt_ref[2 * proj:], a_s[slot][near, :], NT, preferred_element_type=F32)
        g_s[slot][...] = jax.nn.sigmoid(t)

    def attend(h, slot, src, dst):
        s = src[h][...]
        p = jnp.exp2(s - over_keys(s, jnp.max))
        total = over_keys(p, jnp.sum)
        at = slice(h * hd, (h + 1) * hd)
        o = jnp.dot(v_s[slot][at, :], p.astype(BF16), preferred_element_type=F32)
        dst[at, :] = (g_s[slot][at, :] * (o / total)).astype(BF16)

    def sent(g, carry):
        for k in range(CORES):
            z_send(g, k).wait_send()
        return carry

    def drained(g, carry):
        out_copy(g).wait_send()
        remote(outv.at[pl.ds(0, STEP_ROWS)], out_ref.at[pl.ds((1 - core) * rows + g * STEP_ROWS, STEP_ROWS)],
               o_send.at[g], o_recv.at[g], row, partner).wait_recv()
        return carry

    def step(i, carry):
        @pl.when(i < steps)
        def _():
            z_wait(i)

        @pl.when(i > 2)
        def _():
            out_copy(jnp.maximum(i, 3) - 3).start()

        for r in range(STEP_ROWS):
            cur, nxt = r, 1 - r
            finish(jnp.maximum(2 * i + r, 3) - 3, go[0])
            norm(jnp.minimum(2 * i + r, steps * STEP_ROWS - 1), cur)
            for h in range(heads):
                if h < 2:
                    scores(cur, h + 2, sc[0])
                else:
                    scores(nxt, h - 2, sc[0])
                if h == 0:
                    keys_of(nxt)
                    queries_of(nxt)
                if h == 1:
                    gates_of(nxt)
                if h == 2:
                    values_of(nxt)
                attend(h, cur, sc[0], go[0])
        return carry

    def last_rows(i, carry):
        both = range(STEP_ROWS)
        units = [(r, h) for r in both for h in range(heads)]
        out_copy(i - 1).start()
        for r in both:
            norm(i * STEP_ROWS + r, r, near)
        for r in both:
            keys_of(r, near)
            queries_of(r)
            gates_of(r)
            values_of(r, near)
        for r, h in units:
            scores(r, h, sc[r], near)
        z_wait(i)
        for r in both:
            norm(i * STEP_ROWS + r, r, distant)
        for r in both:
            keys_of(r, distant)
        ahead = 2
        for r, h in units[:ahead]:
            scores(r, h, sc[r], distant)
        for r in both:
            values_of(r, distant)
        for n, (r, h) in enumerate(units):
            for r2, h2 in units[n + ahead:n + ahead + 1]:
                scores(r2, h2, sc[r2], distant)
            attend(h, r, sc[r], go[r])
        for r in both:
            finish(i * STEP_ROWS + r, go[r])
        return carry

    z_copy.wait()
    remote(z_hbm.at[pl.ds(0, rows)], zbuf.at[:, theirs_at, :], zp_send, zp_recv, row, partner).wait_recv()
    lax.fori_loop(0, steps + 1, step, 0)
    finish(steps * STEP_ROWS - 1, go[0])
    out_copy(steps - 2).start()
    lax.fori_loop(0, steps + 1 - LAG, sent, 0)
    lax.fori_loop(0, steps + 1 - LAG, drained, 0)
    lax.fori_loop(steps, groups, last_rows, 0)
    to_partner.wait_send()
    lax.fori_loop(steps + 1 - LAG, groups, sent, 0)
    out_copy(groups - 1).start()

    @pl.when(jnp.logical_and(away, detour_out))
    def _():
        hand.wait_send()

    @pl.when(jnp.logical_or(jnp.logical_and(home, detour_out), jnp.logical_and(away, jnp.logical_not(detour_out))))
    def _():
        cross.wait_send()

    @pl.when(home)
    def _():
        for d in range(1, 4):
            spread(bsend, home_slot, 0, d).wait_send()

    @pl.when(lands)
    def _():
        for d in range(1, 4):
            spread(btile.at[cross_slot], cross_slot, 1, d).wait_send()

    for j in range(CORES):
        for t in range(2):
            forward(t, j).wait_send()

    lax.fori_loop(steps + 1 - LAG, groups, drained, 0)


def solution(mesh):
    tile_spec = P(('dp', 'row'), 'col', None)

    def per_device(pair_tile, res_mask, ln_gamma, ln_beta, w_q, w_k, w_v, w_b, w_g, w_o):
        row_len, width, chan = pair_tile.shape
        heads, proj = w_b.shape[1], w_q.shape[1]
        hd = proj // heads
        rows, n_q = row_len // CORES, CORES * width
        n_k = mesh.shape['col'] * width
        groups = rows // STEP_ROWS
        vmem = pltpu.VMEM
        dma = pltpu.SemaphoreType.DMA
        pairs = lambda *s: [vmem(*s)] * 2
        whole = pl.BlockSpec(memory_space=pltpu.VMEM)
        hbm = pl.BlockSpec(memory_space=pltpu.HBM)
        smalls = (res_mask.reshape(1, -1), ln_gamma.reshape(1, -1), ln_beta.reshape(1, -1), w_q, w_k, w_v, w_b.T, w_g, w_o)
        return pl.pallas_call(
            functools.partial(kernel, heads),
            in_specs=[hbm] * (1 + len(smalls)),
            out_specs=whole,
            out_shape=pltpu.VMEM(pair_tile.shape, BF16),
            scratch_shapes=[
                *[vmem(w.shape, w.dtype) for w in smalls], vmem((3 * proj, chan), BF16),
                vmem((rows, n_k, chan), BF16), vmem((row_len, width, chan), BF16), vmem((rows, width, chan), BF16),
                vmem((heads, n_k, n_q), F32), vmem((8, heads, width, width), BF16), *pairs((heads, width, width), BF16),
                vmem((heads, width, width), F32),
                *pairs((n_k, chan), BF16), *pairs((n_k, proj), BF16), *pairs((proj, n_k), BF16),
                *pairs((proj, n_q), BF16), *pairs((proj, n_q), F32),
                *[vmem((n_k, n_q), F32)] * 8, *pairs((proj, n_q), BF16),
                dma((len(smalls),)), dma((2,)), dma, dma, dma((CORES, groups)), dma((CORES, groups)), dma((2,)), dma((2,)), dma((2, 3)), dma((2, CORES)),
                dma((2, CORES)), dma((2, CORES)), dma((groups,)), dma((groups,)),
            ],
            compiler_params=pltpu.CompilerParams(collective_id=0, has_side_effects=True, vmem_limit_bytes=58_000_000),
        )(pair_tile, *smalls)

    return jax.shard_map(per_device, mesh=mesh, in_specs=(tile_spec, P('dp'), P(), P(), P(), P(), P(), P(), P(), P()), out_specs=tile_spec, check_vma=False)
```

```python
import functools

import jax
import jax.numpy as jnp
from jax import lax
from jax.experimental import pallas as pl
from jax.experimental.pallas import tpu as pltpu
from jax.sharding import PartitionSpec as P

LN_EPS = 1e-5
F32 = jnp.float32
BF16 = jnp.bfloat16
NT = (((1,), (1,)), ((), ()))
TN = (((0,), (0,)), ((), ()))
LOG2E = 1.4426950408889634
CORES = 2
STEP_ROWS = 2
BIG = 2
SMALL_ROWS = 8
LAST_ROWS = 4
SMALLS = 9
LAG = 6
EARLY = 3


def layer_norm(z, gamma, beta):
    x = z.astype(F32)
    centered = x - jnp.mean(x, axis=-1, keepdims=True)
    var = jnp.mean(jnp.square(centered), axis=-1, keepdims=True)
    return (centered * lax.rsqrt(var + LN_EPS) * gamma + beta).astype(BF16)


def over_keys(x, op):
    n, width = x.shape
    groups = 8
    t = op(x.reshape(groups, n // 8 // groups, 8, width), axis=1)
    return op(op(t, axis=0), axis=0, keepdims=True)


def kernel(heads, z_hbm, *refs):
    body(heads, z_hbm, refs[:SMALLS], refs[SMALLS + 1:2 * SMALLS + 1], refs[SMALLS], *refs[2 * SMALLS + 1:])


def body(heads, z_hbm, small_hbm, small_refs, out_ref,
           wt_ref, zbuf, own, outv, bias, btile, bsend, relay, brow, a0, a1, k0, k1, v0, v1, q0, q1, g0, g1,
           s0, s1, s2, s3, s4, s5, s6, s7, go0, go1,
           small_sem, local_sem, zp_send, zp_recv, zs_send, zs_recv, b1_send, b1_recv, b2_send, b2_recv,
           b3_send, b3_recv, o_send, o_recv):
    mask_ref, gamma_ref, beta_ref, wq_ref, wk_ref, wv_ref, wbt_ref, wg_ref, wo_ref = small_refs
    rows_all, width, chan = z_hbm.shape
    rows = rows_all // CORES
    n_q = CORES * width
    proj = wk_ref.shape[1]
    hd = proj // heads
    groups = rows // STEP_ROWS
    steps = (rows - LAST_ROWS) // STEP_ROWS
    dp, row, col = lax.axis_index('dp'), lax.axis_index('row'), lax.axis_index('col')
    n_row = lax.axis_size('row')
    core, chip = lax.rem(col, CORES), col // CORES
    partner = chip * CORES + 1 - core
    far = (1 - chip) * CORES
    home_chip = row // CORES
    jslot = lax.rem(row, CORES)
    home = chip == home_chip

    def remote(src, dst, send, recv, r, c):
        return pltpu.make_async_remote_copy(src, dst, send, recv, device_id=(dp, r, c),
                                            device_id_type=pl.DeviceIdType.MESH)

    barrier = pltpu.get_barrier_semaphore()
    peers = [(row, partner), (row, far), (row, far + 1)]
    peers += [(lax.rem(row + d, n_row), col) for d in range(1, 4)]
    for r, c in peers:
        pl.semaphore_signal(barrier, inc=1, device_id=(dp, r, c), device_id_type=pl.DeviceIdType.MESH)

    own_copy = pltpu.make_async_copy(z_hbm, own, local_sem.at[0])
    own_copy.start()
    mine_at = pl.ds(pl.multiple_of(core * width, width), width)
    theirs_at = pl.ds(pl.multiple_of((1 - core) * width, width), width)
    z_copy = pltpu.make_async_copy(z_hbm.at[pl.ds(core * rows, rows)], zbuf.at[:, mine_at, :], local_sem.at[1])
    z_copy.start()
    pl.semaphore_wait(barrier, len(peers))

    to_partner = remote(z_hbm.at[pl.ds((1 - core) * rows, rows)], zbuf.at[:, mine_at, :], zp_send, zp_recv, row, partner)

    bigs = (rows - SMALL_ROWS) // (BIG * STEP_ROWS)

    def z_copy_of(i, n, at_row, k, slot, c):
        at = pl.ds(pl.multiple_of((CORES + slot) * width, width), width)
        return remote(z_hbm.at[pl.ds(k * rows + at_row, n)], zbuf.at[pl.ds(at_row, n), at, :],
                      zs_send.at[k, i], zs_recv.at[slot, i], row, far + c)

    def big(i, k, slot):
        n = BIG * STEP_ROWS
        return z_copy_of(i, n, i * n, k, slot, k)

    def small(g, k, slot):
        return z_copy_of(bigs + g - bigs * BIG, STEP_ROWS, g * STEP_ROWS, k, slot, k)

    def send_step(i, carry):
        for k in range(CORES):
            big(i, k, core).start()
        return carry

    def z_wait(g):
        @pl.when(jnp.logical_and(g < bigs * BIG, lax.rem(g, BIG) == 0))
        def _():
            for k in range(CORES):
                big(jnp.minimum(g, bigs * BIG - 1) // BIG, k, k).wait_recv()

        @pl.when(g >= bigs * BIG)
        def _():
            for k in range(CORES):
                small(jnp.maximum(g, bigs * BIG), k, k).wait_recv()

    lax.fori_loop(0, EARLY, send_step, 0)
    to_partner.start()
    small_copies = [pltpu.make_async_copy(src, dst, small_sem.at[i]) for i, (src, dst) in enumerate(zip(small_hbm, small_refs))]
    for c in small_copies:
        c.start()
    for c in small_copies:
        c.wait()
    for i, w in enumerate((wv_ref, wq_ref, wg_ref)):
        wt_ref[i * proj:(i + 1) * proj] = w[...].T

    own_copy.wait()
    batch = 16
    mean_of = jnp.full((chan, chan), 1 / chan, BF16)

    def bias_step(i, carry):
        z = own[pl.ds(i * batch, batch)].reshape(batch * width, chan)
        centered = z.astype(F32) - jnp.dot(z, mean_of, preferred_element_type=F32)
        var = jnp.mean(jnp.square(centered), axis=-1, keepdims=True)
        a = (centered * lax.rsqrt(var + LN_EPS) * gamma_ref[...] + beta_ref[...]).astype(BF16)
        t = lax.dot_general(wbt_ref[...], a, NT, preferred_element_type=F32)
        for j in range(batch):
            for h in range(heads):
                brow[h, pl.ds(i * batch + j, 1), :] = t[h:h + 1, j * width:(j + 1) * width]
        return carry

    lax.fori_loop(0, rows_all // batch, bias_step, 0)
    home_slot = core * CORES + jslot
    for h in range(heads):
        tile = brow[h].T.astype(BF16)
        bsend[h] = tile

        @pl.when(home)
        def _():
            btile[home_slot, h] = tile

    masks = []
    for s in range(2 * CORES):
        block = chip * CORES + s if s < CORES else far + s - CORES
        m = mask_ref[:, pl.ds(pl.multiple_of(block * width, width), width)]
        masks.append(jnp.broadcast_to(jnp.where(m > 0, 0.0, -1e9).astype(F32), (width, width)).T)

    paired = lax.rem(row + CORES, n_row)
    hand = remote(bsend, relay, b1_send.at[0], b1_recv.at[0], paired, col)
    cross_slot = (CORES + core) * CORES + jslot
    cross = remote(relay, btile.at[cross_slot], b1_send.at[1], b1_recv.at[1], row, far + core)

    direct = remote(bsend, btile.at[cross_slot], b1_send.at[1], b1_recv.at[1], row, far + core)
    detour_out = jnp.logical_or(chip == 1, core == 1)
    detour_in = jnp.logical_or(chip == 0, core == 1)
    away = jnp.logical_not(home)
    lands = jnp.logical_or(jnp.logical_and(detour_in, away), jnp.logical_and(jnp.logical_not(detour_in), home))

    def spread(src, slot, t, d):
        return remote(src, btile.at[slot], b2_send.at[t, d - 1], b2_recv.at[t, jslot], lax.rem(row + d, n_row), col)

    @pl.when(jnp.logical_and(away, detour_out))
    def _():
        hand.start()

    @pl.when(jnp.logical_and(away, jnp.logical_not(detour_out)))
    def _():
        direct.start()

    @pl.when(home)
    def _():
        for d in range(1, 4):
            spread(bsend, home_slot, 0, d).start()

    @pl.when(jnp.logical_and(home, detour_out))
    def _():
        hand.wait_recv()
        cross.start()

    lax.fori_loop(EARLY, bigs, send_step, 0)
    for g in range(bigs * BIG, groups):
        for k in range(CORES):
            small(g, k, core).start()

    @pl.when(lands)
    def _():
        cross.wait_recv()
        for d in range(1, 4):
            spread(btile.at[cross_slot], cross_slot, 1, d).start()

    def forward(t, j):
        slot = (core + CORES * t) * CORES + j
        return remote(btile.at[slot], btile.at[slot], b3_send.at[t, j], b3_recv.at[t, j], row, partner)

    for t in range(2):
        for j in range(CORES):
            slot = (core + CORES * t) * CORES + j
            source = chip * CORES + j
            if t == 1:
                source = jnp.where(detour_in, far + j, source)

            @pl.when(row != source)
            def _():
                remote(bsend, btile.at[slot], b1_send.at[0], b2_recv.at[t, j], row, partner).wait_recv()

            forward(t, j).start()
    for j in range(CORES):
        for t in range(2):
            slot = (1 - core + CORES * t) * CORES + j
            remote(bsend, btile.at[slot], b1_send.at[0], b3_recv.at[t, j], row, partner).wait_recv()

    for s in range(2 * CORES):
        for j in range(CORES):
            for h in range(heads):
                b = btile[s * CORES + j, h].astype(F32)
                bias[h, s * width:(s + 1) * width, j * width:(j + 1) * width] = (b + masks[s]) * LOG2E

    a_s, k_s, v_s, q_s, g_s = (a0, a1), (k0, k1), (v0, v1), (q0, q1), (g0, g1)
    sc, go = ((s0, s1, s2, s3), (s4, s5, s6, s7)), (go0, go1)
    scale = hd ** -0.5 * LOG2E

    every, near, distant = slice(0, 2 * n_q), slice(0, n_q), slice(n_q, 2 * n_q)

    def scores(slot, h, dst, keys=every):
        part = q_s[slot][h * hd:(h + 1) * hd, :]
        none = jnp.zeros_like(part)
        rhs = jnp.concatenate([part if i == h else none for i in range(heads)], axis=0)
        dst[h][keys, :] = jnp.dot(k_s[slot][keys, :], rhs, preferred_element_type=F32) + bias[h, keys, :]

    def finish(r, src):
        for at, dst, i in ((mine_at, out_ref, core * rows + r), (theirs_at, outv, r)):
            upd = lax.dot_general(src[:, at], wo_ref[...], TN, preferred_element_type=F32)
            dst[i] = (zbuf[r, at].astype(F32) + upd).astype(BF16)

    def out_copy(g):
        return remote(outv.at[pl.ds(g * STEP_ROWS, STEP_ROWS)], out_ref.at[pl.ds(core * rows + g * STEP_ROWS, STEP_ROWS)],
                      o_send.at[g], o_recv.at[g], row, partner)

    def norm(r, slot, keys=every):
        a_s[slot][keys, :] = layer_norm(zbuf[r, keys, :], gamma_ref[...], beta_ref[...])

    def keys_of(slot, keys=every):
        k_s[slot][keys, :] = jnp.dot(a_s[slot][keys, :], wk_ref[...], preferred_element_type=F32).astype(BF16)

    def values_of(slot, keys=every):
        t = lax.dot_general(wt_ref[:proj], a_s[slot][keys, :], NT, preferred_element_type=F32)
        v_s[slot][:, keys] = t.astype(BF16)

    def queries_of(slot):
        t = lax.dot_general(wt_ref[proj:2 * proj], a_s[slot][near, :], NT, preferred_element_type=F32)
        q_s[slot][...] = (t * scale).astype(BF16)

    def gates_of(slot):
        t = lax.dot_general(wt_ref[2 * proj:], a_s[slot][near, :], NT, preferred_element_type=F32)
        g_s[slot][...] = jax.nn.sigmoid(t)

    def attend(h, slot, src, dst):
        s = src[h][...]
        p = jnp.exp2(s - over_keys(s, jnp.max))
        total = over_keys(p, jnp.sum)
        at = slice(h * hd, (h + 1) * hd)
        o = jnp.dot(v_s[slot][at, :], p.astype(BF16), preferred_element_type=F32)
        dst[at, :] = (g_s[slot][at, :] * (o / total)).astype(BF16)

    def sent(i, carry):
        for k in range(CORES):
            big(i, k, core).wait_send()
        return carry

    def drained(g, carry):
        out_copy(g).wait_send()
        remote(outv.at[pl.ds(0, STEP_ROWS)], out_ref.at[pl.ds((1 - core) * rows + g * STEP_ROWS, STEP_ROWS)],
               o_send.at[g], o_recv.at[g], row, partner).wait_recv()
        return carry

    def step(i, carry):
        @pl.when(i < steps)
        def _():
            z_wait(i)

        @pl.when(i > 2)
        def _():
            out_copy(jnp.maximum(i, 3) - 3).start()

        for r in range(STEP_ROWS):
            cur, nxt = r, 1 - r
            finish(jnp.maximum(2 * i + r, 3) - 3, go[0])
            norm(jnp.minimum(2 * i + r, steps * STEP_ROWS - 1), cur)
            for h in range(heads):
                if h < 2:
                    scores(cur, h + 2, sc[0])
                else:
                    scores(nxt, h - 2, sc[0])
                if h == 0:
                    keys_of(nxt)
                    queries_of(nxt)
                if h == 1:
                    gates_of(nxt)
                if h == 2:
                    values_of(nxt)
                attend(h, cur, sc[0], go[0])
        return carry

    def last_rows(i, carry):
        both = range(STEP_ROWS)
        units = [(r, h) for r in both for h in range(heads)]
        out_copy(i - 1).start()
        for r in both:
            norm(i * STEP_ROWS + r, r, near)
        for r in both:
            keys_of(r, near)
            queries_of(r)
            gates_of(r)
            values_of(r, near)
        for r, h in units:
            scores(r, h, sc[r], near)
        z_wait(i)
        for r in both:
            norm(i * STEP_ROWS + r, r, distant)
        for r in both:
            keys_of(r, distant)
        ahead = 2
        for r, h in units[:ahead]:
            scores(r, h, sc[r], distant)
        for r in both:
            values_of(r, distant)
        for n, (r, h) in enumerate(units):
            for r2, h2 in units[n + ahead:n + ahead + 1]:
                scores(r2, h2, sc[r2], distant)
            attend(h, r, sc[r], go[r])
        for r in both:
            finish(i * STEP_ROWS + r, go[r])
        return carry

    z_copy.wait()
    remote(z_hbm.at[pl.ds(0, rows)], zbuf.at[:, theirs_at, :], zp_send, zp_recv, row, partner).wait_recv()
    lax.fori_loop(0, steps + 1, step, 0)
    finish(steps * STEP_ROWS - 1, go[0])
    out_copy(steps - 2).start()
    lax.fori_loop(0, bigs - LAG, sent, 0)
    lax.fori_loop(0, steps + 1 - LAG, drained, 0)
    lax.fori_loop(steps, groups, last_rows, 0)
    to_partner.wait_send()
    lax.fori_loop(bigs - LAG, bigs, sent, 0)
    for g in range(bigs * BIG, groups):
        for k in range(CORES):
            small(g, k, core).wait_send()
    out_copy(groups - 1).start()

    @pl.when(jnp.logical_and(away, detour_out))
    def _():
        hand.wait_send()

    @pl.when(jnp.logical_or(jnp.logical_and(home, detour_out), jnp.logical_and(away, jnp.logical_not(detour_out))))
    def _():
        cross.wait_send()

    @pl.when(home)
    def _():
        for d in range(1, 4):
            spread(bsend, home_slot, 0, d).wait_send()

    @pl.when(lands)
    def _():
        for d in range(1, 4):
            spread(btile.at[cross_slot], cross_slot, 1, d).wait_send()

    for j in range(CORES):
        for t in range(2):
            forward(t, j).wait_send()

    lax.fori_loop(steps + 1 - LAG, groups, drained, 0)


def write_out(src, dst, sem):
    parts = sem.shape[0]
    n = src.shape[0] // parts
    copies = [pltpu.make_async_copy(src.at[pl.ds(i * n, n)], dst.at[pl.ds(i * n, n)], sem.at[i]) for i in range(parts)]
    for c in copies:
        c.start()
    for c in copies:
        c.wait()


def solution(mesh):
    tile_spec = P(('dp', 'row'), 'col', None)

    def per_device(pair_tile, res_mask, ln_gamma, ln_beta, w_q, w_k, w_v, w_b, w_g, w_o):
        row_len, width, chan = pair_tile.shape
        heads, proj = w_b.shape[1], w_q.shape[1]
        hd = proj // heads
        rows, n_q = row_len // CORES, CORES * width
        n_k = mesh.shape['col'] * width
        groups = rows // STEP_ROWS
        vmem = pltpu.VMEM
        dma = pltpu.SemaphoreType.DMA
        pairs = lambda *s: [vmem(*s)] * 2
        whole = pl.BlockSpec(memory_space=pltpu.VMEM)
        hbm = pl.BlockSpec(memory_space=pltpu.HBM)
        smalls = (res_mask.reshape(1, -1), ln_gamma.reshape(1, -1), ln_beta.reshape(1, -1), w_q, w_k, w_v, w_b.T, w_g, w_o)
        result = pl.pallas_call(
            functools.partial(kernel, heads),
            in_specs=[hbm] * (1 + len(smalls)),
            out_specs=whole,
            out_shape=pltpu.VMEM(pair_tile.shape, BF16),
            scratch_shapes=[
                *[vmem(w.shape, w.dtype) for w in smalls], vmem((3 * proj, chan), BF16),
                vmem((rows, n_k, chan), BF16), vmem((row_len, width, chan), BF16), vmem((rows, width, chan), BF16),
                vmem((heads, n_k, n_q), F32), vmem((8, heads, width, width), BF16), *pairs((heads, width, width), BF16),
                vmem((heads, width, width), F32),
                *pairs((n_k, chan), BF16), *pairs((n_k, proj), BF16), *pairs((proj, n_k), BF16),
                *pairs((proj, n_q), BF16), *pairs((proj, n_q), F32),
                *[vmem((n_k, n_q), F32)] * 8, *pairs((proj, n_q), BF16),
                dma((len(smalls),)), dma((2,)), dma, dma, dma((CORES, groups)), dma((CORES, groups)), dma((2,)), dma((2,)), dma((2, 3)), dma((2, CORES)),
                dma((2, CORES)), dma((2, CORES)), dma((groups,)), dma((groups,)),
            ],
            compiler_params=pltpu.CompilerParams(collective_id=0, has_side_effects=True, vmem_limit_bytes=58_000_000),
        )(pair_tile, *smalls)
        return pl.pallas_call(
            write_out,
            in_specs=[pl.BlockSpec(memory_space=pl.ANY)],
            out_specs=hbm,
            out_shape=jax.ShapeDtypeStruct(pair_tile.shape, BF16),
            scratch_shapes=[dma((4,))],
            compiler_params=pltpu.CompilerParams(vmem_limit_bytes=4 * 1024 * 1024),
        )(result)

    return jax.shard_map(per_device, mesh=mesh, in_specs=(tile_spec, P('dp'), P(), P(), P(), P(), P(), P(), P(), P()), out_specs=tile_spec, check_vma=False)
```

```python
import functools

import jax
import jax.numpy as jnp
from jax import lax
from jax.experimental import pallas as pl
from jax.experimental.pallas import tpu as pltpu
from jax.sharding import PartitionSpec as P

LN_EPS = 1e-5
F32 = jnp.float32
BF16 = jnp.bfloat16
NT = (((1,), (1,)), ((), ()))
TN = (((0,), (0,)), ((), ()))
LOG2E = 1.4426950408889634
CORES = 2
STEP_ROWS = 2
BIG = 2
SMALL_ROWS = 8
LAST_ROWS = 4
SMALLS = 9
LAG = 6
EARLY = 3


def layer_norm(z, gamma, beta):
    x = z.astype(F32)
    centered = x - jnp.mean(x, axis=-1, keepdims=True)
    var = jnp.mean(jnp.square(centered), axis=-1, keepdims=True)
    return (centered * lax.rsqrt(var + LN_EPS) * gamma + beta).astype(BF16)


def over_keys(x, op):
    n, width = x.shape
    groups = 8
    t = op(x.reshape(groups, n // 8 // groups, 8, width), axis=1)
    return op(op(t, axis=0), axis=0, keepdims=True)


def kernel(heads, z_hbm, *refs):
    body(heads, z_hbm, refs[:SMALLS], refs[SMALLS + 1:2 * SMALLS + 1], refs[SMALLS], *refs[2 * SMALLS + 1:])


def body(heads, z_hbm, small_hbm, small_refs, out_ref,
           wt_ref, zbuf, own, outv, bias, btile, bsend, relay, brow, a0, a1, k0, k1, v0, v1, q0, q1, g0, g1,
           s0, s1, s2, s3, s4, s5, s6, s7, go0, go1,
           round_sem, small_sem, local_sem, zp_send, zp_recv, zs_send, zs_recv, b1_send, b1_recv, b2_send, b2_recv,
           b3_send, b3_recv, o_send, o_recv):
    mask_ref, gamma_ref, beta_ref, wq_ref, wk_ref, wv_ref, wbt_ref, wg_ref, wo_ref = small_refs
    rows_all, width, chan = z_hbm.shape
    rows = rows_all // CORES
    n_q = CORES * width
    proj = wk_ref.shape[1]
    hd = proj // heads
    groups = rows // STEP_ROWS
    steps = (rows - LAST_ROWS) // STEP_ROWS
    dp, row, col = lax.axis_index('dp'), lax.axis_index('row'), lax.axis_index('col')
    n_row = lax.axis_size('row')
    core, chip = lax.rem(col, CORES), col // CORES
    partner = chip * CORES + 1 - core
    far = (1 - chip) * CORES
    home_chip = row // CORES
    jslot = lax.rem(row, CORES)
    home = chip == home_chip

    def remote(src, dst, send, recv, r, c):
        return pltpu.make_async_remote_copy(src, dst, send, recv, device_id=(dp, r, c),
                                            device_id_type=pl.DeviceIdType.MESH)

    def signal(sem, r, c):
        pl.semaphore_signal(sem, inc=1, device_id=(dp, r, c), device_id_type=pl.DeviceIdType.MESH)

    def tell_next_rows(sem):
        @pl.when(row > 0)
        def _():
            signal(sem, jnp.maximum(row, 1) - 1, col)

        @pl.when(row < n_row - 1)
        def _():
            signal(sem, jnp.minimum(row, n_row - 2) + 1, col)

    next_rows = jnp.where(row > 0, 1, 0) + jnp.where(row < n_row - 1, 1, 0)

    barrier = pltpu.get_barrier_semaphore()
    for c in (partner, far, far + 1):
        signal(barrier, row, c)
    tell_next_rows(barrier)

    own_copy = pltpu.make_async_copy(z_hbm, own, local_sem.at[0])
    own_copy.start()
    mine_at = pl.ds(pl.multiple_of(core * width, width), width)
    theirs_at = pl.ds(pl.multiple_of((1 - core) * width, width), width)
    z_copy = pltpu.make_async_copy(z_hbm.at[pl.ds(core * rows, rows)], zbuf.at[:, mine_at, :], local_sem.at[1])
    z_copy.start()
    pl.semaphore_wait(barrier, 3 + next_rows)

    to_partner = remote(z_hbm.at[pl.ds((1 - core) * rows, rows)], zbuf.at[:, mine_at, :], zp_send, zp_recv, row, partner)

    bigs = (rows - SMALL_ROWS) // (BIG * STEP_ROWS)

    def z_copy_of(i, n, at_row, k, slot, c):
        at = pl.ds(pl.multiple_of((CORES + slot) * width, width), width)
        return remote(z_hbm.at[pl.ds(k * rows + at_row, n)], zbuf.at[pl.ds(at_row, n), at, :],
                      zs_send.at[k, i], zs_recv.at[slot, i], row, far + c)

    def big(i, k, slot):
        n = BIG * STEP_ROWS
        return z_copy_of(i, n, i * n, k, slot, k)

    def small(g, k, slot):
        return z_copy_of(bigs + g - bigs * BIG, STEP_ROWS, g * STEP_ROWS, k, slot, k)

    def send_step(i, carry):
        for k in range(CORES):
            big(i, k, core).start()
        return carry

    def z_wait(g):
        @pl.when(jnp.logical_and(g < bigs * BIG, lax.rem(g, BIG) == 0))
        def _():
            for k in range(CORES):
                big(jnp.minimum(g, bigs * BIG - 1) // BIG, k, k).wait_recv()

        @pl.when(g >= bigs * BIG)
        def _():
            for k in range(CORES):
                small(jnp.maximum(g, bigs * BIG), k, k).wait_recv()

    lax.fori_loop(0, EARLY, send_step, 0)
    to_partner.start()
    small_copies = [pltpu.make_async_copy(src, dst, small_sem.at[i]) for i, (src, dst) in enumerate(zip(small_hbm, small_refs))]
    for c in small_copies:
        c.start()
    for c in small_copies:
        c.wait()
    for i, w in enumerate((wv_ref, wq_ref, wg_ref)):
        wt_ref[i * proj:(i + 1) * proj] = w[...].T

    own_copy.wait()
    batch = 16
    mean_of = jnp.full((chan, chan), 1 / chan, BF16)

    def bias_step(i, carry):
        z = own[pl.ds(i * batch, batch)].reshape(batch * width, chan)
        centered = z.astype(F32) - jnp.dot(z, mean_of, preferred_element_type=F32)
        var = jnp.mean(jnp.square(centered), axis=-1, keepdims=True)
        a = (centered * lax.rsqrt(var + LN_EPS) * gamma_ref[...] + beta_ref[...]).astype(BF16)
        t = lax.dot_general(wbt_ref[...], a, NT, preferred_element_type=F32)
        for j in range(batch):
            for h in range(heads):
                brow[h, pl.ds(i * batch + j, 1), :] = t[h:h + 1, j * width:(j + 1) * width]
        return carry

    lax.fori_loop(0, rows_all // batch, bias_step, 0)
    home_slot = core * CORES + jslot
    for h in range(heads):
        tile = brow[h].T.astype(BF16)
        bsend[h] = tile

        @pl.when(home)
        def _():
            btile[home_slot, h] = tile

    for i in range(2):
        tell_next_rows(round_sem.at[i])
        pl.semaphore_wait(round_sem.at[i], next_rows)

    masks = []
    for s in range(2 * CORES):
        block = chip * CORES + s if s < CORES else far + s - CORES
        m = mask_ref[:, pl.ds(pl.multiple_of(block * width, width), width)]
        masks.append(jnp.broadcast_to(jnp.where(m > 0, 0.0, -1e9).astype(F32), (width, width)).T)

    paired = lax.rem(row + CORES, n_row)
    hand = remote(bsend, relay, b1_send.at[0], b1_recv.at[0], paired, col)
    cross_slot = (CORES + core) * CORES + jslot
    cross = remote(relay, btile.at[cross_slot], b1_send.at[1], b1_recv.at[1], row, far + core)

    direct = remote(bsend, btile.at[cross_slot], b1_send.at[1], b1_recv.at[1], row, far + core)
    detour_out = jnp.logical_or(chip == 1, core == 1)
    detour_in = jnp.logical_or(chip == 0, core == 1)
    away = jnp.logical_not(home)
    lands = jnp.logical_or(jnp.logical_and(detour_in, away), jnp.logical_and(jnp.logical_not(detour_in), home))

    def spread(src, slot, t, d):
        return remote(src, btile.at[slot], b2_send.at[t, d - 1], b2_recv.at[t, jslot], lax.rem(row + d, n_row), col)

    @pl.when(jnp.logical_and(away, detour_out))
    def _():
        hand.start()

    @pl.when(jnp.logical_and(away, jnp.logical_not(detour_out)))
    def _():
        direct.start()

    @pl.when(home)
    def _():
        for d in range(1, 4):
            spread(bsend, home_slot, 0, d).start()

    @pl.when(jnp.logical_and(home, detour_out))
    def _():
        hand.wait_recv()
        cross.start()

    lax.fori_loop(EARLY, bigs, send_step, 0)
    for g in range(bigs * BIG, groups):
        for k in range(CORES):
            small(g, k, core).start()

    @pl.when(lands)
    def _():
        cross.wait_recv()
        for d in range(1, 4):
            spread(btile.at[cross_slot], cross_slot, 1, d).start()

    def forward(t, j):
        slot = (core + CORES * t) * CORES + j
        return remote(btile.at[slot], btile.at[slot], b3_send.at[t, j], b3_recv.at[t, j], row, partner)

    for t in range(2):
        for j in range(CORES):
            slot = (core + CORES * t) * CORES + j
            source = chip * CORES + j
            if t == 1:
                source = jnp.where(detour_in, far + j, source)

            @pl.when(row != source)
            def _():
                remote(bsend, btile.at[slot], b1_send.at[0], b2_recv.at[t, j], row, partner).wait_recv()

            forward(t, j).start()
    for j in range(CORES):
        for t in range(2):
            slot = (1 - core + CORES * t) * CORES + j
            remote(bsend, btile.at[slot], b1_send.at[0], b3_recv.at[t, j], row, partner).wait_recv()

    for s in range(2 * CORES):
        for j in range(CORES):
            for h in range(heads):
                b = btile[s * CORES + j, h].astype(F32)
                bias[h, s * width:(s + 1) * width, j * width:(j + 1) * width] = (b + masks[s]) * LOG2E

    a_s, k_s, v_s, q_s, g_s = (a0, a1), (k0, k1), (v0, v1), (q0, q1), (g0, g1)
    sc, go = ((s0, s1, s2, s3), (s4, s5, s6, s7)), (go0, go1)
    scale = hd ** -0.5 * LOG2E

    every, near, distant = slice(0, 2 * n_q), slice(0, n_q), slice(n_q, 2 * n_q)

    def scores(slot, h, dst, keys=every):
        part = q_s[slot][h * hd:(h + 1) * hd, :]
        none = jnp.zeros_like(part)
        rhs = jnp.concatenate([part if i == h else none for i in range(heads)], axis=0)
        dst[h][keys, :] = jnp.dot(k_s[slot][keys, :], rhs, preferred_element_type=F32) + bias[h, keys, :]

    def finish(r, src):
        for at, dst, i in ((theirs_at, outv, r), (mine_at, out_ref, core * rows + r)):
            upd = lax.dot_general(src[:, at], wo_ref[...], TN, preferred_element_type=F32)
            dst[i] = (zbuf[r, at].astype(F32) + upd).astype(BF16)

    def out_copy(g):
        return remote(outv.at[pl.ds(g * STEP_ROWS, STEP_ROWS)], out_ref.at[pl.ds(core * rows + g * STEP_ROWS, STEP_ROWS)],
                      o_send.at[g], o_recv.at[g], row, partner)

    def norm(r, slot, keys=every):
        a_s[slot][keys, :] = layer_norm(zbuf[r, keys, :], gamma_ref[...], beta_ref[...])

    def keys_of(slot, keys=every):
        k_s[slot][keys, :] = jnp.dot(a_s[slot][keys, :], wk_ref[...], preferred_element_type=F32).astype(BF16)

    def values_of(slot, keys=every):
        t = lax.dot_general(wt_ref[:proj], a_s[slot][keys, :], NT, preferred_element_type=F32)
        v_s[slot][:, keys] = t.astype(BF16)

    def queries_of(slot):
        t = lax.dot_general(wt_ref[proj:2 * proj], a_s[slot][near, :], NT, preferred_element_type=F32)
        q_s[slot][...] = (t * scale).astype(BF16)

    def gates_of(slot):
        t = lax.dot_general(wt_ref[2 * proj:], a_s[slot][near, :], NT, preferred_element_type=F32)
        g_s[slot][...] = jax.nn.sigmoid(t)

    def attend(h, slot, src, dst):
        s = src[h][...]
        p = jnp.exp2(s - over_keys(s, jnp.max))
        total = over_keys(p, jnp.sum)
        at = slice(h * hd, (h + 1) * hd)
        o = jnp.dot(v_s[slot][at, :], p.astype(BF16), preferred_element_type=F32)
        dst[at, :] = (g_s[slot][at, :] * (o / total)).astype(BF16)

    def sent(i, carry):
        for k in range(CORES):
            big(i, k, core).wait_send()
        return carry

    def drained(g, carry):
        out_copy(g).wait_send()
        remote(outv.at[pl.ds(0, STEP_ROWS)], out_ref.at[pl.ds((1 - core) * rows + g * STEP_ROWS, STEP_ROWS)],
               o_send.at[g], o_recv.at[g], row, partner).wait_recv()
        return carry

    def step(i, carry):
        @pl.when(i < steps)
        def _():
            z_wait(i)

        @pl.when(i > 2)
        def _():
            out_copy(jnp.maximum(i, 3) - 3).start()

        for r in range(STEP_ROWS):
            cur, nxt = r, 1 - r
            finish(jnp.maximum(2 * i + r, 3) - 3, go[0])
            norm(jnp.minimum(2 * i + r, steps * STEP_ROWS - 1), cur)
            for h in range(heads):
                if h < 2:
                    scores(cur, h + 2, sc[0])
                else:
                    scores(nxt, h - 2, sc[0])
                if h == 0:
                    keys_of(nxt)
                    queries_of(nxt)
                if h == 1:
                    gates_of(nxt)
                if h == 2:
                    values_of(nxt)
                attend(h, cur, sc[0], go[0])
        return carry

    def last_rows(i, carry):
        both = range(STEP_ROWS)
        units = [(r, h) for r in both for h in range(heads)]
        out_copy(i - 1).start()
        for r in both:
            norm(i * STEP_ROWS + r, r, near)
        for r in both:
            keys_of(r, near)
            queries_of(r)
            gates_of(r)
            values_of(r, near)
        for r, h in units:
            scores(r, h, sc[r], near)
        z_wait(i)
        for r in both:
            norm(i * STEP_ROWS + r, r, distant)
        for r in both:
            keys_of(r, distant)
        ahead = 2
        for r, h in units[:ahead]:
            scores(r, h, sc[r], distant)
        for r in both:
            values_of(r, distant)
        for n, (r, h) in enumerate(units):
            for r2, h2 in units[n + ahead:n + ahead + 1]:
                scores(r2, h2, sc[r2], distant)
            attend(h, r, sc[r], go[r])
        for r in both:
            finish(i * STEP_ROWS + r, go[r])
        return carry

    z_copy.wait()
    remote(z_hbm.at[pl.ds(0, rows)], zbuf.at[:, theirs_at, :], zp_send, zp_recv, row, partner).wait_recv()
    lax.fori_loop(0, steps + 1, step, 0)
    finish(steps * STEP_ROWS - 1, go[0])
    out_copy(steps - 2).start()
    lax.fori_loop(0, bigs - LAG, sent, 0)
    lax.fori_loop(0, steps + 1 - LAG, drained, 0)
    lax.fori_loop(steps, groups, last_rows, 0)
    to_partner.wait_send()
    out_copy(groups - 1).start()
    lax.fori_loop(bigs - LAG, bigs, sent, 0)
    for g in range(bigs * BIG, groups):
        for k in range(CORES):
            small(g, k, core).wait_send()

    @pl.when(jnp.logical_and(away, detour_out))
    def _():
        hand.wait_send()

    @pl.when(jnp.logical_or(jnp.logical_and(home, detour_out), jnp.logical_and(away, jnp.logical_not(detour_out))))
    def _():
        cross.wait_send()

    @pl.when(home)
    def _():
        for d in range(1, 4):
            spread(bsend, home_slot, 0, d).wait_send()

    @pl.when(lands)
    def _():
        for d in range(1, 4):
            spread(btile.at[cross_slot], cross_slot, 1, d).wait_send()

    for j in range(CORES):
        for t in range(2):
            forward(t, j).wait_send()

    lax.fori_loop(steps + 1 - LAG, groups, drained, 0)


def write_out(src, dst, sem):
    parts = sem.shape[0]
    n = src.shape[0] // parts
    copies = [pltpu.make_async_copy(src.at[pl.ds(i * n, n)], dst.at[pl.ds(i * n, n)], sem.at[i]) for i in range(parts)]
    for c in copies:
        c.start()
    for c in copies:
        c.wait()


def solution(mesh):
    tile_spec = P(('dp', 'row'), 'col', None)

    def per_device(pair_tile, res_mask, ln_gamma, ln_beta, w_q, w_k, w_v, w_b, w_g, w_o):
        row_len, width, chan = pair_tile.shape
        heads, proj = w_b.shape[1], w_q.shape[1]
        hd = proj // heads
        rows, n_q = row_len // CORES, CORES * width
        n_k = mesh.shape['col'] * width
        groups = rows // STEP_ROWS
        vmem = pltpu.VMEM
        dma = pltpu.SemaphoreType.DMA
        pairs = lambda *s: [vmem(*s)] * 2
        whole = pl.BlockSpec(memory_space=pltpu.VMEM)
        hbm = pl.BlockSpec(memory_space=pltpu.HBM)
        smalls = (res_mask.reshape(1, -1), ln_gamma.reshape(1, -1), ln_beta.reshape(1, -1), w_q, w_k, w_v, w_b.T, w_g, w_o)
        result = pl.pallas_call(
            functools.partial(kernel, heads),
            in_specs=[hbm] * (1 + len(smalls)),
            out_specs=whole,
            out_shape=pltpu.VMEM(pair_tile.shape, BF16),
            scratch_shapes=[
                *[vmem(w.shape, w.dtype) for w in smalls], vmem((3 * proj, chan), BF16),
                vmem((rows, n_k, chan), BF16), vmem((row_len, width, chan), BF16), vmem((rows, width, chan), BF16),
                vmem((heads, n_k, n_q), F32), vmem((8, heads, width, width), BF16), *pairs((heads, width, width), BF16),
                vmem((heads, width, width), F32),
                *pairs((n_k, chan), BF16), *pairs((n_k, proj), BF16), *pairs((proj, n_k), BF16),
                *pairs((proj, n_q), BF16), *pairs((proj, n_q), F32),
                *[vmem((n_k, n_q), F32)] * 8, *pairs((proj, n_q), BF16),
                pltpu.SemaphoreType.REGULAR((2,)), dma((len(smalls),)), dma((2,)), dma, dma, dma((CORES, groups)), dma((CORES, groups)), dma((2,)), dma((2,)), dma((2, 3)), dma((2, CORES)),
                dma((2, CORES)), dma((2, CORES)), dma((groups,)), dma((groups,)),
            ],
            compiler_params=pltpu.CompilerParams(collective_id=0, has_side_effects=True, vmem_limit_bytes=58_000_000),
        )(pair_tile, *smalls)
        return pl.pallas_call(
            write_out,
            in_specs=[pl.BlockSpec(memory_space=pl.ANY)],
            out_specs=hbm,
            out_shape=jax.ShapeDtypeStruct(pair_tile.shape, BF16),
            scratch_shapes=[dma((4,))],
            compiler_params=pltpu.CompilerParams(vmem_limit_bytes=4 * 1024 * 1024),
        )(result)

    return jax.shard_map(per_device, mesh=mesh, in_specs=(tile_spec, P('dp'), P(), P(), P(), P(), P(), P(), P(), P()), out_specs=tile_spec, check_vma=False)
```

```python
import functools

import jax
import jax.numpy as jnp
from jax import lax
from jax.experimental import pallas as pl
from jax.experimental.pallas import tpu as pltpu
from jax.sharding import PartitionSpec as P

LN_EPS = 1e-5
F32 = jnp.float32
BF16 = jnp.bfloat16
NT = (((1,), (1,)), ((), ()))
TN = (((0,), (0,)), ((), ()))
LOG2E = 1.4426950408889634
CORES = 2
STEP_ROWS = 2
BIG = 2
SMALL_ROWS = 8
LAST_ROWS = 4
STRAIGHT = 1
SMALLS = 9
LAG = 6
EARLY = 3


def layer_norm(z, gamma, beta):
    x = z.astype(F32)
    centered = x - jnp.mean(x, axis=-1, keepdims=True)
    var = jnp.mean(jnp.square(centered), axis=-1, keepdims=True)
    return (centered * lax.rsqrt(var + LN_EPS) * gamma + beta).astype(BF16)


def over_keys(x, op):
    n, width = x.shape
    groups = 8
    t = op(x.reshape(groups, n // 8 // groups, 8, width), axis=1)
    return op(op(t, axis=0), axis=0, keepdims=True)


def kernel(heads, z_hbm, *refs):
    body(heads, z_hbm, refs[:SMALLS], refs[SMALLS + 1:2 * SMALLS + 1], refs[SMALLS], *refs[2 * SMALLS + 1:])


def body(heads, z_hbm, small_hbm, small_refs, out_ref,
           wt_ref, zbuf, own, outv, bias, btile, bsend, relay, brow, a0, a1, k0, k1, v0, v1, q0, q1, g0, g1,
           s0, s1, s2, s3, s4, s5, s6, s7, go0, go1,
           round_sem, small_sem, local_sem, zp_send, zp_recv, zs_send, zs_recv, b1_send, b1_recv, b2_send, b2_recv,
           b3_send, b3_recv, o_send, o_recv):
    mask_ref, gamma_ref, beta_ref, wq_ref, wk_ref, wv_ref, wbt_ref, wg_ref, wo_ref = small_refs
    rows_all, width, chan = z_hbm.shape
    rows = rows_all // CORES
    n_q = CORES * width
    proj = wk_ref.shape[1]
    hd = proj // heads
    groups = rows // STEP_ROWS
    steps = (rows - LAST_ROWS) // STEP_ROWS
    dp, row, col = lax.axis_index('dp'), lax.axis_index('row'), lax.axis_index('col')
    n_row = lax.axis_size('row')
    core, chip = lax.rem(col, CORES), col // CORES
    partner = chip * CORES + 1 - core
    far = (1 - chip) * CORES
    home_chip = row // CORES
    jslot = lax.rem(row, CORES)
    home = chip == home_chip

    def remote(src, dst, send, recv, r, c):
        return pltpu.make_async_remote_copy(src, dst, send, recv, device_id=(dp, r, c),
                                            device_id_type=pl.DeviceIdType.MESH)

    def signal(sem, r, c):
        pl.semaphore_signal(sem, inc=1, device_id=(dp, r, c), device_id_type=pl.DeviceIdType.MESH)

    def tell_next_rows(sem):
        @pl.when(row > 0)
        def _():
            signal(sem, jnp.maximum(row, 1) - 1, col)

        @pl.when(row < n_row - 1)
        def _():
            signal(sem, jnp.minimum(row, n_row - 2) + 1, col)

    next_rows = jnp.where(row > 0, 1, 0) + jnp.where(row < n_row - 1, 1, 0)

    barrier = pltpu.get_barrier_semaphore()
    for c in (partner, far, far + 1):
        signal(barrier, row, c)
    tell_next_rows(barrier)

    own_copy = pltpu.make_async_copy(z_hbm, own, local_sem.at[0])
    own_copy.start()
    mine_at = pl.ds(pl.multiple_of(core * width, width), width)
    theirs_at = pl.ds(pl.multiple_of((1 - core) * width, width), width)
    z_copy = pltpu.make_async_copy(z_hbm.at[pl.ds(core * rows, rows)], zbuf.at[:, mine_at, :], local_sem.at[1])
    z_copy.start()
    pl.semaphore_wait(barrier, 3 + next_rows)

    to_partner = remote(z_hbm.at[pl.ds((1 - core) * rows, rows)], zbuf.at[:, mine_at, :], zp_send, zp_recv, row, partner)

    bigs = (rows - SMALL_ROWS) // (BIG * STEP_ROWS)

    def z_copy_of(i, n, at_row, k, slot, c):
        at = pl.ds(pl.multiple_of((CORES + slot) * width, width), width)
        return remote(z_hbm.at[pl.ds(k * rows + at_row, n)], zbuf.at[pl.ds(at_row, n), at, :],
                      zs_send.at[k, i], zs_recv.at[slot, i], row, far + c)

    def big(i, k, slot):
        n = BIG * STEP_ROWS
        return z_copy_of(i, n, i * n, k, slot, k)

    def small(g, k, slot):
        return z_copy_of(bigs + g - bigs * BIG, STEP_ROWS, g * STEP_ROWS, k, slot, k)

    def send_step(i, carry):
        for k in range(CORES):
            big(i, k, core).start()
        return carry

    def z_wait(g):
        @pl.when(jnp.logical_and(g < bigs * BIG, lax.rem(g, BIG) == 0))
        def _():
            for k in range(CORES):
                big(jnp.minimum(g, bigs * BIG - 1) // BIG, k, k).wait_recv()

        @pl.when(g >= bigs * BIG)
        def _():
            for k in range(CORES):
                small(jnp.maximum(g, bigs * BIG), k, k).wait_recv()

    lax.fori_loop(0, EARLY, send_step, 0)
    to_partner.start()
    small_copies = [pltpu.make_async_copy(src, dst, small_sem.at[i]) for i, (src, dst) in enumerate(zip(small_hbm, small_refs))]
    for c in small_copies:
        c.start()
    for c in small_copies:
        c.wait()
    for i, w in enumerate((wv_ref, wq_ref, wg_ref)):
        wt_ref[i * proj:(i + 1) * proj] = w[...].T

    own_copy.wait()
    batch = 16
    mean_of = jnp.full((chan, chan), 1 / chan, BF16)

    def bias_step(i, carry):
        z = own[pl.ds(i * batch, batch)].reshape(batch * width, chan)
        centered = z.astype(F32) - jnp.dot(z, mean_of, preferred_element_type=F32)
        var = jnp.mean(jnp.square(centered), axis=-1, keepdims=True)
        a = (centered * lax.rsqrt(var + LN_EPS) * gamma_ref[...] + beta_ref[...]).astype(BF16)
        t = lax.dot_general(wbt_ref[...], a, NT, preferred_element_type=F32)
        for j in range(batch):
            for h in range(heads):
                brow[h, pl.ds(i * batch + j, 1), :] = t[h:h + 1, j * width:(j + 1) * width]
        return carry

    lax.fori_loop(0, rows_all // batch, bias_step, 0)
    home_slot = core * CORES + jslot
    for h in range(heads):
        tile = brow[h].T.astype(BF16)
        bsend[h] = tile

        @pl.when(home)
        def _():
            btile[home_slot, h] = tile

    for i in range(2):
        tell_next_rows(round_sem.at[i])
        pl.semaphore_wait(round_sem.at[i], next_rows)

    masks = []
    for s in range(2 * CORES):
        block = chip * CORES + s if s < CORES else far + s - CORES
        m = mask_ref[:, pl.ds(pl.multiple_of(block * width, width), width)]
        masks.append(jnp.broadcast_to(jnp.where(m > 0, 0.0, -1e9).astype(F32), (width, width)).T)

    paired = lax.rem(row + CORES, n_row)
    parts = (slice(0, heads), slice(0, STRAIGHT), slice(STRAIGHT, heads))
    of = lambda ref, t: ref.at[pl.ds(parts[t].start, parts[t].stop - parts[t].start)]
    tile_of = lambda slot, t: of(btile.at[slot], t)
    cross_slot = (CORES + core) * CORES + jslot
    straight = remote(of(bsend, 1), tile_of(cross_slot, 1), b1_send.at[0], b1_recv.at[0], row, far + core)
    hand = remote(of(bsend, 2), of(relay, 2), b1_send.at[1], b1_recv.at[1], paired, col)
    cross = remote(of(relay, 2), tile_of(cross_slot, 2), b1_send.at[2], b1_recv.at[2], row, far + core)
    away = jnp.logical_not(home)

    def spread(t, d):
        slot = home_slot if t == 0 else cross_slot
        return remote(bsend if t == 0 else tile_of(slot, t), tile_of(slot, t), b2_send.at[t, d - 1], b2_recv.at[t, jslot],
                      lax.rem(row + d, n_row), col)

    @pl.when(away)
    def _():
        hand.start()
        straight.start()

    @pl.when(home)
    def _():
        for d in range(1, 4):
            spread(0, d).start()
        hand.wait_recv()
        cross.start()

    lax.fori_loop(EARLY, bigs, send_step, 0)
    for g in range(bigs * BIG, groups):
        for k in range(CORES):
            small(g, k, core).start()

    @pl.when(home)
    def _():
        straight.wait_recv()
        for d in range(1, 4):
            spread(1, d).start()

    @pl.when(away)
    def _():
        cross.wait_recv()
        for d in range(1, 4):
            spread(2, d).start()

    def forward(t, j):
        slot = (core + CORES * t) * CORES + j
        return remote(btile.at[slot], btile.at[slot], b3_send.at[t, j], b3_recv.at[t, j], row, partner)

    for t in range(2):
        for j in range(CORES):
            slot = (core + CORES * t) * CORES + j
            for part, source in ((0, chip * CORES + j),) if t == 0 else ((1, chip * CORES + j), (2, far + j)):

                @pl.when(row != source)
                def _():
                    remote(of(bsend, part), tile_of(slot, part), b1_send.at[0], b2_recv.at[part, j], row, partner).wait_recv()

            forward(t, j).start()
    for j in range(CORES):
        for t in range(2):
            slot = (1 - core + CORES * t) * CORES + j
            remote(bsend, btile.at[slot], b1_send.at[0], b3_recv.at[t, j], row, partner).wait_recv()

    for s in range(2 * CORES):
        for j in range(CORES):
            for h in range(heads):
                b = btile[s * CORES + j, h].astype(F32)
                bias[h, s * width:(s + 1) * width, j * width:(j + 1) * width] = (b + masks[s]) * LOG2E

    a_s, k_s, v_s, q_s, g_s = (a0, a1), (k0, k1), (v0, v1), (q0, q1), (g0, g1)
    sc, go = ((s0, s1, s2, s3), (s4, s5, s6, s7)), (go0, go1)
    scale = hd ** -0.5 * LOG2E

    every, near, distant = slice(0, 2 * n_q), slice(0, n_q), slice(n_q, 2 * n_q)

    def scores(slot, h, dst, keys=every):
        part = q_s[slot][h * hd:(h + 1) * hd, :]
        none = jnp.zeros_like(part)
        rhs = jnp.concatenate([part if i == h else none for i in range(heads)], axis=0)
        dst[h][keys, :] = jnp.dot(k_s[slot][keys, :], rhs, preferred_element_type=F32) + bias[h, keys, :]

    def finish(r, src):
        for at, dst, i in ((theirs_at, outv, r), (mine_at, out_ref, core * rows + r)):
            upd = lax.dot_general(src[:, at], wo_ref[...], TN, preferred_element_type=F32)
            dst[i] = (zbuf[r, at].astype(F32) + upd).astype(BF16)

    def out_copy(g):
        return remote(outv.at[pl.ds(g * STEP_ROWS, STEP_ROWS)], out_ref.at[pl.ds(core * rows + g * STEP_ROWS, STEP_ROWS)],
                      o_send.at[g], o_recv.at[g], row, partner)

    def norm(r, slot, keys=every):
        a_s[slot][keys, :] = layer_norm(zbuf[r, keys, :], gamma_ref[...], beta_ref[...])

    def keys_of(slot, keys=every):
        k_s[slot][keys, :] = jnp.dot(a_s[slot][keys, :], wk_ref[...], preferred_element_type=F32).astype(BF16)

    def values_of(slot, keys=every):
        t = lax.dot_general(wt_ref[:proj], a_s[slot][keys, :], NT, preferred_element_type=F32)
        v_s[slot][:, keys] = t.astype(BF16)

    def queries_of(slot):
        t = lax.dot_general(wt_ref[proj:2 * proj], a_s[slot][near, :], NT, preferred_element_type=F32)
        q_s[slot][...] = (t * scale).astype(BF16)

    def gates_of(slot):
        t = lax.dot_general(wt_ref[2 * proj:], a_s[slot][near, :], NT, preferred_element_type=F32)
        g_s[slot][...] = jax.nn.sigmoid(t)

    def attend(h, slot, src, dst):
        s = src[h][...]
        p = jnp.exp2(s - over_keys(s, jnp.max))
        total = over_keys(p, jnp.sum)
        at = slice(h * hd, (h + 1) * hd)
        o = jnp.dot(v_s[slot][at, :], p.astype(BF16), preferred_element_type=F32)
        dst[at, :] = (g_s[slot][at, :] * (o / total)).astype(BF16)

    def sent(i, carry):
        for k in range(CORES):
            big(i, k, core).wait_send()
        return carry

    def drained(g, carry):
        out_copy(g).wait_send()
        remote(outv.at[pl.ds(0, STEP_ROWS)], out_ref.at[pl.ds((1 - core) * rows + g * STEP_ROWS, STEP_ROWS)],
               o_send.at[g], o_recv.at[g], row, partner).wait_recv()
        return carry

    def step(i, carry):
        @pl.when(i < steps)
        def _():
            z_wait(i)

        @pl.when(i > 2)
        def _():
            out_copy(jnp.maximum(i, 3) - 3).start()

        for r in range(STEP_ROWS):
            cur, nxt = r, 1 - r
            finish(jnp.maximum(2 * i + r, 3) - 3, go[0])
            norm(jnp.minimum(2 * i + r, steps * STEP_ROWS - 1), cur)
            for h in range(heads):
                if h < 2:
                    scores(cur, h + 2, sc[0])
                else:
                    scores(nxt, h - 2, sc[0])
                if h == 0:
                    keys_of(nxt)
                    queries_of(nxt)
                if h == 1:
                    gates_of(nxt)
                if h == 2:
                    values_of(nxt)
                attend(h, cur, sc[0], go[0])
        return carry

    def last_rows(i, carry):
        both = range(STEP_ROWS)
        units = [(r, h) for r in both for h in range(heads)]
        out_copy(i - 1).start()
        for r in both:
            norm(i * STEP_ROWS + r, r, near)
        for r in both:
            keys_of(r, near)
            queries_of(r)
            gates_of(r)
            values_of(r, near)
        for r, h in units:
            scores(r, h, sc[r], near)
        z_wait(i)
        for r in both:
            norm(i * STEP_ROWS + r, r, distant)
        for r in both:
            keys_of(r, distant)
        ahead = 2
        for r, h in units[:ahead]:
            scores(r, h, sc[r], distant)
        for r in both:
            values_of(r, distant)
        for n, (r, h) in enumerate(units):
            for r2, h2 in units[n + ahead:n + ahead + 1]:
                scores(r2, h2, sc[r2], distant)
            attend(h, r, sc[r], go[r])
        for r in both:
            finish(i * STEP_ROWS + r, go[r])
        return carry

    z_copy.wait()
    remote(z_hbm.at[pl.ds(0, rows)], zbuf.at[:, theirs_at, :], zp_send, zp_recv, row, partner).wait_recv()
    lax.fori_loop(0, steps + 1, step, 0)
    finish(steps * STEP_ROWS - 1, go[0])
    out_copy(steps - 2).start()
    lax.fori_loop(0, bigs - LAG, sent, 0)
    lax.fori_loop(0, steps + 1 - LAG, drained, 0)
    lax.fori_loop(steps, groups, last_rows, 0)
    to_partner.wait_send()
    out_copy(groups - 1).start()
    lax.fori_loop(bigs - LAG, bigs, sent, 0)
    for g in range(bigs * BIG, groups):
        for k in range(CORES):
            small(g, k, core).wait_send()

    @pl.when(away)
    def _():
        hand.wait_send()
        straight.wait_send()
        for d in range(1, 4):
            spread(2, d).wait_send()

    @pl.when(home)
    def _():
        cross.wait_send()
        for t in range(2):
            for d in range(1, 4):
                spread(t, d).wait_send()

    for j in range(CORES):
        for t in range(2):
            forward(t, j).wait_send()

    lax.fori_loop(steps + 1 - LAG, groups, drained, 0)


def write_out(src, dst, sem):
    parts = sem.shape[0]
    n = src.shape[0] // parts
    copies = [pltpu.make_async_copy(src.at[pl.ds(i * n, n)], dst.at[pl.ds(i * n, n)], sem.at[i]) for i in range(parts)]
    for c in copies:
        c.start()
    for c in copies:
        c.wait()


def solution(mesh):
    tile_spec = P(('dp', 'row'), 'col', None)

    def per_device(pair_tile, res_mask, ln_gamma, ln_beta, w_q, w_k, w_v, w_b, w_g, w_o):
        row_len, width, chan = pair_tile.shape
        heads, proj = w_b.shape[1], w_q.shape[1]
        hd = proj // heads
        rows, n_q = row_len // CORES, CORES * width
        n_k = mesh.shape['col'] * width
        groups = rows // STEP_ROWS
        vmem = pltpu.VMEM
        dma = pltpu.SemaphoreType.DMA
        pairs = lambda *s: [vmem(*s)] * 2
        whole = pl.BlockSpec(memory_space=pltpu.VMEM)
        hbm = pl.BlockSpec(memory_space=pltpu.HBM)
        smalls = (res_mask.reshape(1, -1), ln_gamma.reshape(1, -1), ln_beta.reshape(1, -1), w_q, w_k, w_v, w_b.T, w_g, w_o)
        result = pl.pallas_call(
            functools.partial(kernel, heads),
            in_specs=[hbm] * (1 + len(smalls)),
            out_specs=whole,
            out_shape=pltpu.VMEM(pair_tile.shape, BF16),
            scratch_shapes=[
                *[vmem(w.shape, w.dtype) for w in smalls], vmem((3 * proj, chan), BF16),
                vmem((rows, n_k, chan), BF16), vmem((row_len, width, chan), BF16), vmem((rows, width, chan), BF16),
                vmem((heads, n_k, n_q), F32), vmem((8, heads, width, width), BF16), *pairs((heads, width, width), BF16),
                vmem((heads, width, width), F32),
                *pairs((n_k, chan), BF16), *pairs((n_k, proj), BF16), *pairs((proj, n_k), BF16),
                *pairs((proj, n_q), BF16), *pairs((proj, n_q), F32),
                *[vmem((n_k, n_q), F32)] * 8, *pairs((proj, n_q), BF16),
                pltpu.SemaphoreType.REGULAR((2,)), dma((len(smalls),)), dma((2,)), dma, dma, dma((CORES, groups)), dma((CORES, groups)), dma((3,)), dma((3,)), dma((3, 3)), dma((3, CORES)),
                dma((2, CORES)), dma((2, CORES)), dma((groups,)), dma((groups,)),
            ],
            compiler_params=pltpu.CompilerParams(collective_id=0, has_side_effects=True, vmem_limit_bytes=58_000_000),
        )(pair_tile, *smalls)
        return pl.pallas_call(
            write_out,
            in_specs=[pl.BlockSpec(memory_space=pl.ANY)],
            out_specs=hbm,
            out_shape=jax.ShapeDtypeStruct(pair_tile.shape, BF16),
            scratch_shapes=[dma((4,))],
            compiler_params=pltpu.CompilerParams(vmem_limit_bytes=4 * 1024 * 1024),
        )(result)

    return jax.shard_map(per_device, mesh=mesh, in_specs=(tile_spec, P('dp'), P(), P(), P(), P(), P(), P(), P(), P()), out_specs=tile_spec, check_vma=False)
```

```python
import functools

import jax
import jax.numpy as jnp
from jax import lax
from jax.experimental import pallas as pl
from jax.experimental.pallas import tpu as pltpu
from jax.sharding import PartitionSpec as P

LN_EPS = 1e-5
F32 = jnp.float32
BF16 = jnp.bfloat16
NT = (((1,), (1,)), ((), ()))
TN = (((0,), (0,)), ((), ()))
LOG2E = 1.4426950408889634
CORES = 2
STEP_ROWS = 2
BIG = 2
SMALL_ROWS = 8
LAST_ROWS = 4
STRAIGHT = 1
SMALLS = 9
LAG = 6
EARLY = 3


def layer_norm(z, gamma, beta):
    x = z.astype(F32)
    centered = x - jnp.mean(x, axis=-1, keepdims=True)
    var = jnp.mean(jnp.square(centered), axis=-1, keepdims=True)
    return (centered * lax.rsqrt(var + LN_EPS) * gamma + beta).astype(BF16)


def over_keys(x, op):
    n, width = x.shape
    groups = 8
    t = op(x.reshape(groups, n // 8 // groups, 8, width), axis=1)
    return op(op(t, axis=0), axis=0, keepdims=True)


def kernel(heads, z_hbm, *refs):
    body(heads, z_hbm, refs[:SMALLS], refs[SMALLS + 1:2 * SMALLS + 1], refs[SMALLS], *refs[2 * SMALLS + 1:])


def body(heads, z_hbm, small_hbm, small_refs, out_ref,
           wt_ref, zbuf, own, outv, bias, btile, bsend, relay, brow, a0, a1, k0, k1, v0, v1, q0, q1, g0, g1,
           s0, s1, s2, s3, s4, s5, s6, s7, go0, go1, st0, st1, pa0, pa1,
           round_sem, small_sem, local_sem, zp_send, zp_recv, zs_send, zs_recv, b1_send, b1_recv, b2_send, b2_recv,
           b3_send, b3_recv, o_send, o_recv):
    mask_ref, gamma_ref, beta_ref, wq_ref, wk_ref, wv_ref, wbt_ref, wg_ref, wo_ref = small_refs
    rows_all, width, chan = z_hbm.shape
    rows = rows_all // CORES
    n_q = CORES * width
    proj = wk_ref.shape[1]
    hd = proj // heads
    groups = rows // STEP_ROWS
    steps = (rows - LAST_ROWS) // STEP_ROWS
    dp, row, col = lax.axis_index('dp'), lax.axis_index('row'), lax.axis_index('col')
    n_row = lax.axis_size('row')
    core, chip = lax.rem(col, CORES), col // CORES
    partner = chip * CORES + 1 - core
    far = (1 - chip) * CORES
    home_chip = row // CORES
    jslot = lax.rem(row, CORES)
    home = chip == home_chip

    def remote(src, dst, send, recv, r, c):
        return pltpu.make_async_remote_copy(src, dst, send, recv, device_id=(dp, r, c),
                                            device_id_type=pl.DeviceIdType.MESH)

    def signal(sem, r, c):
        pl.semaphore_signal(sem, inc=1, device_id=(dp, r, c), device_id_type=pl.DeviceIdType.MESH)

    def tell_next_rows(sem):
        @pl.when(row > 0)
        def _():
            signal(sem, jnp.maximum(row, 1) - 1, col)

        @pl.when(row < n_row - 1)
        def _():
            signal(sem, jnp.minimum(row, n_row - 2) + 1, col)

    next_rows = jnp.where(row > 0, 1, 0) + jnp.where(row < n_row - 1, 1, 0)

    barrier = pltpu.get_barrier_semaphore()
    for c in (partner, far, far + 1):
        signal(barrier, row, c)
    tell_next_rows(barrier)

    own_copy = pltpu.make_async_copy(z_hbm, own, local_sem.at[0])
    own_copy.start()
    mine_at = pl.ds(pl.multiple_of(core * width, width), width)
    theirs_at = pl.ds(pl.multiple_of((1 - core) * width, width), width)
    z_copy = pltpu.make_async_copy(z_hbm.at[pl.ds(core * rows, rows)], zbuf.at[:, mine_at, :], local_sem.at[1])
    z_copy.start()
    pl.semaphore_wait(barrier, 3 + next_rows)

    to_partner = remote(z_hbm.at[pl.ds((1 - core) * rows, rows)], zbuf.at[:, mine_at, :], zp_send, zp_recv, row, partner)

    bigs = (rows - SMALL_ROWS) // (BIG * STEP_ROWS)

    def z_copy_of(i, n, at_row, k, slot, c):
        at = pl.ds(pl.multiple_of((CORES + slot) * width, width), width)
        return remote(z_hbm.at[pl.ds(k * rows + at_row, n)], zbuf.at[pl.ds(at_row, n), at, :],
                      zs_send.at[k, i], zs_recv.at[slot, i], row, far + c)

    def big(i, k, slot):
        n = BIG * STEP_ROWS
        return z_copy_of(i, n, i * n, k, slot, k)

    def small(g, k, slot):
        return z_copy_of(bigs + g - bigs * BIG, STEP_ROWS, g * STEP_ROWS, k, slot, k)

    def send_step(i, carry):
        for k in range(CORES):
            big(i, k, core).start()
        return carry

    def z_wait(g):
        @pl.when(jnp.logical_and(g < bigs * BIG, lax.rem(g, BIG) == 0))
        def _():
            for k in range(CORES):
                big(jnp.minimum(g, bigs * BIG - 1) // BIG, k, k).wait_recv()

        @pl.when(g >= bigs * BIG)
        def _():
            for k in range(CORES):
                small(jnp.maximum(g, bigs * BIG), k, k).wait_recv()

    lax.fori_loop(0, EARLY, send_step, 0)
    to_partner.start()
    small_copies = [pltpu.make_async_copy(src, dst, small_sem.at[i]) for i, (src, dst) in enumerate(zip(small_hbm, small_refs))]
    for c in small_copies:
        c.start()
    for c in small_copies:
        c.wait()
    for i, w in enumerate((wv_ref, wq_ref, wg_ref)):
        wt_ref[i * proj:(i + 1) * proj] = w[...].T

    own_copy.wait()
    batch = 16
    mean_of = jnp.full((chan, chan), 1 / chan, BF16)

    def bias_step(i, carry):
        z = own[pl.ds(i * batch, batch)].reshape(batch * width, chan)
        centered = z.astype(F32) - jnp.dot(z, mean_of, preferred_element_type=F32)
        var = jnp.mean(jnp.square(centered), axis=-1, keepdims=True)
        a = (centered * lax.rsqrt(var + LN_EPS) * gamma_ref[...] + beta_ref[...]).astype(BF16)
        t = lax.dot_general(wbt_ref[...], a, NT, preferred_element_type=F32)
        for j in range(batch):
            for h in range(heads):
                brow[h, pl.ds(i * batch + j, 1), :] = t[h:h + 1, j * width:(j + 1) * width]
        return carry

    lax.fori_loop(0, rows_all // batch, bias_step, 0)
    home_slot = core * CORES + jslot
    for h in range(heads):
        tile = brow[h].T.astype(BF16)
        bsend[h] = tile

        @pl.when(home)
        def _():
            btile[home_slot, h] = tile

    for i in range(2):
        tell_next_rows(round_sem.at[i])
        pl.semaphore_wait(round_sem.at[i], next_rows)

    masks = []
    for s in range(2 * CORES):
        block = chip * CORES + s if s < CORES else far + s - CORES
        m = mask_ref[:, pl.ds(pl.multiple_of(block * width, width), width)]
        masks.append(jnp.broadcast_to(jnp.where(m > 0, 0.0, -1e9).astype(F32), (width, width)).T)

    paired = lax.rem(row + CORES, n_row)
    parts = (slice(0, heads), slice(0, STRAIGHT), slice(STRAIGHT, heads))
    of = lambda ref, t: ref.at[pl.ds(parts[t].start, parts[t].stop - parts[t].start)]
    tile_of = lambda slot, t: of(btile.at[slot], t)
    cross_slot = (CORES + core) * CORES + jslot
    straight = remote(of(bsend, 1), tile_of(cross_slot, 1), b1_send.at[0], b1_recv.at[0], row, far + core)
    hand = remote(of(bsend, 2), of(relay, 2), b1_send.at[1], b1_recv.at[1], paired, col)
    cross = remote(of(relay, 2), tile_of(cross_slot, 2), b1_send.at[2], b1_recv.at[2], row, far + core)
    away = jnp.logical_not(home)

    def spread(t, d):
        slot = home_slot if t == 0 else cross_slot
        return remote(bsend if t == 0 else tile_of(slot, t), tile_of(slot, t), b2_send.at[t, d - 1], b2_recv.at[t, jslot],
                      lax.rem(row + d, n_row), col)

    @pl.when(away)
    def _():
        hand.start()
        straight.start()

    @pl.when(home)
    def _():
        for d in range(1, 4):
            spread(0, d).start()
        hand.wait_recv()
        cross.start()

    lax.fori_loop(EARLY, bigs, send_step, 0)
    for g in range(bigs * BIG, groups):
        for k in range(CORES):
            small(g, k, core).start()

    @pl.when(home)
    def _():
        straight.wait_recv()
        for d in range(1, 4):
            spread(1, d).start()

    @pl.when(away)
    def _():
        cross.wait_recv()
        for d in range(1, 4):
            spread(2, d).start()

    def forward(t, j):
        slot = (core + CORES * t) * CORES + j
        return remote(btile.at[slot], btile.at[slot], b3_send.at[t, j], b3_recv.at[t, j], row, partner)

    for t in range(2):
        for j in range(CORES):
            slot = (core + CORES * t) * CORES + j
            for part, source in ((0, chip * CORES + j),) if t == 0 else ((1, chip * CORES + j), (2, far + j)):

                @pl.when(row != source)
                def _():
                    remote(of(bsend, part), tile_of(slot, part), b1_send.at[0], b2_recv.at[part, j], row, partner).wait_recv()

            forward(t, j).start()
    for j in range(CORES):
        for t in range(2):
            slot = (1 - core + CORES * t) * CORES + j
            remote(bsend, btile.at[slot], b1_send.at[0], b3_recv.at[t, j], row, partner).wait_recv()

    for s in range(2 * CORES):
        for j in range(CORES):
            for h in range(heads):
                b = btile[s * CORES + j, h].astype(F32)
                bias[h, s * width:(s + 1) * width, j * width:(j + 1) * width] = (b + masks[s]) * LOG2E

    a_s, k_s, v_s, q_s, g_s = (a0, a1), (k0, k1), (v0, v1), (q0, q1), (g0, g1)
    sc, go, stats, partial = ((s0, s1, s2, s3), (s4, s5, s6, s7)), (go0, go1), (st0, st1), (pa0, pa1)
    scale = hd ** -0.5 * LOG2E

    every, near, distant = slice(0, 2 * n_q), slice(0, n_q), slice(n_q, 2 * n_q)

    def scores(slot, h, dst, keys=every):
        part = q_s[slot][h * hd:(h + 1) * hd, :]
        none = jnp.zeros_like(part)
        rhs = jnp.concatenate([part if i == h else none for i in range(heads)], axis=0)
        dst[h][keys, :] = jnp.dot(k_s[slot][keys, :], rhs, preferred_element_type=F32) + bias[h, keys, :]

    def finish(r, src):
        for at, dst, i in ((theirs_at, outv, r), (mine_at, out_ref, core * rows + r)):
            upd = lax.dot_general(src[:, at], wo_ref[...], TN, preferred_element_type=F32)
            dst[i] = (zbuf[r, at].astype(F32) + upd).astype(BF16)

    def out_copy(g):
        return remote(outv.at[pl.ds(g * STEP_ROWS, STEP_ROWS)], out_ref.at[pl.ds(core * rows + g * STEP_ROWS, STEP_ROWS)],
                      o_send.at[g], o_recv.at[g], row, partner)

    def norm(r, slot, keys=every):
        a_s[slot][keys, :] = layer_norm(zbuf[r, keys, :], gamma_ref[...], beta_ref[...])

    def keys_of(slot, keys=every):
        k_s[slot][keys, :] = jnp.dot(a_s[slot][keys, :], wk_ref[...], preferred_element_type=F32).astype(BF16)

    def values_of(slot, keys=every):
        t = lax.dot_general(wt_ref[:proj], a_s[slot][keys, :], NT, preferred_element_type=F32)
        v_s[slot][:, keys] = t.astype(BF16)

    def queries_of(slot):
        t = lax.dot_general(wt_ref[proj:2 * proj], a_s[slot][near, :], NT, preferred_element_type=F32)
        q_s[slot][...] = (t * scale).astype(BF16)

    def gates_of(slot):
        t = lax.dot_general(wt_ref[2 * proj:], a_s[slot][near, :], NT, preferred_element_type=F32)
        g_s[slot][...] = jax.nn.sigmoid(t)

    def attend(h, slot, src, dst):
        s = src[h][...]
        p = jnp.exp2(s - over_keys(s, jnp.max))
        total = over_keys(p, jnp.sum)
        at = slice(h * hd, (h + 1) * hd)
        o = jnp.dot(v_s[slot][at, :], p.astype(BF16), preferred_element_type=F32)
        dst[at, :] = (g_s[slot][at, :] * (o / total)).astype(BF16)

    def sent(i, carry):
        for k in range(CORES):
            big(i, k, core).wait_send()
        return carry

    def drained(g, carry):
        out_copy(g).wait_send()
        remote(outv.at[pl.ds(0, STEP_ROWS)], out_ref.at[pl.ds((1 - core) * rows + g * STEP_ROWS, STEP_ROWS)],
               o_send.at[g], o_recv.at[g], row, partner).wait_recv()
        return carry

    def weigh(h, slot, keys, top):
        s = sc[slot][h][keys, :]
        m = over_keys(s, jnp.max)
        if top is not None:
            m = jnp.maximum(m, top)
        p = jnp.exp2(s - m)
        at = slice(h * hd, (h + 1) * hd)
        return m, over_keys(p, jnp.sum), jnp.dot(v_s[slot][at, keys], p.astype(BF16), preferred_element_type=F32)

    def attend_near(h, slot):
        m, total, o = weigh(h, slot, near, None)
        stats[slot][h:h + 1, :] = m
        stats[slot][heads + h:heads + h + 1, :] = total
        partial[slot][h * hd:(h + 1) * hd, :] = o

    def attend_distant(h, slot, dst):
        top = stats[slot][h:h + 1, :]
        m, total, o = weigh(h, slot, distant, top)
        rescale = jnp.exp2(top - m)
        at = slice(h * hd, (h + 1) * hd)
        o = partial[slot][at, :] * rescale + o
        total = stats[slot][heads + h:heads + h + 1, :] * rescale + total
        dst[at, :] = (g_s[slot][at, :] * (o / total)).astype(BF16)

    def step(i, carry):
        @pl.when(i < steps)
        def _():
            z_wait(i)

        @pl.when(i > 2)
        def _():
            out_copy(jnp.maximum(i, 3) - 3).start()

        for r in range(STEP_ROWS):
            cur, nxt = r, 1 - r
            finish(jnp.maximum(2 * i + r, 3) - 3, go[0])
            norm(jnp.minimum(2 * i + r, steps * STEP_ROWS - 1), cur)
            for h in range(heads):
                if h < 2:
                    scores(cur, h + 2, sc[0])
                else:
                    scores(nxt, h - 2, sc[0])
                if h == 0:
                    keys_of(nxt)
                    queries_of(nxt)
                if h == 1:
                    gates_of(nxt)
                if h == 2:
                    values_of(nxt)
                attend(h, cur, sc[0], go[0])
        return carry

    def last_rows(i, carry):
        both = range(STEP_ROWS)
        units = [(r, h) for r in both for h in range(heads)]
        out_copy(i - 1).start()
        for r in both:
            norm(i * STEP_ROWS + r, r, near)
        for r in both:
            keys_of(r, near)
            queries_of(r)
            gates_of(r)
            values_of(r, near)
        ahead = 2
        for r, h in units[:ahead]:
            scores(r, h, sc[r], near)
        for n, (r, h) in enumerate(units):
            for r2, h2 in units[n + ahead:n + ahead + 1]:
                scores(r2, h2, sc[r2], near)
            attend_near(h, r)
        z_wait(i)
        for r in both:
            norm(i * STEP_ROWS + r, r, distant)
        for r in both:
            keys_of(r, distant)
        for r, h in units[:ahead]:
            scores(r, h, sc[r], distant)
        for r in both:
            values_of(r, distant)
        for n, (r, h) in enumerate(units):
            for r2, h2 in units[n + ahead:n + ahead + 1]:
                scores(r2, h2, sc[r2], distant)
            attend_distant(h, r, go[r])
        for r in both:
            finish(i * STEP_ROWS + r, go[r])
        return carry

    z_copy.wait()
    remote(z_hbm.at[pl.ds(0, rows)], zbuf.at[:, theirs_at, :], zp_send, zp_recv, row, partner).wait_recv()
    lax.fori_loop(0, steps + 1, step, 0)
    finish(steps * STEP_ROWS - 1, go[0])
    out_copy(steps - 2).start()
    lax.fori_loop(0, bigs - LAG, sent, 0)
    lax.fori_loop(0, steps + 1 - LAG, drained, 0)
    lax.fori_loop(steps, groups, last_rows, 0)
    to_partner.wait_send()
    out_copy(groups - 1).start()
    lax.fori_loop(bigs - LAG, bigs, sent, 0)
    for g in range(bigs * BIG, groups):
        for k in range(CORES):
            small(g, k, core).wait_send()

    @pl.when(away)
    def _():
        hand.wait_send()
        straight.wait_send()
        for d in range(1, 4):
            spread(2, d).wait_send()

    @pl.when(home)
    def _():
        cross.wait_send()
        for t in range(2):
            for d in range(1, 4):
                spread(t, d).wait_send()

    for j in range(CORES):
        for t in range(2):
            forward(t, j).wait_send()

    lax.fori_loop(steps + 1 - LAG, groups, drained, 0)


def write_out(src, dst, sem):
    parts = sem.shape[0]
    n = src.shape[0] // parts
    copies = [pltpu.make_async_copy(src.at[pl.ds(i * n, n)], dst.at[pl.ds(i * n, n)], sem.at[i]) for i in range(parts)]
    for c in copies:
        c.start()
    for c in copies:
        c.wait()


def solution(mesh):
    tile_spec = P(('dp', 'row'), 'col', None)

    def per_device(pair_tile, res_mask, ln_gamma, ln_beta, w_q, w_k, w_v, w_b, w_g, w_o):
        row_len, width, chan = pair_tile.shape
        heads, proj = w_b.shape[1], w_q.shape[1]
        hd = proj // heads
        rows, n_q = row_len // CORES, CORES * width
        n_k = mesh.shape['col'] * width
        groups = rows // STEP_ROWS
        vmem = pltpu.VMEM
        dma = pltpu.SemaphoreType.DMA
        pairs = lambda *s: [vmem(*s)] * 2
        whole = pl.BlockSpec(memory_space=pltpu.VMEM)
        hbm = pl.BlockSpec(memory_space=pltpu.HBM)
        smalls = (res_mask.reshape(1, -1), ln_gamma.reshape(1, -1), ln_beta.reshape(1, -1), w_q, w_k, w_v, w_b.T, w_g, w_o)
        result = pl.pallas_call(
            functools.partial(kernel, heads),
            in_specs=[hbm] * (1 + len(smalls)),
            out_specs=whole,
            out_shape=pltpu.VMEM(pair_tile.shape, BF16),
            scratch_shapes=[
                *[vmem(w.shape, w.dtype) for w in smalls], vmem((3 * proj, chan), BF16),
                vmem((rows, n_k, chan), BF16), vmem((row_len, width, chan), BF16), vmem((rows, width, chan), BF16),
                vmem((heads, n_k, n_q), F32), vmem((8, heads, width, width), BF16), *pairs((heads, width, width), BF16),
                vmem((heads, width, width), F32),
                *pairs((n_k, chan), BF16), *pairs((n_k, proj), BF16), *pairs((proj, n_k), BF16),
                *pairs((proj, n_q), BF16), *pairs((proj, n_q), F32),
                *[vmem((n_k, n_q), F32)] * 8, *pairs((proj, n_q), BF16),
                *pairs((2 * heads, n_q), F32), *pairs((proj, n_q), F32),
                pltpu.SemaphoreType.REGULAR((2,)), dma((len(smalls),)), dma((2,)), dma, dma, dma((CORES, groups)), dma((CORES, groups)), dma((3,)), dma((3,)), dma((3, 3)), dma((3, CORES)),
                dma((2, CORES)), dma((2, CORES)), dma((groups,)), dma((groups,)),
            ],
            compiler_params=pltpu.CompilerParams(collective_id=0, has_side_effects=True, vmem_limit_bytes=58_000_000),
        )(pair_tile, *smalls)
        return pl.pallas_call(
            write_out,
            in_specs=[pl.BlockSpec(memory_space=pl.ANY)],
            out_specs=hbm,
            out_shape=jax.ShapeDtypeStruct(pair_tile.shape, BF16),
            scratch_shapes=[dma((4,))],
            compiler_params=pltpu.CompilerParams(vmem_limit_bytes=4 * 1024 * 1024),
        )(result)

    return jax.shard_map(per_device, mesh=mesh, in_specs=(tile_spec, P('dp'), P(), P(), P(), P(), P(), P(), P(), P()), out_specs=tile_spec, check_vma=False)
```

```python
import functools

import jax
import jax.numpy as jnp
from jax import lax
from jax.experimental import pallas as pl
from jax.experimental.pallas import tpu as pltpu
from jax.sharding import PartitionSpec as P

LN_EPS = 1e-5
F32 = jnp.float32
BF16 = jnp.bfloat16
NT = (((1,), (1,)), ((), ()))
TN = (((0,), (0,)), ((), ()))
LOG2E = 1.4426950408889634
CORES = 2
STEP_ROWS = 2
BIG = 2
SMALL_ROWS = 8
LAST_ROWS = 8
STRAIGHT = 1
SMALLS = 9
SETTLE = 26
SETTLED_Z = 11
SETTLED_OUT = 22
EARLY = 3


def layer_norm(z, gamma, beta):
    x = z.astype(F32)
    centered = x - jnp.mean(x, axis=-1, keepdims=True)
    var = jnp.mean(jnp.square(centered), axis=-1, keepdims=True)
    return (centered * lax.rsqrt(var + LN_EPS) * gamma + beta).astype(BF16)


def over_keys(x, op):
    n, width = x.shape
    groups = 8
    t = op(x.reshape(groups, n // 8 // groups, 8, width), axis=1)
    return op(op(t, axis=0), axis=0, keepdims=True)


def kernel(heads, z_hbm, *refs):
    body(heads, z_hbm, refs[:SMALLS], refs[SMALLS + 1:2 * SMALLS + 1], refs[SMALLS], *refs[2 * SMALLS + 1:])


def body(heads, z_hbm, small_hbm, small_refs, out_ref,
           wt_ref, zbuf, own, outv, bias, btile, bsend, relay, brow, a0, a1, k0, k1, v0, v1, q0, q1, g0, g1,
           s0, s1, s2, s3, s4, s5, s6, s7, go0, go1,
           round_sem, small_sem, local_sem, zp_send, zp_recv, zs_send, zs_recv, b1_send, b1_recv, b2_send, b2_recv,
           b3_send, b3_recv, o_send, o_recv):
    mask_ref, gamma_ref, beta_ref, wq_ref, wk_ref, wv_ref, wbt_ref, wg_ref, wo_ref = small_refs
    rows_all, width, chan = z_hbm.shape
    rows = rows_all // CORES
    n_q = CORES * width
    proj = wk_ref.shape[1]
    hd = proj // heads
    groups = rows // STEP_ROWS
    steps = (rows - LAST_ROWS) // STEP_ROWS
    dp, row, col = lax.axis_index('dp'), lax.axis_index('row'), lax.axis_index('col')
    n_row = lax.axis_size('row')
    core, chip = lax.rem(col, CORES), col // CORES
    partner = chip * CORES + 1 - core
    far = (1 - chip) * CORES
    home_chip = row // CORES
    jslot = lax.rem(row, CORES)
    home = chip == home_chip

    def remote(src, dst, send, recv, r, c):
        return pltpu.make_async_remote_copy(src, dst, send, recv, device_id=(dp, r, c),
                                            device_id_type=pl.DeviceIdType.MESH)

    def signal(sem, r, c):
        pl.semaphore_signal(sem, inc=1, device_id=(dp, r, c), device_id_type=pl.DeviceIdType.MESH)

    def tell_next_rows(sem):
        @pl.when(row > 0)
        def _():
            signal(sem, jnp.maximum(row, 1) - 1, col)

        @pl.when(row < n_row - 1)
        def _():
            signal(sem, jnp.minimum(row, n_row - 2) + 1, col)

    next_rows = jnp.where(row > 0, 1, 0) + jnp.where(row < n_row - 1, 1, 0)

    barrier = pltpu.get_barrier_semaphore()
    for c in (partner, far, far + 1):
        signal(barrier, row, c)
    tell_next_rows(barrier)

    own_copy = pltpu.make_async_copy(z_hbm, own, local_sem.at[0])
    own_copy.start()
    mine_at = pl.ds(pl.multiple_of(core * width, width), width)
    theirs_at = pl.ds(pl.multiple_of((1 - core) * width, width), width)
    z_copy = pltpu.make_async_copy(z_hbm.at[pl.ds(core * rows, rows)], zbuf.at[:, mine_at, :], local_sem.at[1])
    z_copy.start()
    pl.semaphore_wait(barrier, 3 + next_rows)

    to_partner = remote(z_hbm.at[pl.ds((1 - core) * rows, rows)], zbuf.at[:, mine_at, :], zp_send, zp_recv, row, partner)

    bigs = (rows - SMALL_ROWS) // (BIG * STEP_ROWS)

    def z_copy_of(i, n, at_row, k, slot, c):
        at = pl.ds(pl.multiple_of((CORES + slot) * width, width), width)
        return remote(z_hbm.at[pl.ds(k * rows + at_row, n)], zbuf.at[pl.ds(at_row, n), at, :],
                      zs_send.at[k, i], zs_recv.at[slot, i], row, far + c)

    def big(i, k, slot):
        n = BIG * STEP_ROWS
        return z_copy_of(i, n, i * n, k, slot, k)

    def small(g, k, slot):
        return z_copy_of(bigs + g - bigs * BIG, STEP_ROWS, g * STEP_ROWS, k, slot, k)

    def send_step(i, carry):
        for k in range(CORES):
            big(i, k, core).start()
        return carry

    def z_wait(g):
        @pl.when(jnp.logical_and(g < bigs * BIG, lax.rem(g, BIG) == 0))
        def _():
            for k in range(CORES):
                big(jnp.minimum(g, bigs * BIG - 1) // BIG, k, k).wait_recv()

        @pl.when(g >= bigs * BIG)
        def _():
            for k in range(CORES):
                small(jnp.maximum(g, bigs * BIG), k, k).wait_recv()

    lax.fori_loop(0, EARLY, send_step, 0)
    to_partner.start()
    small_copies = [pltpu.make_async_copy(src, dst, small_sem.at[i]) for i, (src, dst) in enumerate(zip(small_hbm, small_refs))]
    for c in small_copies:
        c.start()
    for c in small_copies:
        c.wait()
    for i, w in enumerate((wv_ref, wq_ref, wg_ref)):
        wt_ref[i * proj:(i + 1) * proj] = w[...].T

    own_copy.wait()
    batch = 16
    mean_of = jnp.full((chan, chan), 1 / chan, BF16)

    def bias_step(i, carry):
        z = own[pl.ds(i * batch, batch)].reshape(batch * width, chan)
        centered = z.astype(F32) - jnp.dot(z, mean_of, preferred_element_type=F32)
        var = jnp.mean(jnp.square(centered), axis=-1, keepdims=True)
        a = (centered * lax.rsqrt(var + LN_EPS) * gamma_ref[...] + beta_ref[...]).astype(BF16)
        t = lax.dot_general(wbt_ref[...], a, NT, preferred_element_type=F32)
        for j in range(batch):
            for h in range(heads):
                brow[h, pl.ds(i * batch + j, 1), :] = t[h:h + 1, j * width:(j + 1) * width]
        return carry

    lax.fori_loop(0, rows_all // batch, bias_step, 0)
    home_slot = core * CORES + jslot
    for h in range(heads):
        tile = brow[h].T.astype(BF16)
        bsend[h] = tile

        @pl.when(home)
        def _():
            btile[home_slot, h] = tile

    for i in range(2):
        tell_next_rows(round_sem.at[i])
        pl.semaphore_wait(round_sem.at[i], next_rows)

    masks = []
    for s in range(2 * CORES):
        block = chip * CORES + s if s < CORES else far + s - CORES
        m = mask_ref[:, pl.ds(pl.multiple_of(block * width, width), width)]
        masks.append(jnp.broadcast_to(jnp.where(m > 0, 0.0, -1e9).astype(F32), (width, width)).T)

    paired = lax.rem(row + CORES, n_row)
    parts = (slice(0, heads), slice(0, STRAIGHT), slice(STRAIGHT, heads))
    of = lambda ref, t: ref.at[pl.ds(parts[t].start, parts[t].stop - parts[t].start)]
    tile_of = lambda slot, t: of(btile.at[slot], t)
    cross_slot = (CORES + core) * CORES + jslot
    straight = remote(of(bsend, 1), tile_of(cross_slot, 1), b1_send.at[0], b1_recv.at[0], row, far + core)
    hand = remote(of(bsend, 2), of(relay, 2), b1_send.at[1], b1_recv.at[1], paired, col)
    cross = remote(of(relay, 2), tile_of(cross_slot, 2), b1_send.at[2], b1_recv.at[2], row, far + core)
    away = jnp.logical_not(home)

    def spread(t, d):
        slot = home_slot if t == 0 else cross_slot
        return remote(bsend if t == 0 else tile_of(slot, t), tile_of(slot, t), b2_send.at[t, d - 1], b2_recv.at[t, jslot],
                      lax.rem(row + d, n_row), col)

    @pl.when(away)
    def _():
        hand.start()
        straight.start()

    @pl.when(home)
    def _():
        for d in range(1, 4):
            spread(0, d).start()
        hand.wait_recv()
        cross.start()

    lax.fori_loop(EARLY, bigs, send_step, 0)
    for g in range(bigs * BIG, groups):
        for k in range(CORES):
            small(g, k, core).start()

    @pl.when(home)
    def _():
        straight.wait_recv()
        for d in range(1, 4):
            spread(1, d).start()

    @pl.when(away)
    def _():
        cross.wait_recv()
        for d in range(1, 4):
            spread(2, d).start()

    def forward(t, j):
        slot = (core + CORES * t) * CORES + j
        return remote(btile.at[slot], btile.at[slot], b3_send.at[t, j], b3_recv.at[t, j], row, partner)

    for t in range(2):
        for j in range(CORES):
            slot = (core + CORES * t) * CORES + j
            for part, source in ((0, chip * CORES + j),) if t == 0 else ((1, chip * CORES + j), (2, far + j)):

                @pl.when(row != source)
                def _():
                    remote(of(bsend, part), tile_of(slot, part), b1_send.at[0], b2_recv.at[part, j], row, partner).wait_recv()

            forward(t, j).start()
    for j in range(CORES):
        for t in range(2):
            slot = (1 - core + CORES * t) * CORES + j
            remote(bsend, btile.at[slot], b1_send.at[0], b3_recv.at[t, j], row, partner).wait_recv()

    for s in range(2 * CORES):
        for j in range(CORES):
            for h in range(heads):
                b = btile[s * CORES + j, h].astype(F32)
                bias[h, s * width:(s + 1) * width, j * width:(j + 1) * width] = (b + masks[s]) * LOG2E

    a_s, k_s, v_s, q_s, g_s = (a0, a1), (k0, k1), (v0, v1), (q0, q1), (g0, g1)
    sc, go = ((s0, s1, s2, s3), (s4, s5, s6, s7)), (go0, go1)
    scale = hd ** -0.5 * LOG2E

    every, near, distant = slice(0, 2 * n_q), slice(0, n_q), slice(n_q, 2 * n_q)

    def scores(slot, h, dst, keys=every):
        part = q_s[slot][h * hd:(h + 1) * hd, :]
        none = jnp.zeros_like(part)
        rhs = jnp.concatenate([part if i == h else none for i in range(heads)], axis=0)
        dst[h][keys, :] = jnp.dot(k_s[slot][keys, :], rhs, preferred_element_type=F32) + bias[h, keys, :]

    def finish(r, src):
        for at, dst, i in ((theirs_at, outv, r), (mine_at, out_ref, core * rows + r)):
            upd = lax.dot_general(src[:, at], wo_ref[...], TN, preferred_element_type=F32)
            dst[i] = (zbuf[r, at].astype(F32) + upd).astype(BF16)

    def out_copy(g):
        return remote(outv.at[pl.ds(g * STEP_ROWS, STEP_ROWS)], out_ref.at[pl.ds(core * rows + g * STEP_ROWS, STEP_ROWS)],
                      o_send.at[g], o_recv.at[g], row, partner)

    def norm(r, slot, keys=every):
        a_s[slot][keys, :] = layer_norm(zbuf[r, keys, :], gamma_ref[...], beta_ref[...])

    def keys_of(slot, keys=every):
        k_s[slot][keys, :] = jnp.dot(a_s[slot][keys, :], wk_ref[...], preferred_element_type=F32).astype(BF16)

    def values_of(slot, keys=every):
        t = lax.dot_general(wt_ref[:proj], a_s[slot][keys, :], NT, preferred_element_type=F32)
        v_s[slot][:, keys] = t.astype(BF16)

    def queries_of(slot):
        t = lax.dot_general(wt_ref[proj:2 * proj], a_s[slot][near, :], NT, preferred_element_type=F32)
        q_s[slot][...] = (t * scale).astype(BF16)

    def gates_of(slot):
        t = lax.dot_general(wt_ref[2 * proj:], a_s[slot][near, :], NT, preferred_element_type=F32)
        g_s[slot][...] = jax.nn.sigmoid(t)

    def attend(h, slot, src, dst):
        s = src[h][...]
        p = jnp.exp2(s - over_keys(s, jnp.max))
        total = over_keys(p, jnp.sum)
        at = slice(h * hd, (h + 1) * hd)
        o = jnp.dot(v_s[slot][at, :], p.astype(BF16), preferred_element_type=F32)
        dst[at, :] = (g_s[slot][at, :] * (o / total)).astype(BF16)

    def sent(i, carry):
        for k in range(CORES):
            big(i, k, core).wait_send()
        return carry

    def drained(g, carry):
        out_copy(g).wait_send()
        remote(outv.at[pl.ds(0, STEP_ROWS)], out_ref.at[pl.ds((1 - core) * rows + g * STEP_ROWS, STEP_ROWS)],
               o_send.at[g], o_recv.at[g], row, partner).wait_recv()
        return carry

    def step(i, carry):
        @pl.when(i == SETTLE)
        def _():
            lax.fori_loop(0, SETTLED_Z, sent, 0)
            lax.fori_loop(0, SETTLED_OUT, drained, 0)

        @pl.when(i < steps)
        def _():
            z_wait(i)

        @pl.when(i > 2)
        def _():
            out_copy(jnp.maximum(i, 3) - 3).start()

        for r in range(STEP_ROWS):
            cur, nxt = r, 1 - r
            finish(jnp.maximum(2 * i + r, 3) - 3, go[0])
            norm(jnp.minimum(2 * i + r, steps * STEP_ROWS - 1), cur)
            for h in range(heads):
                if h < 2:
                    scores(cur, h + 2, sc[0])
                else:
                    scores(nxt, h - 2, sc[0])
                if h == 0:
                    keys_of(nxt)
                    queries_of(nxt)
                if h == 1:
                    gates_of(nxt)
                if h == 2:
                    values_of(nxt)
                attend(h, cur, sc[0], go[0])
        return carry

    def last_rows(i, carry):
        both = range(STEP_ROWS)
        units = [(r, h) for r in both for h in range(heads)]
        out_copy(i - 1).start()
        for r in both:
            norm(i * STEP_ROWS + r, r, near)
        for r in both:
            keys_of(r, near)
            queries_of(r)
            gates_of(r)
            values_of(r, near)
        for r, h in units:
            scores(r, h, sc[r], near)
        z_wait(i)
        for r in both:
            norm(i * STEP_ROWS + r, r, distant)
        for r in both:
            keys_of(r, distant)
        ahead = 2
        for r, h in units[:ahead]:
            scores(r, h, sc[r], distant)
        for r in both:
            values_of(r, distant)
        for n, (r, h) in enumerate(units):
            for r2, h2 in units[n + ahead:n + ahead + 1]:
                scores(r2, h2, sc[r2], distant)
            attend(h, r, sc[r], go[r])
        for r in both:
            finish(i * STEP_ROWS + r, go[r])
        return carry

    z_copy.wait()
    remote(z_hbm.at[pl.ds(0, rows)], zbuf.at[:, theirs_at, :], zp_send, zp_recv, row, partner).wait_recv()
    lax.fori_loop(0, steps + 1, step, 0)
    finish(steps * STEP_ROWS - 1, go[0])
    out_copy(steps - 2).start()
    lax.fori_loop(steps, groups, last_rows, 0)
    to_partner.wait_send()
    out_copy(groups - 1).start()
    lax.fori_loop(SETTLED_Z, bigs, sent, 0)
    for g in range(bigs * BIG, groups):
        for k in range(CORES):
            small(g, k, core).wait_send()

    @pl.when(away)
    def _():
        hand.wait_send()
        straight.wait_send()
        for d in range(1, 4):
            spread(2, d).wait_send()

    @pl.when(home)
    def _():
        cross.wait_send()
        for t in range(2):
            for d in range(1, 4):
                spread(t, d).wait_send()

    for j in range(CORES):
        for t in range(2):
            forward(t, j).wait_send()

    lax.fori_loop(SETTLED_OUT, groups, drained, 0)


def write_out(src, dst, sem):
    parts = sem.shape[0]
    n = src.shape[0] // parts
    copies = [pltpu.make_async_copy(src.at[pl.ds(i * n, n)], dst.at[pl.ds(i * n, n)], sem.at[i]) for i in range(parts)]
    for c in copies:
        c.start()
    for c in copies:
        c.wait()


def solution(mesh):
    tile_spec = P(('dp', 'row'), 'col', None)

    def per_device(pair_tile, res_mask, ln_gamma, ln_beta, w_q, w_k, w_v, w_b, w_g, w_o):
        row_len, width, chan = pair_tile.shape
        heads, proj = w_b.shape[1], w_q.shape[1]
        hd = proj // heads
        rows, n_q = row_len // CORES, CORES * width
        n_k = mesh.shape['col'] * width
        groups = rows // STEP_ROWS
        vmem = pltpu.VMEM
        dma = pltpu.SemaphoreType.DMA
        pairs = lambda *s: [vmem(*s)] * 2
        whole = pl.BlockSpec(memory_space=pltpu.VMEM)
        hbm = pl.BlockSpec(memory_space=pltpu.HBM)
        smalls = (res_mask.reshape(1, -1), ln_gamma.reshape(1, -1), ln_beta.reshape(1, -1), w_q, w_k, w_v, w_b.T, w_g, w_o)
        result = pl.pallas_call(
            functools.partial(kernel, heads),
            in_specs=[hbm] * (1 + len(smalls)),
            out_specs=whole,
            out_shape=pltpu.VMEM(pair_tile.shape, BF16),
            scratch_shapes=[
                *[vmem(w.shape, w.dtype) for w in smalls], vmem((3 * proj, chan), BF16),
                vmem((rows, n_k, chan), BF16), vmem((row_len, width, chan), BF16), vmem((rows, width, chan), BF16),
                vmem((heads, n_k, n_q), F32), vmem((8, heads, width, width), BF16), *pairs((heads, width, width), BF16),
                vmem((heads, width, width), F32),
                *pairs((n_k, chan), BF16), *pairs((n_k, proj), BF16), *pairs((proj, n_k), BF16),
                *pairs((proj, n_q), BF16), *pairs((proj, n_q), F32),
                *[vmem((n_k, n_q), F32)] * 8, *pairs((proj, n_q), BF16),
                pltpu.SemaphoreType.REGULAR((2,)), dma((len(smalls),)), dma((2,)), dma, dma, dma((CORES, groups)), dma((CORES, groups)), dma((3,)), dma((3,)), dma((3, 3)), dma((3, CORES)),
                dma((2, CORES)), dma((2, CORES)), dma((groups,)), dma((groups,)),
            ],
            compiler_params=pltpu.CompilerParams(collective_id=0, has_side_effects=True, vmem_limit_bytes=58_000_000),
        )(pair_tile, *smalls)
        return pl.pallas_call(
            write_out,
            in_specs=[pl.BlockSpec(memory_space=pl.ANY)],
            out_specs=hbm,
            out_shape=jax.ShapeDtypeStruct(pair_tile.shape, BF16),
            scratch_shapes=[dma((4,))],
            compiler_params=pltpu.CompilerParams(vmem_limit_bytes=4 * 1024 * 1024),
        )(result)

    return jax.shard_map(per_device, mesh=mesh, in_specs=(tile_spec, P('dp'), P(), P(), P(), P(), P(), P(), P(), P()), out_specs=tile_spec, check_vma=False)
```

```python
import functools

import jax
import jax.numpy as jnp
from jax import lax
from jax.experimental import pallas as pl
from jax.experimental.pallas import tpu as pltpu
from jax.sharding import PartitionSpec as P

LN_EPS = 1e-5
F32 = jnp.float32
BF16 = jnp.bfloat16
NT = (((1,), (1,)), ((), ()))
TN = (((0,), (0,)), ((), ()))
LOG2E = 1.4426950408889634
CORES = 2
STEP_ROWS = 2
BIG = 2
SMALL_ROWS = 8
LAST_ROWS = 2
STRAIGHT = 1
SMALLS = 9
EARLY = 3


def layer_norm(z, gamma, beta):
    x = z.astype(F32)
    centered = x - jnp.mean(x, axis=-1, keepdims=True)
    var = jnp.mean(jnp.square(centered), axis=-1, keepdims=True)
    return (centered * lax.rsqrt(var + LN_EPS) * gamma + beta).astype(BF16)


def over_keys(x, op):
    n, width = x.shape
    groups = 8
    t = op(x.reshape(groups, n // 8 // groups, 8, width), axis=1)
    return op(op(t, axis=0), axis=0, keepdims=True)


def kernel(heads, z_hbm, *refs):
    body(heads, z_hbm, refs[:SMALLS], refs[SMALLS + 1:2 * SMALLS + 1], refs[SMALLS], *refs[2 * SMALLS + 1:])


def body(heads, z_hbm, small_hbm, small_refs, out_ref,
           wt_ref, zbuf, own, outv, bias, btile, bsend, relay, brow, a0, a1, k0, k1, v0, v1, q0, q1, g0, g1,
           s0, s1, s2, s3, s4, s5, s6, s7, go0, go1,
           round_sem, small_sem, local_sem, zp_send, zp_recv, zs_send, zs_recv, b1_send, b1_recv, b2_send, b2_recv,
           b3_send, b3_recv, o_send, o_recv):
    mask_ref, gamma_ref, beta_ref, wq_ref, wk_ref, wv_ref, wbt_ref, wg_ref, wo_ref = small_refs
    rows_all, width, chan = z_hbm.shape
    rows = rows_all // CORES
    n_q = CORES * width
    proj = wk_ref.shape[1]
    hd = proj // heads
    groups = rows // STEP_ROWS
    steps = (rows - LAST_ROWS) // STEP_ROWS
    dp, row, col = lax.axis_index('dp'), lax.axis_index('row'), lax.axis_index('col')
    n_row = lax.axis_size('row')
    core, chip = lax.rem(col, CORES), col // CORES
    partner = chip * CORES + 1 - core
    far = (1 - chip) * CORES
    home_chip = row // CORES
    jslot = lax.rem(row, CORES)
    home = chip == home_chip

    def remote(src, dst, send, recv, r, c):
        return pltpu.make_async_remote_copy(src, dst, send, recv, device_id=(dp, r, c),
                                            device_id_type=pl.DeviceIdType.MESH)

    def signal(sem, r, c):
        pl.semaphore_signal(sem, inc=1, device_id=(dp, r, c), device_id_type=pl.DeviceIdType.MESH)

    def tell_next_rows(sem):
        @pl.when(row > 0)
        def _():
            signal(sem, jnp.maximum(row, 1) - 1, col)

        @pl.when(row < n_row - 1)
        def _():
            signal(sem, jnp.minimum(row, n_row - 2) + 1, col)

    next_rows = jnp.where(row > 0, 1, 0) + jnp.where(row < n_row - 1, 1, 0)

    barrier = pltpu.get_barrier_semaphore()
    for c in (partner, far, far + 1):
        signal(barrier, row, c)
    tell_next_rows(barrier)

    own_copy = pltpu.make_async_copy(z_hbm, own, local_sem.at[0])
    own_copy.start()
    mine_at = pl.ds(pl.multiple_of(core * width, width), width)
    theirs_at = pl.ds(pl.multiple_of((1 - core) * width, width), width)
    z_copy = pltpu.make_async_copy(z_hbm.at[pl.ds(core * rows, rows)], zbuf.at[:, mine_at, :], local_sem.at[1])
    z_copy.start()
    pl.semaphore_wait(barrier, 3 + next_rows)

    to_partner = remote(z_hbm.at[pl.ds((1 - core) * rows, rows)], zbuf.at[:, mine_at, :], zp_send, zp_recv, row, partner)

    bigs = (rows - SMALL_ROWS) // (BIG * STEP_ROWS)

    def z_copy_of(i, n, at_row, k, slot, c):
        at = pl.ds(pl.multiple_of((CORES + slot) * width, width), width)
        return remote(z_hbm.at[pl.ds(k * rows + at_row, n)], zbuf.at[pl.ds(at_row, n), at, :],
                      zs_send.at[k, i], zs_recv.at[slot, i], row, far + c)

    def big(i, k, slot):
        n = BIG * STEP_ROWS
        return z_copy_of(i, n, i * n, k, slot, k)

    def small(g, k, slot):
        return z_copy_of(bigs + g - bigs * BIG, STEP_ROWS, g * STEP_ROWS, k, slot, k)

    def send_step(i, carry):
        for k in range(CORES):
            big(i, k, core).start()
        return carry

    def z_wait(g):
        @pl.when(jnp.logical_and(g < bigs * BIG, lax.rem(g, BIG) == 0))
        def _():
            for k in range(CORES):
                big(jnp.minimum(g, bigs * BIG - 1) // BIG, k, k).wait_recv()

        @pl.when(g >= bigs * BIG)
        def _():
            for k in range(CORES):
                small(jnp.maximum(g, bigs * BIG), k, k).wait_recv()

    lax.fori_loop(0, EARLY, send_step, 0)
    to_partner.start()
    small_copies = [pltpu.make_async_copy(src, dst, small_sem.at[i]) for i, (src, dst) in enumerate(zip(small_hbm, small_refs))]
    for c in small_copies:
        c.start()
    for c in small_copies:
        c.wait()
    for i, w in enumerate((wv_ref, wq_ref, wg_ref)):
        wt_ref[i * proj:(i + 1) * proj] = w[...].T

    own_copy.wait()
    batch = 16
    mean_of = jnp.full((chan, chan), 1 / chan, BF16)

    def bias_step(i, carry):
        z = own[pl.ds(i * batch, batch)].reshape(batch * width, chan)
        centered = z.astype(F32) - jnp.dot(z, mean_of, preferred_element_type=F32)
        var = jnp.mean(jnp.square(centered), axis=-1, keepdims=True)
        a = (centered * lax.rsqrt(var + LN_EPS) * gamma_ref[...] + beta_ref[...]).astype(BF16)
        t = lax.dot_general(wbt_ref[...], a, NT, preferred_element_type=F32)
        for j in range(batch):
            for h in range(heads):
                brow[h, pl.ds(i * batch + j, 1), :] = t[h:h + 1, j * width:(j + 1) * width]
        return carry

    lax.fori_loop(0, rows_all // batch, bias_step, 0)
    home_slot = core * CORES + jslot
    for h in range(heads):
        tile = brow[h].T.astype(BF16)
        bsend[h] = tile

        @pl.when(home)
        def _():
            btile[home_slot, h] = tile

    for i in range(2):
        tell_next_rows(round_sem.at[i])
        pl.semaphore_wait(round_sem.at[i], next_rows)

    masks = []
    for s in range(2 * CORES):
        block = chip * CORES + s if s < CORES else far + s - CORES
        m = mask_ref[:, pl.ds(pl.multiple_of(block * width, width), width)]
        masks.append(jnp.broadcast_to(jnp.where(m > 0, 0.0, -1e9).astype(F32), (width, width)).T)

    paired = lax.rem(row + CORES, n_row)
    parts = (slice(0, heads), slice(0, STRAIGHT), slice(STRAIGHT, heads))
    of = lambda ref, t: ref.at[pl.ds(parts[t].start, parts[t].stop - parts[t].start)]
    tile_of = lambda slot, t: of(btile.at[slot], t)
    cross_slot = (CORES + core) * CORES + jslot
    straight = remote(of(bsend, 1), tile_of(cross_slot, 1), b1_send.at[0], b1_recv.at[0], row, far + core)
    hand = remote(of(bsend, 2), of(relay, 2), b1_send.at[1], b1_recv.at[1], paired, col)
    cross = remote(of(relay, 2), tile_of(cross_slot, 2), b1_send.at[2], b1_recv.at[2], row, far + core)
    away = jnp.logical_not(home)

    def spread(t, d):
        slot = home_slot if t == 0 else cross_slot
        return remote(bsend if t == 0 else tile_of(slot, t), tile_of(slot, t), b2_send.at[t, d - 1], b2_recv.at[t, jslot],
                      lax.rem(row + d, n_row), col)

    @pl.when(away)
    def _():
        hand.start()
        straight.start()

    @pl.when(home)
    def _():
        for d in range(1, 4):
            spread(0, d).start()
        hand.wait_recv()
        cross.start()

    lax.fori_loop(EARLY, bigs, send_step, 0)
    for g in range(bigs * BIG, groups):
        for k in range(CORES):
            small(g, k, core).start()

    @pl.when(home)
    def _():
        straight.wait_recv()
        for d in range(1, 4):
            spread(1, d).start()

    @pl.when(away)
    def _():
        cross.wait_recv()
        for d in range(1, 4):
            spread(2, d).start()

    def forward(t, j):
        slot = (core + CORES * t) * CORES + j
        return remote(btile.at[slot], btile.at[slot], b3_send.at[t, j], b3_recv.at[t, j], row, partner)

    for t in range(2):
        for j in range(CORES):
            slot = (core + CORES * t) * CORES + j
            for part, source in ((0, chip * CORES + j),) if t == 0 else ((1, chip * CORES + j), (2, far + j)):

                @pl.when(row != source)
                def _():
                    remote(of(bsend, part), tile_of(slot, part), b1_send.at[0], b2_recv.at[part, j], row, partner).wait_recv()

            forward(t, j).start()
    for j in range(CORES):
        for t in range(2):
            slot = (1 - core + CORES * t) * CORES + j
            remote(bsend, btile.at[slot], b1_send.at[0], b3_recv.at[t, j], row, partner).wait_recv()

    for s in range(2 * CORES):
        for j in range(CORES):
            for h in range(heads):
                b = btile[s * CORES + j, h].astype(F32)
                bias[h, s * width:(s + 1) * width, j * width:(j + 1) * width] = (b + masks[s]) * LOG2E

    a_s, k_s, v_s, q_s, g_s = (a0, a1), (k0, k1), (v0, v1), (q0, q1), (g0, g1)
    sc, go = ((s0, s1, s2, s3), (s4, s5, s6, s7)), (go0, go1)
    scale = hd ** -0.5 * LOG2E

    every, near, distant = slice(0, 2 * n_q), slice(0, n_q), slice(n_q, 2 * n_q)

    def scores(slot, h, dst, keys=every):
        part = q_s[slot][h * hd:(h + 1) * hd, :]
        none = jnp.zeros_like(part)
        rhs = jnp.concatenate([part if i == h else none for i in range(heads)], axis=0)
        dst[h][keys, :] = jnp.dot(k_s[slot][keys, :], rhs, preferred_element_type=F32) + bias[h, keys, :]

    def finish(r, src):
        for at, dst, i in ((theirs_at, outv, r), (mine_at, out_ref, core * rows + r)):
            upd = lax.dot_general(src[:, at], wo_ref[...], TN, preferred_element_type=F32)
            dst[i] = (zbuf[r, at].astype(F32) + upd).astype(BF16)

    def out_copy(g):
        return remote(outv.at[pl.ds(g * STEP_ROWS, STEP_ROWS)], out_ref.at[pl.ds(core * rows + g * STEP_ROWS, STEP_ROWS)],
                      o_send.at[g], o_recv.at[g], row, partner)

    def norm(r, slot, keys=every):
        a_s[slot][keys, :] = layer_norm(zbuf[r, keys, :], gamma_ref[...], beta_ref[...])

    def keys_of(slot, keys=every):
        k_s[slot][keys, :] = jnp.dot(a_s[slot][keys, :], wk_ref[...], preferred_element_type=F32).astype(BF16)

    def values_of(slot, keys=every):
        t = lax.dot_general(wt_ref[:proj], a_s[slot][keys, :], NT, preferred_element_type=F32)
        v_s[slot][:, keys] = t.astype(BF16)

    def queries_of(slot):
        t = lax.dot_general(wt_ref[proj:2 * proj], a_s[slot][near, :], NT, preferred_element_type=F32)
        q_s[slot][...] = (t * scale).astype(BF16)

    def gates_of(slot):
        t = lax.dot_general(wt_ref[2 * proj:], a_s[slot][near, :], NT, preferred_element_type=F32)
        g_s[slot][...] = jax.nn.sigmoid(t)

    def attend(h, slot, src, dst):
        s = src[h][...]
        p = jnp.exp2(s - over_keys(s, jnp.max))
        total = over_keys(p, jnp.sum)
        at = slice(h * hd, (h + 1) * hd)
        o = jnp.dot(v_s[slot][at, :], p.astype(BF16), preferred_element_type=F32)
        dst[at, :] = (g_s[slot][at, :] * (o / total)).astype(BF16)

    def sent(i, carry):
        for k in range(CORES):
            big(i, k, core).wait_send()
        return carry

    def drained(g, carry):
        out_copy(g).wait_send()
        remote(outv.at[pl.ds(0, STEP_ROWS)], out_ref.at[pl.ds((1 - core) * rows + g * STEP_ROWS, STEP_ROWS)],
               o_send.at[g], o_recv.at[g], row, partner).wait_recv()
        return carry

    def step(i, carry):
        @pl.when(i < steps)
        def _():
            z_wait(i)

        @pl.when(i > 2)
        def _():
            out_copy(jnp.maximum(i, 3) - 3).start()

        for r in range(STEP_ROWS):
            cur, nxt = r, 1 - r
            finish(jnp.maximum(2 * i + r, 3) - 3, go[0])
            norm(jnp.minimum(2 * i + r, steps * STEP_ROWS - 1), cur)
            for h in range(heads):
                if h < 2:
                    scores(cur, h + 2, sc[0])
                else:
                    scores(nxt, h - 2, sc[0])
                if h == 0:
                    keys_of(nxt)
                    queries_of(nxt)
                if h == 1:
                    gates_of(nxt)
                if h == 2:
                    values_of(nxt)
                attend(h, cur, sc[0], go[0])
        return carry

    def last_rows(i, carry):
        both = range(STEP_ROWS)
        units = [(r, h) for r in both for h in range(heads)]
        out_copy(i - 1).start()
        for r in both:
            norm(i * STEP_ROWS + r, r, near)
        for r in both:
            keys_of(r, near)
            queries_of(r)
            gates_of(r)
            values_of(r, near)
        for r, h in units:
            scores(r, h, sc[r], near)
        z_wait(i)
        for r in both:
            norm(i * STEP_ROWS + r, r, distant)
        for r in both:
            keys_of(r, distant)
        ahead = 2
        for r, h in units[:ahead]:
            scores(r, h, sc[r], distant)
        for r in both:
            values_of(r, distant)
        for n, (r, h) in enumerate(units):
            for r2, h2 in units[n + ahead:n + ahead + 1]:
                scores(r2, h2, sc[r2], distant)
            attend(h, r, sc[r], go[r])
        for r in both:
            finish(i * STEP_ROWS + r, go[r])
        return carry

    z_copy.wait()
    remote(z_hbm.at[pl.ds(0, rows)], zbuf.at[:, theirs_at, :], zp_send, zp_recv, row, partner).wait_recv()
    lax.fori_loop(0, steps + 1, step, 0)
    finish(steps * STEP_ROWS - 1, go[0])
    out_copy(steps - 2).start()
    lax.fori_loop(steps, groups, last_rows, 0)
    to_partner.wait_send()
    out_copy(groups - 1).start()
    lax.fori_loop(0, bigs, sent, 0)
    for g in range(bigs * BIG, groups):
        for k in range(CORES):
            small(g, k, core).wait_send()

    @pl.when(away)
    def _():
        hand.wait_send()
        straight.wait_send()
        for d in range(1, 4):
            spread(2, d).wait_send()

    @pl.when(home)
    def _():
        cross.wait_send()
        for t in range(2):
            for d in range(1, 4):
                spread(t, d).wait_send()

    for j in range(CORES):
        for t in range(2):
            forward(t, j).wait_send()

    lax.fori_loop(0, groups, drained, 0)


def write_out(src, dst, sem):
    parts = sem.shape[0]
    n = src.shape[0] // parts
    copies = [pltpu.make_async_copy(src.at[pl.ds(i * n, n)], dst.at[pl.ds(i * n, n)], sem.at[i]) for i in range(parts)]
    for c in copies:
        c.start()
    for c in copies:
        c.wait()


def solution(mesh):
    tile_spec = P(('dp', 'row'), 'col', None)

    def per_device(pair_tile, res_mask, ln_gamma, ln_beta, w_q, w_k, w_v, w_b, w_g, w_o):
        row_len, width, chan = pair_tile.shape
        heads, proj = w_b.shape[1], w_q.shape[1]
        hd = proj // heads
        rows, n_q = row_len // CORES, CORES * width
        n_k = mesh.shape['col'] * width
        groups = rows // STEP_ROWS
        vmem = pltpu.VMEM
        dma = pltpu.SemaphoreType.DMA
        pairs = lambda *s: [vmem(*s)] * 2
        whole = pl.BlockSpec(memory_space=pltpu.VMEM)
        hbm = pl.BlockSpec(memory_space=pltpu.HBM)
        smalls = (res_mask.reshape(1, -1), ln_gamma.reshape(1, -1), ln_beta.reshape(1, -1), w_q, w_k, w_v, w_b.T, w_g, w_o)
        result = pl.pallas_call(
            functools.partial(kernel, heads),
            in_specs=[hbm] * (1 + len(smalls)),
            out_specs=whole,
            out_shape=pltpu.VMEM(pair_tile.shape, BF16),
            scratch_shapes=[
                *[vmem(w.shape, w.dtype) for w in smalls], vmem((3 * proj, chan), BF16),
                vmem((rows, n_k, chan), BF16), vmem((row_len, width, chan), BF16), vmem((rows, width, chan), BF16),
                vmem((heads, n_k, n_q), F32), vmem((8, heads, width, width), BF16), *pairs((heads, width, width), BF16),
                vmem((heads, width, width), F32),
                *pairs((n_k, chan), BF16), *pairs((n_k, proj), BF16), *pairs((proj, n_k), BF16),
                *pairs((proj, n_q), BF16), *pairs((proj, n_q), F32),
                *[vmem((n_k, n_q), F32)] * 8, *pairs((proj, n_q), BF16),
                pltpu.SemaphoreType.REGULAR((2,)), dma((len(smalls),)), dma((2,)), dma, dma, dma((CORES, groups)), dma((CORES, groups)), dma((3,)), dma((3,)), dma((3, 3)), dma((3, CORES)),
                dma((2, CORES)), dma((2, CORES)), dma((groups,)), dma((groups,)),
            ],
            compiler_params=pltpu.CompilerParams(collective_id=0, has_side_effects=True, vmem_limit_bytes=58_000_000),
        )(pair_tile, *smalls)
        return pl.pallas_call(
            write_out,
            in_specs=[pl.BlockSpec(memory_space=pl.ANY)],
            out_specs=hbm,
            out_shape=jax.ShapeDtypeStruct(pair_tile.shape, BF16),
            scratch_shapes=[dma((4,))],
            compiler_params=pltpu.CompilerParams(vmem_limit_bytes=4 * 1024 * 1024),
        )(result)

    return jax.shard_map(per_device, mesh=mesh, in_specs=(tile_spec, P('dp'), P(), P(), P(), P(), P(), P(), P(), P()), out_specs=tile_spec, check_vma=False)
```

```python
import functools

import jax
import jax.numpy as jnp
from jax import lax
from jax.experimental import pallas as pl
from jax.experimental.pallas import tpu as pltpu
from jax.sharding import PartitionSpec as P

LN_EPS = 1e-5
F32 = jnp.float32
BF16 = jnp.bfloat16
NT = (((1,), (1,)), ((), ()))
TN = (((0,), (0,)), ((), ()))
LOG2E = 1.4426950408889634
CORES = 2
STEP_ROWS = 2
BIG = 2
SMALL_ROWS = 8
LAST_ROWS = 4
STRAIGHT = 1
SMALLS = 9
SETTLE = 29
SETTLED_Z = 12
SETTLED_OUT = 24
EARLY = 3


def layer_norm(z, gamma, beta):
    x = z.astype(F32)
    centered = x - jnp.mean(x, axis=-1, keepdims=True)
    var = jnp.mean(jnp.square(centered), axis=-1, keepdims=True)
    return (centered * lax.rsqrt(var + LN_EPS) * gamma + beta).astype(BF16)


def over_keys(x, op):
    n, width = x.shape
    groups = 8
    t = op(x.reshape(groups, n // 8 // groups, 8, width), axis=1)
    return op(op(t, axis=0), axis=0, keepdims=True)


def kernel(heads, z_hbm, *refs):
    body(heads, z_hbm, refs[:SMALLS], refs[SMALLS + 1:2 * SMALLS + 1], refs[SMALLS], *refs[2 * SMALLS + 1:])


def body(heads, z_hbm, small_hbm, small_refs, out_ref,
           wt_ref, zbuf, own, outv, bias, btile, bsend, relay, brow, a0, a1, k0, k1, v0, v1, q0, q1, g0, g1,
           s0, s1, s2, s3, s4, s5, s6, s7, go0, go1,
           round_sem, small_sem, local_sem, zp_send, zp_recv, zs_send, zs_recv, b1_send, b1_recv, b2_send, b2_recv,
           b3_send, b3_recv, o_send, o_recv):
    mask_ref, gamma_ref, beta_ref, wq_ref, wk_ref, wv_ref, wbt_ref, wg_ref, wo_ref = small_refs
    rows_all, width, chan = z_hbm.shape
    rows = rows_all // CORES
    n_q = CORES * width
    proj = wk_ref.shape[1]
    hd = proj // heads
    groups = rows // STEP_ROWS
    steps = (rows - LAST_ROWS) // STEP_ROWS
    dp, row, col = lax.axis_index('dp'), lax.axis_index('row'), lax.axis_index('col')
    n_row = lax.axis_size('row')
    core, chip = lax.rem(col, CORES), col // CORES
    partner = chip * CORES + 1 - core
    far = (1 - chip) * CORES
    home_chip = row // CORES
    jslot = lax.rem(row, CORES)
    home = chip == home_chip

    def remote(src, dst, send, recv, r, c):
        return pltpu.make_async_remote_copy(src, dst, send, recv, device_id=(dp, r, c),
                                            device_id_type=pl.DeviceIdType.MESH)

    def signal(sem, r, c):
        pl.semaphore_signal(sem, inc=1, device_id=(dp, r, c), device_id_type=pl.DeviceIdType.MESH)

    def tell_next_rows(sem):
        @pl.when(row > 0)
        def _():
            signal(sem, jnp.maximum(row, 1) - 1, col)

        @pl.when(row < n_row - 1)
        def _():
            signal(sem, jnp.minimum(row, n_row - 2) + 1, col)

    next_rows = jnp.where(row > 0, 1, 0) + jnp.where(row < n_row - 1, 1, 0)

    barrier = pltpu.get_barrier_semaphore()
    for c in (partner, far, far + 1):
        signal(barrier, row, c)
    tell_next_rows(barrier)

    own_copy = pltpu.make_async_copy(z_hbm, own, local_sem.at[0])
    own_copy.start()
    mine_at = pl.ds(pl.multiple_of(core * width, width), width)
    theirs_at = pl.ds(pl.multiple_of((1 - core) * width, width), width)
    z_copy = pltpu.make_async_copy(z_hbm.at[pl.ds(core * rows, rows)], zbuf.at[:, mine_at, :], local_sem.at[1])
    z_copy.start()
    pl.semaphore_wait(barrier, 3 + next_rows)

    to_partner = remote(z_hbm.at[pl.ds((1 - core) * rows, rows)], zbuf.at[:, mine_at, :], zp_send, zp_recv, row, partner)

    bigs = (rows - SMALL_ROWS) // (BIG * STEP_ROWS)

    def z_copy_of(i, n, at_row, k, slot, c):
        at = pl.ds(pl.multiple_of((CORES + slot) * width, width), width)
        return remote(z_hbm.at[pl.ds(k * rows + at_row, n)], zbuf.at[pl.ds(at_row, n), at, :],
                      zs_send.at[k, i], zs_recv.at[slot, i], row, far + c)

    def big(i, k, slot):
        n = BIG * STEP_ROWS
        return z_copy_of(i, n, i * n, k, slot, k)

    def small(g, k, slot):
        return z_copy_of(bigs + g - bigs * BIG, STEP_ROWS, g * STEP_ROWS, k, slot, k)

    def send_step(i, carry):
        for k in range(CORES):
            big(i, k, core).start()
        return carry

    def z_wait(g):
        @pl.when(jnp.logical_and(g < bigs * BIG, lax.rem(g, BIG) == 0))
        def _():
            for k in range(CORES):
                big(jnp.minimum(g, bigs * BIG - 1) // BIG, k, k).wait_recv()

        @pl.when(g >= bigs * BIG)
        def _():
            for k in range(CORES):
                small(jnp.maximum(g, bigs * BIG), k, k).wait_recv()

    lax.fori_loop(0, EARLY, send_step, 0)
    to_partner.start()
    small_copies = [pltpu.make_async_copy(src, dst, small_sem.at[i]) for i, (src, dst) in enumerate(zip(small_hbm, small_refs))]
    for c in small_copies:
        c.start()
    for c in small_copies:
        c.wait()
    for i, w in enumerate((wv_ref, wq_ref, wg_ref)):
        wt_ref[i * proj:(i + 1) * proj] = w[...].T

    own_copy.wait()
    batch = 16
    mean_of = jnp.full((chan, chan), 1 / chan, BF16)

    def bias_step(i, carry):
        z = own[pl.ds(i * batch, batch)].reshape(batch * width, chan)
        centered = z.astype(F32) - jnp.dot(z, mean_of, preferred_element_type=F32)
        var = jnp.mean(jnp.square(centered), axis=-1, keepdims=True)
        a = (centered * lax.rsqrt(var + LN_EPS) * gamma_ref[...] + beta_ref[...]).astype(BF16)
        t = lax.dot_general(wbt_ref[...], a, NT, preferred_element_type=F32)
        for j in range(batch):
            for h in range(heads):
                brow[h, pl.ds(i * batch + j, 1), :] = t[h:h + 1, j * width:(j + 1) * width]
        return carry

    lax.fori_loop(0, rows_all // batch, bias_step, 0)
    home_slot = core * CORES + jslot
    for h in range(heads):
        tile = brow[h].T.astype(BF16)
        bsend[h] = tile

        @pl.when(home)
        def _():
            btile[home_slot, h] = tile

    for i in range(2):
        tell_next_rows(round_sem.at[i])
        pl.semaphore_wait(round_sem.at[i], next_rows)

    masks = []
    for s in range(2 * CORES):
        block = chip * CORES + s if s < CORES else far + s - CORES
        m = mask_ref[:, pl.ds(pl.multiple_of(block * width, width), width)]
        masks.append(jnp.broadcast_to(jnp.where(m > 0, 0.0, -1e9).astype(F32), (width, width)).T)

    paired = lax.rem(row + CORES, n_row)
    parts = (slice(0, heads), slice(0, STRAIGHT), slice(STRAIGHT, heads))
    of = lambda ref, t: ref.at[pl.ds(parts[t].start, parts[t].stop - parts[t].start)]
    tile_of = lambda slot, t: of(btile.at[slot], t)
    cross_slot = (CORES + core) * CORES + jslot
    straight = remote(of(bsend, 1), tile_of(cross_slot, 1), b1_send.at[0], b1_recv.at[0], row, far + core)
    hand = remote(of(bsend, 2), of(relay, 2), b1_send.at[1], b1_recv.at[1], paired, col)
    cross = remote(of(relay, 2), tile_of(cross_slot, 2), b1_send.at[2], b1_recv.at[2], row, far + core)
    away = jnp.logical_not(home)

    def spread(t, d):
        slot = home_slot if t == 0 else cross_slot
        return remote(bsend if t == 0 else tile_of(slot, t), tile_of(slot, t), b2_send.at[t, d - 1], b2_recv.at[t, jslot],
                      lax.rem(row + d, n_row), col)

    @pl.when(away)
    def _():
        hand.start()
        straight.start()

    @pl.when(home)
    def _():
        for d in range(1, 4):
            spread(0, d).start()
        hand.wait_recv()
        cross.start()

    lax.fori_loop(EARLY, bigs, send_step, 0)
    for g in range(bigs * BIG, groups):
        for k in range(CORES):
            small(g, k, core).start()

    @pl.when(home)
    def _():
        straight.wait_recv()
        for d in range(1, 4):
            spread(1, d).start()

    @pl.when(away)
    def _():
        cross.wait_recv()
        for d in range(1, 4):
            spread(2, d).start()

    def forward(t, j):
        slot = (core + CORES * t) * CORES + j
        return remote(btile.at[slot], btile.at[slot], b3_send.at[t, j], b3_recv.at[t, j], row, partner)

    for t in range(2):
        for j in range(CORES):
            slot = (core + CORES * t) * CORES + j
            for part, source in ((0, chip * CORES + j),) if t == 0 else ((1, chip * CORES + j), (2, far + j)):

                @pl.when(row != source)
                def _():
                    remote(of(bsend, part), tile_of(slot, part), b1_send.at[0], b2_recv.at[part, j], row, partner).wait_recv()

            forward(t, j).start()
    for j in range(CORES):
        for t in range(2):
            slot = (1 - core + CORES * t) * CORES + j
            remote(bsend, btile.at[slot], b1_send.at[0], b3_recv.at[t, j], row, partner).wait_recv()

    for s in range(2 * CORES):
        for j in range(CORES):
            for h in range(heads):
                b = btile[s * CORES + j, h].astype(F32)
                bias[h, s * width:(s + 1) * width, j * width:(j + 1) * width] = (b + masks[s]) * LOG2E

    a_s, k_s, v_s, q_s, g_s = (a0, a1), (k0, k1), (v0, v1), (q0, q1), (g0, g1)
    sc, go = ((s0, s1, s2, s3), (s4, s5, s6, s7)), (go0, go1)
    scale = hd ** -0.5 * LOG2E

    every, near, distant = slice(0, 2 * n_q), slice(0, n_q), slice(n_q, 2 * n_q)

    def scores(slot, h, dst, keys=every):
        part = q_s[slot][h * hd:(h + 1) * hd, :]
        none = jnp.zeros_like(part)
        rhs = jnp.concatenate([part if i == h else none for i in range(heads)], axis=0)
        dst[h][keys, :] = jnp.dot(k_s[slot][keys, :], rhs, preferred_element_type=F32) + bias[h, keys, :]

    def finish(r, src):
        for at, dst, i in ((theirs_at, outv, r), (mine_at, out_ref, core * rows + r)):
            upd = lax.dot_general(src[:, at], wo_ref[...], TN, preferred_element_type=F32)
            dst[i] = (zbuf[r, at].astype(F32) + upd).astype(BF16)

    def out_copy(g):
        return remote(outv.at[pl.ds(g * STEP_ROWS, STEP_ROWS)], out_ref.at[pl.ds(core * rows + g * STEP_ROWS, STEP_ROWS)],
                      o_send.at[g], o_recv.at[g], row, partner)

    def norm(r, slot, keys=every):
        a_s[slot][keys, :] = layer_norm(zbuf[r, keys, :], gamma_ref[...], beta_ref[...])

    def keys_of(slot, keys=every):
        k_s[slot][keys, :] = jnp.dot(a_s[slot][keys, :], wk_ref[...], preferred_element_type=F32).astype(BF16)

    def values_of(slot, keys=every):
        t = lax.dot_general(wt_ref[:proj], a_s[slot][keys, :], NT, preferred_element_type=F32)
        v_s[slot][:, keys] = t.astype(BF16)

    def queries_of(slot):
        t = lax.dot_general(wt_ref[proj:2 * proj], a_s[slot][near, :], NT, preferred_element_type=F32)
        q_s[slot][...] = (t * scale).astype(BF16)

    def gates_of(slot):
        t = lax.dot_general(wt_ref[2 * proj:], a_s[slot][near, :], NT, preferred_element_type=F32)
        g_s[slot][...] = jax.nn.sigmoid(t)

    def attend(h, slot, src, dst):
        s = src[h][...]
        p = jnp.exp2(s - over_keys(s, jnp.max))
        total = over_keys(p, jnp.sum)
        at = slice(h * hd, (h + 1) * hd)
        o = jnp.dot(v_s[slot][at, :], p.astype(BF16), preferred_element_type=F32)
        dst[at, :] = (g_s[slot][at, :] * (o / total)).astype(BF16)

    def sent(i, carry):
        for k in range(CORES):
            big(i, k, core).wait_send()
        return carry

    def drained(g, carry):
        out_copy(g).wait_send()
        remote(outv.at[pl.ds(0, STEP_ROWS)], out_ref.at[pl.ds((1 - core) * rows + g * STEP_ROWS, STEP_ROWS)],
               o_send.at[g], o_recv.at[g], row, partner).wait_recv()
        return carry

    def step(i, carry):
        @pl.when(i == SETTLE)
        def _():
            lax.fori_loop(0, SETTLED_Z, sent, 0)
            lax.fori_loop(0, SETTLED_OUT, drained, 0)

        @pl.when(i < steps)
        def _():
            z_wait(i)

        @pl.when(i > 2)
        def _():
            out_copy(jnp.maximum(i, 3) - 3).start()

        for r in range(STEP_ROWS):
            cur, nxt = r, 1 - r
            finish(jnp.maximum(2 * i + r, 3) - 3, go[0])
            norm(jnp.minimum(2 * i + r, steps * STEP_ROWS - 1), cur)
            for h in range(heads):
                if h < 2:
                    scores(cur, h + 2, sc[0])
                else:
                    scores(nxt, h - 2, sc[0])
                if h == 0:
                    keys_of(nxt)
                    queries_of(nxt)
                if h == 1:
                    gates_of(nxt)
                if h == 2:
                    values_of(nxt)
                attend(h, cur, sc[0], go[0])
        return carry

    def last_rows(i, carry):
        both = range(STEP_ROWS)
        units = [(r, h) for r in both for h in range(heads)]
        out_copy(i - 1).start()
        for r in both:
            norm(i * STEP_ROWS + r, r, near)
        for r in both:
            keys_of(r, near)
            queries_of(r)
            gates_of(r)
            values_of(r, near)
        for r, h in units:
            scores(r, h, sc[r], near)
        z_wait(i)
        for r in both:
            norm(i * STEP_ROWS + r, r, distant)
        for r in both:
            keys_of(r, distant)
        ahead = 2
        for r, h in units[:ahead]:
            scores(r, h, sc[r], distant)
        for r in both:
            values_of(r, distant)
        for n, (r, h) in enumerate(units):
            for r2, h2 in units[n + ahead:n + ahead + 1]:
                scores(r2, h2, sc[r2], distant)
            attend(h, r, sc[r], go[r])
        for r in both:
            finish(i * STEP_ROWS + r, go[r])
        return carry

    z_copy.wait()
    remote(z_hbm.at[pl.ds(0, rows)], zbuf.at[:, theirs_at, :], zp_send, zp_recv, row, partner).wait_recv()
    lax.fori_loop(0, steps + 1, step, 0)
    finish(steps * STEP_ROWS - 1, go[0])
    out_copy(steps - 2).start()
    lax.fori_loop(steps, groups, last_rows, 0)
    to_partner.wait_send()
    out_copy(groups - 1).start()
    lax.fori_loop(SETTLED_Z, bigs, sent, 0)
    for g in range(bigs * BIG, groups):
        for k in range(CORES):
            small(g, k, core).wait_send()

    @pl.when(away)
    def _():
        hand.wait_send()
        straight.wait_send()
        for d in range(1, 4):
            spread(2, d).wait_send()

    @pl.when(home)
    def _():
        cross.wait_send()
        for t in range(2):
            for d in range(1, 4):
                spread(t, d).wait_send()

    for j in range(CORES):
        for t in range(2):
            forward(t, j).wait_send()

    lax.fori_loop(SETTLED_OUT, groups, drained, 0)


def write_out(src, dst, sem):
    parts = sem.shape[0]
    n = src.shape[0] // parts
    copies = [pltpu.make_async_copy(src.at[pl.ds(i * n, n)], dst.at[pl.ds(i * n, n)], sem.at[i]) for i in range(parts)]
    for c in copies:
        c.start()
    for c in copies:
        c.wait()


def solution(mesh):
    tile_spec = P(('dp', 'row'), 'col', None)

    def per_device(pair_tile, res_mask, ln_gamma, ln_beta, w_q, w_k, w_v, w_b, w_g, w_o):
        row_len, width, chan = pair_tile.shape
        heads, proj = w_b.shape[1], w_q.shape[1]
        hd = proj // heads
        rows, n_q = row_len // CORES, CORES * width
        n_k = mesh.shape['col'] * width
        groups = rows // STEP_ROWS
        vmem = pltpu.VMEM
        dma = pltpu.SemaphoreType.DMA
        pairs = lambda *s: [vmem(*s)] * 2
        whole = pl.BlockSpec(memory_space=pltpu.VMEM)
        hbm = pl.BlockSpec(memory_space=pltpu.HBM)
        smalls = (res_mask.reshape(1, -1), ln_gamma.reshape(1, -1), ln_beta.reshape(1, -1), w_q, w_k, w_v, w_b.T, w_g, w_o)
        result = pl.pallas_call(
            functools.partial(kernel, heads),
            in_specs=[hbm] * (1 + len(smalls)),
            out_specs=whole,
            out_shape=pltpu.VMEM(pair_tile.shape, BF16),
            scratch_shapes=[
                *[vmem(w.shape, w.dtype) for w in smalls], vmem((3 * proj, chan), BF16),
                vmem((rows, n_k, chan), BF16), vmem((row_len, width, chan), BF16), vmem((rows, width, chan), BF16),
                vmem((heads, n_k, n_q), F32), vmem((8, heads, width, width), BF16), *pairs((heads, width, width), BF16),
                vmem((heads, width, width), F32),
                *pairs((n_k, chan), BF16), *pairs((n_k, proj), BF16), *pairs((proj, n_k), BF16),
                *pairs((proj, n_q), BF16), *pairs((proj, n_q), F32),
                *[vmem((n_k, n_q), F32)] * 8, *pairs((proj, n_q), BF16),
                pltpu.SemaphoreType.REGULAR((2,)), dma((len(smalls),)), dma((2,)), dma, dma, dma((CORES, groups)), dma((CORES, groups)), dma((3,)), dma((3,)), dma((3, 3)), dma((3, CORES)),
                dma((2, CORES)), dma((2, CORES)), dma((groups,)), dma((groups,)),
            ],
            compiler_params=pltpu.CompilerParams(collective_id=0, has_side_effects=True, vmem_limit_bytes=58_000_000),
        )(pair_tile, *smalls)
        return pl.pallas_call(
            write_out,
            in_specs=[pl.BlockSpec(memory_space=pl.ANY)],
            out_specs=hbm,
            out_shape=jax.ShapeDtypeStruct(pair_tile.shape, BF16),
            scratch_shapes=[dma((4,))],
            compiler_params=pltpu.CompilerParams(vmem_limit_bytes=4 * 1024 * 1024),
        )(result)

    return jax.shard_map(per_device, mesh=mesh, in_specs=(tile_spec, P('dp'), P(), P(), P(), P(), P(), P(), P(), P()), out_specs=tile_spec, check_vma=False)
```
